32 devices in a mesh: dp: 8 (over z, y), mp: 4 (over x, core).
Axes of the slice: x: 2, y: 2, z: 4, core: 2. Of those that a mesh axis runs over, the one named last changes fastest.
Arguments:
- tokens: bfloat16 [49152, 512], P('dp'), may hold values from -6 to 6
- w_uvqk: bfloat16 [512, 2048], P(None, 'mp')
- w_out: bfloat16 [512, 512], replicated, may hold values from -0.25 to 0.25
- hist_len: int32 [8, 24], P('dp'), may hold values from 64 to 256, as said below
- owner: int32 [8, 24], P('dp'), may hold values from 0 to 7, as said below
- recv_offset: int32 [8, 24], P('dp'), may hold values from 0 to 47, as said below
- block_start: int32 [8, 24], P('dp'), may hold values from 0 to 47, as said below
Outputs:
- packed_out: bfloat16 [49152, 512], P('dp', 'mp')
- user_state: bfloat16 [192, 512], P('dp', 'mp')
The draws below stay inside these ranges and needn't reach their ends.
Inputs may be any that keep to these rules, and one draw needn't show every extreme that they name: User (d, u) has ceil(hist_len / 128) blocks, at most 2. owner[d, u] = (p(d) + r(u mod 8)) mod 8 for two permutations p, r of the indices of dp drawn from the seed: every owner receives exactly 24 users, and one device sends at most 3 users to one owner. On some owner every received user has 2 blocks. `recv_offset`: the users of one owner occupy disjoint runs of its 48 blocks, in the order of u; on some owner they fill all 48 blocks. `block_start`: the users of one device occupy disjoint runs of its 48 blocks, in the order of u.
All inputs are finite; a program needn't handle non-finite values.
Results may differ from the reference program's by a relative error of at most 0.0059.
Values may be sent and summed in bfloat16 or wider, within the bound.
A program may use at most 128 MiB of HBM per device.

```python
import jax
import jax.numpy as jnp
from jax import lax

D = 512
HEADS = 4
BLOCK = 128
MAXB = 2
USERS_DEV = 24
BLK_DEV = 48
ROWS = 49152
N_DP = 8


def place_runs(key, run_sizes, salt_value):
    before = jnp.cumsum(run_sizes, axis=1) - run_sizes
    spare_blocks = BLK_DEV - jnp.sum(run_sizes, axis=1, keepdims=True)
    gap_sums = jnp.cumsum(jax.random.randint(jax.random.fold_in(key, salt_value), run_sizes.shape, 0, 2), axis=1)
    return (before + jnp.minimum(gap_sums, spare_blocks)).astype(jnp.int32)


def draw_tables(key):
    device_count = N_DP
    user_count = USERS_DEV
    dev_perm = jax.random.permutation(jax.random.fold_in(key, 101), device_count).astype(jnp.int32)
    user_perm = jax.random.permutation(jax.random.fold_in(key, 102), device_count).astype(jnp.int32)
    user_ids = jnp.arange(user_count, dtype=jnp.int32)
    shifts = user_perm[user_ids % device_count]
    owners = ((dev_perm[:, None] + shifts[None, :]) % device_count).astype(jnp.int32)
    hottest = jax.random.randint(jax.random.fold_in(key, 103), (), 0, device_count)
    coin_flip = jax.random.randint(jax.random.fold_in(key, 104), (device_count, user_count), 0, 4)
    small_count = jax.random.randint(jax.random.fold_in(key, 108), (device_count, user_count), 1, MAXB + 1)
    counts = jnp.where(coin_flip > 0, MAXB, small_count)
    counts = jnp.where(owners == hottest, MAXB, counts).astype(jnp.int32)
    least_tail = jnp.where(counts == 1, BLOCK // 2, 1)
    extra_rows = jax.random.randint(jax.random.fold_in(key, 105), (device_count, user_count), 0, BLOCK + 1)
    last_fill = least_tail + extra_rows % (BLOCK + 1 - least_tail)
    lengths = ((counts - 1) * BLOCK + last_fill).astype(jnp.int32)
    starts = place_runs(key, counts, 106)
    inverse = jnp.zeros((device_count,), jnp.int32).at[dev_perm].set(jnp.arange(device_count, dtype=jnp.int32))
    sources = inverse[(jnp.arange(device_count, dtype=jnp.int32)[:, None] - shifts[None, :]) % device_count]
    incoming = counts[sources, user_ids[None, :]]
    landing = place_runs(key, incoming, 107)
    offsets = landing[owners, user_ids[None, :]].astype(jnp.int32)
    return (lengths, owners, offsets, starts)


def draw_hist_len(key, part):
    return draw_tables(key)[0]


def draw_owner(key, part):
    return draw_tables(key)[1]


def draw_recv_offset(key, part):
    return draw_tables(key)[2]


def draw_block_start(key, part):
    return draw_tables(key)[3]


def draw_w_uvqk(key, part):
    base_draw = jax.random.normal(jax.random.fold_in(key, 1), (D, 4 * D), jnp.float32)
    log_scale = jax.random.uniform(jax.random.fold_in(key, 2), (1, 4 * D), jnp.float32, -1.2, 1.2)
    return (base_draw * jnp.exp(log_scale) / jnp.sqrt(D * 1.0)).astype(jnp.bfloat16)


def shard_levels(rng, extent, split, least, high):
    factor_of = 1.0
    for dim, parts in split:
        steps = jax.random.uniform(jax.random.fold_in(jax.random.fold_in(rng, 6), dim), (parts,), jnp.float32, least / len(split), high / len(split))
        factor_of = factor_of * jnp.repeat(jnp.exp(steps), extent[dim] // parts).reshape((-1,) + (1,) * (len(extent) - 1 - dim))
    return factor_of


def normal_values(key, extent, spread, bound, split=(), held_as=jnp.bfloat16):
    values = jax.random.normal(key, extent, jnp.float32) * spread
    if len(split) > 0:
        values = shard_levels(key, extent, split, -0.22, 0.18) * values
    return jnp.clip(values, min=-bound, max=bound).astype(held_as)


def setup_inputs(seed: int = 0) -> dict:
    key_of = jax.random.split(jax.random.key(seed), 8)
    tokens = normal_values(key_of[0], (ROWS, D), 1.0, 6.0, ((0, 8),))
    w_uvqk = draw_w_uvqk(jax.random.fold_in(key_of[7], 71), 0)
    w_out = normal_values(key_of[2], (D, D), D ** -0.5, 0.25)
    hist_len = draw_hist_len(jax.random.fold_in(key_of[7], 71), 0)
    owner = draw_owner(jax.random.fold_in(key_of[7], 71), 0)
    recv_offset = draw_recv_offset(jax.random.fold_in(key_of[7], 71), 0)
    block_start = draw_block_start(jax.random.fold_in(key_of[7], 71), 0)
    return dict(tokens=tokens, w_uvqk=w_uvqk, w_out=w_out, hist_len=hist_len, owner=owner, recv_offset=recv_offset, block_start=block_start)


EPS = 1e-05

def norm_rows(values):
    average = lax.optimization_barrier(jnp.mean(values, axis=-1, keepdims=True))
    variance = lax.optimization_barrier(jnp.mean(values * values, axis=-1, keepdims=True)) - average * average
    return (values - average) * lax.rsqrt(variance + EPS)

def rounded(values):
    return lax.optimization_barrier(values.astype(jnp.bfloat16)).astype(jnp.float32)

def reference(tokens, w_uvqk, w_out, hist_len, owner, recv_offset, block_start):
    head_size = D // HEADS
    window_rows = MAXB * BLOCK
    total_rows = tokens.shape[0]
    device_count = hist_len.shape[0]
    user_count = hist_len.shape[1]
    padded = jnp.concatenate([tokens, jnp.zeros((window_rows, D), tokens.dtype)], 0)
    position = jnp.arange(window_rows, dtype=jnp.int32)
    causal = position[None, :] <= position[:, None]
    device_ids = (jnp.arange(device_count * user_count, dtype=jnp.int32) // user_count).astype(jnp.int32)
    flat_len = hist_len.reshape(-1).astype(jnp.int32)
    flat_start = block_start.reshape(-1).astype(jnp.int32)
    flat_owner = owner.reshape(-1).astype(jnp.int32)
    flat_offset = recv_offset.reshape(-1).astype(jnp.int32)

    def one_user(user_item):
        device_id, length, start = user_item
        first_row = ((device_id * BLK_DEV + start) * BLOCK).astype(jnp.int32)
        rows_in = lax.dynamic_slice_in_dim(padded, first_row, window_rows, 0)
        widened = rows_in.astype(jnp.float32)
        normed = norm_rows(widened).astype(jnp.bfloat16)
        projected = jax.nn.silu(jnp.dot(normed, w_uvqk, preferred_element_type=jnp.float32))
        pieces = rounded(projected).reshape(window_rows, HEADS, 4, head_size)
        raw_scores = jnp.einsum('ihd,jhd->hij', pieces[:, :, 2], pieces[:, :, 3]) * head_size ** (-0.5)
        allowed = causal & (position[None, :] < length)
        weights = rounded(jnp.where(allowed[None], jax.nn.silu(raw_scores) / window_rows, 0.0))
        attended = jnp.einsum('hij,jhd->ihd', weights, pieces[:, :, 1]).reshape(window_rows, D)
        gated_rows = (norm_rows(attended) * pieces[:, :, 0].reshape(window_rows, D)).astype(jnp.bfloat16)
        mixed_rows = jnp.dot(gated_rows, w_out, preferred_element_type=jnp.float32) + widened
        return mixed_rows.astype(jnp.bfloat16)
    outputs = lax.map(one_user, (device_ids, flat_len, flat_start))
    targets = ((flat_owner * BLK_DEV + flat_offset) * BLOCK)[:, None] + position[None, :]
    targets = jnp.where(position[None, :] < flat_len[:, None], targets, total_rows).astype(jnp.int32)
    packed = jnp.zeros((total_rows + 1, D), jnp.bfloat16)
    packed = packed.at[targets.reshape(-1)].set(outputs.reshape(-1, D))[:total_rows]
    user_state = outputs[jnp.arange(device_count * user_count, dtype=jnp.int32), flat_len - 1]
    return (packed, user_state)
```

```python
import functools

import jax
import jax.numpy as jnp
from jax import lax
from jax.experimental import pallas as pl
from jax.experimental.pallas import tpu as pltpu
from jax.sharding import PartitionSpec as P

D = 512
HEADS = 4
HEAD = D // HEADS
BLOCK = 128
MAXB = 2
WIN = MAXB * BLOCK
EPS = 1e-05
CHUNKS = 4
MESH = pl.DeviceIdType.MESH


def norm_rows(values):
    average = jnp.mean(values, axis=-1, keepdims=True)
    variance = jnp.mean(values * values, axis=-1, keepdims=True) - average * average
    return (values - average) * lax.rsqrt(variance + EPS)


def layer_kernel(
    dp_size, mp_size, per_pair, user_count,
    tok_hbm, w_hbm, wout_hbm, owner_hbm, len_hbm, off_hbm, start_hbm,
    packed, state,
    tok, buf, wg, wop, send, state_out, arr, state_in, state32, meta_my, meta_in, inv_v,
    owner_s, len_s, off_s, start_s, meta_s, inv_s,
    tab_sem, tok_sem, w_sem, wop_sem, w_send, w_recv, meta_send, meta_recv, row_send, row_recv,
    send_sem, recv_sem, state_send, state_recv, local_sem,
):
    d = lax.axis_index("dp")
    m = lax.axis_index("mp")
    quarter = D // mp_size
    reach = dp_size // mp_size
    slots = reach * per_pair
    pairs = dp_size * per_pair
    blocks = packed.shape[0]
    last_block = tok_hbm.shape[0] - 1
    barrier = pltpu.get_barrier_semaphore()

    def greet(step, carry):
        o = lax.rem(d + step // mp_size, dp_size)
        q = lax.rem(m + lax.rem(step, mp_size), mp_size)
        pl.semaphore_signal(barrier, inc=1, device_id={"dp": o, "mp": q}, device_id_type=MESH)
        return carry

    tables = [
        pltpu.make_async_copy(src, dst, tab_sem.at[i])
        for i, (src, dst) in enumerate(
            ((owner_hbm, owner_s), (len_hbm, len_s), (off_hbm, off_s), (start_hbm, start_s))
        )
    ]
    for table in tables:
        table.start()
    tok_copy = pltpu.make_async_copy(tok_hbm, tok, tok_sem)
    tok_copy.start()
    own_w = pltpu.make_async_copy(w_hbm, wg.at[0], w_sem)
    own_w.start()
    lax.fori_loop(1, dp_size * mp_size, greet, 0)

    def flip(bits):
        if bits == 1:
            return m + 1 - 2 * lax.rem(m, 2)
        return lax.rem(m + 2, 4)

    wop_copies = []
    for bits in range(mp_size):
        head = m
        if bits & 1:
            head = head + 1 - 2 * lax.rem(head, 2)
        if bits & 2:
            head = lax.rem(head + 2, 4)
        copy = pltpu.make_async_copy(
            wout_hbm.at[pl.ds(pl.multiple_of(head * HEAD, HEAD), HEAD)],
            wop.at[pl.ds(bits * HEAD, HEAD)], wop_sem.at[bits],
        )
        copy.start()
        wop_copies.append(copy)

    def target(s):
        k = s // per_pair
        return lax.rem(d + m + mp_size * k, dp_size)

    def source(s):
        k = s // per_pair
        return lax.rem(d - m - mp_size * k + 2 * dp_size, dp_size), s - k * per_pair

    def moves(s):
        k = s // per_pair
        j = s - k * per_pair
        return jnp.logical_and(j < 1 + lax.rem(m, 2), target(s) != d)

    def crosses(s):
        return (target(s) < dp_size // 2) != (d < dp_size // 2)

    def find(o):
        first = 0
        found = 0
        for u in range(min(dp_size, user_count)):
            hit = owner_s[0, u] == o
            first = jnp.where(hit, u, first)
            found = jnp.where(hit, 1, found)
        return first, found

    def user_of(o, j):
        first, found = find(o)
        u = first + j * dp_size
        valid = jnp.logical_and(found == 1, u < user_count)
        return jnp.minimum(u, user_count - 1), valid

    for table in tables:
        table.wait()

    lanes = lax.broadcasted_iota(jnp.int32, (1, 128), 1)

    def fill_meta(o, carry):
        first, found = find(o)
        row = jnp.zeros((1, 128), jnp.int32)
        for j in range(per_pair):
            u = first + j * dp_size
            valid = jnp.logical_and(found == 1, u < user_count)
            u = jnp.minimum(u, user_count - 1)
            row = jnp.where(lanes == 2 * j, jnp.where(valid, len_s[0, u], 0), row)
            row = jnp.where(lanes == 2 * j + 1, off_s[0, u], row)
        meta_my[o] = row
        return carry

    lax.fori_loop(0, dp_size, fill_meta, 0)
    meta_in[d] = meta_my[d]
    zero_block = 2 * pairs
    arr[zero_block] = jnp.zeros((BLOCK, quarter), arr.dtype)
    tok_copy.wait()

    def stage(s):
        k = s // per_pair
        u, _ = user_of(target(s), s - k * per_pair)
        start = start_s[0, u]
        for b in range(MAXB):
            buf[0, s, b] = tok[jnp.minimum(start + b, last_block)]

    def stage_moved(s, carry):
        @pl.when(moves(s))
        def _():
            stage(s)

        return carry

    def stage_home(s, carry):
        @pl.when(jnp.logical_not(moves(s)))
        def _():
            stage(s)

        return carry

    lax.fori_loop(0, slots, stage_moved, 0)
    own_w.wait()

    pl.semaphore_wait(barrier, dp_size * mp_size - 1)

    def meta_copy(step):
        o = lax.rem(d + step, dp_size)
        return pltpu.make_async_remote_copy(
            src_ref=meta_my.at[o], dst_ref=meta_in.at[d], send_sem=meta_send.at[step],
            recv_sem=meta_recv.at[d], device_id={"dp": o}, device_id_type=MESH,
        )

    def start_meta(step, carry):
        meta_copy(step).start()
        return carry

    lax.fori_loop(1, dp_size, start_meta, 0)

    def row_copy(s):
        return pltpu.make_async_remote_copy(
            src_ref=buf.at[0, s], dst_ref=buf.at[1, s], send_sem=row_send.at[s],
            recv_sem=row_recv.at[s], device_id={"dp": target(s)}, device_id_type=MESH,
        )

    def row_local(s):
        return pltpu.make_async_copy(buf.at[0, s], buf.at[1, s], row_recv.at[s])

    def start_rows(i, carry):
        late = i // slots
        s = i - late * slots

        @pl.when(jnp.logical_and(moves(s), crosses(s) == (late == 0)))
        def _():
            row_copy(s).start()

        return carry

    lax.fori_loop(0, 2 * slots, start_rows, 0)

    piece = D // CHUNKS

    def w_copy(src, dst, chunk, peer, index):
        rows = pl.ds(chunk * piece, piece)
        return pltpu.make_async_remote_copy(
            src_ref=wg.at[src, rows], dst_ref=wg.at[dst, rows], send_sem=w_send.at[index, chunk],
            recv_sem=w_recv.at[index, chunk], device_id={"mp": peer}, device_id_type=MESH,
        )

    far = [w_copy(0, 2, c, flip(2), 1) for c in range(CHUNKS)]
    near = [w_copy(0, 1, c, flip(1), 0) for c in range(CHUNKS)]
    relay = [w_copy(2, 3, c, flip(1), 2) for c in range(CHUNKS)]
    for copy in far:
        copy.start()
    for copy in near:
        copy.start()

    lax.fori_loop(0, slots, stage_home, 0)

    causal = lax.broadcasted_iota(jnp.int32, (BLOCK, BLOCK), 1) <= lax.broadcasted_iota(
        jnp.int32, (BLOCK, BLOCK), 0
    )
    half_scale = 0.5 * HEAD ** (-0.5)

    def scores(q, k):
        t = lax.dot_general(
            q, k, (((1,), (1,)), ((), ())), preferred_element_type=jnp.float32
        ) * half_scale
        return t + t * jnp.tanh(t)

    def one_head(rows_in, bits):
        h = jnp.dot(rows_in, wg[bits], preferred_element_type=jnp.float32) * 0.5
        p = (h + h * jnp.tanh(h)).astype(jnp.bfloat16)
        u, v, q, k = (p[:, i * HEAD : (i + 1) * HEAD] for i in range(4))
        low = jnp.where(causal, scores(q[:BLOCK], k[:BLOCK]), 0.0).astype(jnp.bfloat16)
        back = scores(q[BLOCK:], k[:BLOCK])
        diag = jnp.where(causal, scores(q[BLOCK:], k[BLOCK:]), 0.0)
        high = jnp.concatenate([back, diag], 1).astype(jnp.bfloat16)
        first = jnp.dot(low, v[:BLOCK], preferred_element_type=jnp.float32)
        second = jnp.dot(high, v, preferred_element_type=jnp.float32)
        return u, jnp.concatenate([first, second], 0) * (1.0 / WIN)

    for copy in wop_copies:
        copy.wait()
    for copy in near:
        copy.wait()
    for c in range(CHUNKS):
        far[c].wait()
        relay[c].start()
    for c in range(CHUNKS):
        relay[c].wait()

    def route(s):
        src, j = source(s)
        moved = moves(s)
        home = jnp.where(moved, src, d)
        there = jnp.where(moved, d, target(s))
        return moved, home, there, j

    def send_copy(s, q):
        _, home, there, j = route(s)
        pair = home * per_pair + j
        return pltpu.make_async_remote_copy(
            src_ref=send.at[s, q], dst_ref=arr.at[pl.ds(MAXB * pair, MAXB)],
            send_sem=send_sem.at[s, q], recv_sem=recv_sem.at[pair],
            device_id={"dp": there, "mp": q}, device_id_type=MESH,
        )

    def send_local(s, q, pair):
        return pltpu.make_async_copy(
            send.at[s, q], arr.at[pl.ds(MAXB * pair, MAXB)], recv_sem.at[pair]
        )

    def state_copy(s, q):
        _, home, there, j = route(s)
        pair = there * per_pair + j
        return pltpu.make_async_remote_copy(
            src_ref=state_out.at[s, q], dst_ref=state_in.at[pair], send_sem=state_send.at[s, q],
            recv_sem=state_recv.at[pair], device_id={"dp": home, "mp": q}, device_id_type=MESH,
        )

    def state_local(s, q, pair):
        return pltpu.make_async_copy(state_out.at[s, q], state_in.at[pair], state_recv.at[pair])

    picks = lax.broadcasted_iota(jnp.int32, (8, WIN), 1)
    positions = lax.broadcasted_iota(jnp.int32, (WIN, D), 0)

    def one_user(s, length):
        moved, home, there, j = route(s)
        rows_in = buf[jnp.where(moved, 1, 0), s].reshape(WIN, D).astype(jnp.float32)
        n = norm_rows(rows_in).astype(jnp.bfloat16)
        parts = [one_head(n, bits) for bits in range(mp_size)]
        a = jnp.concatenate([part[1] for part in parts], 1)
        g = jnp.concatenate([part[0] for part in parts], 1).astype(jnp.float32)
        gated = (norm_rows(a) * g).astype(jnp.bfloat16)
        y = jnp.dot(gated, wop[...], preferred_element_type=jnp.float32)
        y = jnp.where(positions < length, y + rows_in, 0.0).astype(jnp.bfloat16)
        for q in range(mp_size):
            send[s, q] = y[:, q * quarter : (q + 1) * quarter].reshape(MAXB, BLOCK, quarter)
        pick = jnp.where(picks == length - 1, 1.0, 0.0).astype(jnp.bfloat16)
        chosen = jnp.dot(pick, y, preferred_element_type=jnp.float32)
        for q in range(mp_size):
            state_out[s, q] = chosen[:, q * quarter : (q + 1) * quarter]
        pair = home * per_pair + j
        state_pair = there * per_pair + j
        for q in range(mp_size):
            own = jnp.logical_and(there == d, q == m)

            @pl.when(jnp.logical_not(own))
            def _():
                send_copy(s, q).start()

            @pl.when(own)
            def _():
                send_local(s, q, pair).start()

        for q in range(mp_size):
            own = jnp.logical_and(home == d, q == m)

            @pl.when(jnp.logical_not(own))
            def _():
                state_copy(s, q).start()

            @pl.when(own)
            def _():
                state_local(s, q, state_pair).start()

    def got_meta(step, carry):
        src = lax.rem(d + step, dp_size)
        pltpu.make_async_copy(meta_my.at[src], meta_in.at[src], meta_recv.at[src]).wait()
        return carry

    def read_meta():
        lax.fori_loop(1, dp_size, got_meta, 0)
        to_smem = pltpu.make_async_copy(meta_in, meta_s, local_sem)
        to_smem.start()
        to_smem.wait()

        def invert(i, row):
            src = i // per_pair
            j = i - src * per_pair
            length = meta_s[src, 0, 2 * j]
            offset = meta_s[src, 0, 2 * j + 1]
            for b in range(MAXB):
                at = jnp.where(length > b * BLOCK, offset + b, -1)
                row = jnp.where(lanes == at, MAXB * i + b, row)
            return row

        inv_v[...] = lax.fori_loop(
            0, pairs, invert, jnp.full((1, 128), zero_block, jnp.int32)
        )
        back = pltpu.make_async_copy(inv_v, inv_s, local_sem)
        back.start()
        back.wait()

    read_meta()

    def turn(i, carry):
        phase = i // slots
        s = i - phase * slots
        moved = moves(s)
        mine = jnp.where(moved, 2, jnp.where(crosses(s), 0, 1))

        @pl.when(mine == phase)
        def _():
            @pl.when(moved)
            def _():
                row_local(s).wait()

            k = s // per_pair
            j = s - k * per_pair
            src, _ = source(s)
            u, valid = user_of(target(s), j)
            home_len = jnp.where(valid, len_s[0, u], 0)
            one_user(s, jnp.where(moved, meta_s[src, 0, 2 * j], home_len))

        return carry

    lax.fori_loop(0, 3 * slots, turn, 0)

    def end_meta(step, carry):
        meta_copy(step).wait_send()
        return carry

    lax.fori_loop(1, dp_size, end_meta, 0)

    def end_rows(s, carry):
        @pl.when(moves(s))
        def _():
            row_copy(s).wait_send()

        return carry

    lax.fori_loop(0, slots, end_rows, 0)

    def sent(s, carry):
        _, home, there, _ = route(s)
        for q in range(mp_size):

            @pl.when(jnp.logical_not(jnp.logical_and(there == d, q == m)))
            def _():
                send_copy(s, q).wait_send()

            @pl.when(jnp.logical_not(jnp.logical_and(home == d, q == m)))
            def _():
                state_copy(s, q).wait_send()

        return carry

    lax.fori_loop(0, slots, sent, 0)

    def got(i, carry):
        send_local(0, 0, i).wait()
        state_local(0, 0, i).wait()
        return carry

    lax.fori_loop(0, pairs, got, 0)

    def place(b, carry):
        packed[b] = arr[inv_s[0, b]]
        return carry

    lax.fori_loop(0, blocks, place, 0)

    def pick_state(u, carry):
        at = owner_s[0, u] * per_pair + u // dp_size
        state32[pl.ds(u, 1), :] = state_in[at, 0:1, :]
        return carry

    lax.fori_loop(0, user_count, pick_state, 0)
    state[...] = state32[...].astype(state.dtype)


def per_device(tokens, w_uvqk, w_out, hist_len, owner, recv_offset, block_start):
    dp_size = lax.axis_size("dp")
    mp_size = lax.axis_size("mp")
    user_count = hist_len.shape[1]
    per_pair = -(-user_count // dp_size)
    pairs = dp_size * per_pair
    reach = dp_size // mp_size
    slots = reach * per_pair
    quarter = D // mp_size
    rows = tokens.shape[0]
    blocks = rows // BLOCK

    vmem = pl.BlockSpec(memory_space=pltpu.VMEM)
    anywhere = pl.BlockSpec(memory_space=pltpu.HBM)
    bf16, f32, i32 = jnp.bfloat16, jnp.float32, jnp.int32
    dma = pltpu.SemaphoreType.DMA
    packed, state = pl.pallas_call(
        functools.partial(layer_kernel, dp_size, mp_size, per_pair, user_count),
        out_shape=(
            jax.ShapeDtypeStruct((blocks, BLOCK, quarter), bf16),
            jax.ShapeDtypeStruct((user_count, quarter), bf16),
        ),
        in_specs=[anywhere] * 7,
        out_specs=(vmem, vmem),
        scratch_shapes=[
            pltpu.VMEM((blocks, BLOCK, D), bf16),
            pltpu.VMEM((2, slots, MAXB, BLOCK, D), bf16),
            pltpu.VMEM((mp_size, D, 4 * HEAD), bf16),
            pltpu.VMEM((D, D), bf16),
            pltpu.VMEM((slots, mp_size, MAXB, BLOCK, quarter), bf16),
            pltpu.VMEM((slots, mp_size, 8, quarter), f32),
            pltpu.VMEM((MAXB * pairs + 1, BLOCK, quarter), bf16),
            pltpu.VMEM((pairs, 8, quarter), f32),
            pltpu.VMEM((user_count, quarter), f32),
            pltpu.VMEM((dp_size, 1, 128), i32),
            pltpu.VMEM((dp_size, 1, 128), i32),
            pltpu.VMEM((1, 128), i32),
            pltpu.SMEM((1, user_count), i32),
            pltpu.SMEM((1, user_count), i32),
            pltpu.SMEM((1, user_count), i32),
            pltpu.SMEM((1, user_count), i32),
            pltpu.SMEM((dp_size, 1, 128), i32),
            pltpu.SMEM((1, 128), i32),
            dma((4,)),
            dma,
            dma,
            dma((mp_size,)),
            dma((3, CHUNKS)),
            dma((3, CHUNKS)),
            dma((dp_size,)),
            dma((dp_size,)),
            dma((slots,)),
            dma((slots,)),
            dma((slots, mp_size)),
            dma((pairs,)),
            dma((slots, mp_size)),
            dma((pairs,)),
            dma,
        ],
        compiler_params=pltpu.CompilerParams(
            collective_id=0, has_side_effects=True, vmem_limit_bytes=48 * 1024 * 1024
        ),
        name="layer",
    )(
        tokens.reshape(blocks, BLOCK, D), w_uvqk, w_out, owner, hist_len, recv_offset, block_start
    )
    return packed.reshape(rows, quarter), state


def solution(mesh):
    in_specs = (
        P("dp", None),
        P(None, "mp"),
        P(),
        P("dp", None),
        P("dp", None),
        P("dp", None),
        P("dp", None),
    )
    out_specs = (P("dp", "mp"), P("dp", "mp"))
    return jax.shard_map(
        per_device, mesh=mesh, in_specs=in_specs, out_specs=out_specs, check_vma=False
    )
```

```python
import functools

import jax
import jax.numpy as jnp
from jax import lax
from jax.experimental import pallas as pl
from jax.experimental.pallas import tpu as pltpu
from jax.sharding import PartitionSpec as P

D = 512
HEADS = 4
HEAD = D // HEADS
BLOCK = 128
MAXB = 2
WIN = MAXB * BLOCK
EPS = 1e-05
CHUNKS = 4
MESH = pl.DeviceIdType.MESH


def norm_rows(values):
    average = jnp.mean(values, axis=-1, keepdims=True)
    variance = jnp.mean(values * values, axis=-1, keepdims=True) - average * average
    return (values - average) * lax.rsqrt(variance + EPS)


def layer_kernel(
    dp_size, mp_size, per_pair, user_count,
    tok_hbm, w_hbm, wout_hbm, owner_s, len_s, off_s, start_s,
    packed, state,
    tok, buf, wg, wop, send, state_out, arr, state_in, state32, meta_my, meta_in, inv_v,
    meta_s, inv_s,
    tok_sem, w_sem, wop_sem, w_send, w_recv, meta_send, meta_recv, row_send, row_recv,
    send_sem, recv_sem, state_send, state_recv, local_sem,
):
    d = lax.axis_index("dp")
    m = lax.axis_index("mp")
    quarter = D // mp_size
    reach = dp_size // mp_size
    slots = reach * per_pair
    pairs = dp_size * per_pair
    blocks = packed.shape[0]
    last_block = tok_hbm.shape[0] - 1
    barrier = pltpu.get_barrier_semaphore()

    def greet(step, carry):
        o = lax.rem(d + step // mp_size, dp_size)
        q = lax.rem(m + lax.rem(step, mp_size), mp_size)
        pl.semaphore_signal(barrier, inc=1, device_id={"dp": o, "mp": q}, device_id_type=MESH)
        return carry

    tok_copy = pltpu.make_async_copy(tok_hbm, tok, tok_sem)
    tok_copy.start()
    own_w = pltpu.make_async_copy(w_hbm, wg.at[0], w_sem)
    own_w.start()
    lax.fori_loop(1, dp_size * mp_size, greet, 0)

    def flip(bits):
        if bits == 1:
            return m + 1 - 2 * lax.rem(m, 2)
        return lax.rem(m + 2, 4)

    wop_copies = []
    for bits in range(mp_size):
        head = m
        if bits & 1:
            head = head + 1 - 2 * lax.rem(head, 2)
        if bits & 2:
            head = lax.rem(head + 2, 4)
        copy = pltpu.make_async_copy(
            wout_hbm.at[pl.ds(pl.multiple_of(head * HEAD, HEAD), HEAD)],
            wop.at[pl.ds(bits * HEAD, HEAD)], wop_sem.at[bits],
        )
        copy.start()
        wop_copies.append(copy)

    def target(s):
        k = s // per_pair
        return lax.rem(d + m + mp_size * k, dp_size)

    def source(s):
        k = s // per_pair
        return lax.rem(d - m - mp_size * k + 2 * dp_size, dp_size), s - k * per_pair

    def moves(s):
        k = s // per_pair
        j = s - k * per_pair
        return jnp.logical_and(j < 1 + lax.rem(m, 2), target(s) != d)

    def crosses(s):
        return (target(s) < dp_size // 2) != (d < dp_size // 2)

    def find(o):
        first = 0
        found = 0
        for u in range(min(dp_size, user_count)):
            hit = owner_s[0, u] == o
            first = jnp.where(hit, u, first)
            found = jnp.where(hit, 1, found)
        return first, found

    def user_of(o, j):
        first, found = find(o)
        u = first + j * dp_size
        valid = jnp.logical_and(found == 1, u < user_count)
        return jnp.minimum(u, user_count - 1), valid

    lanes = lax.broadcasted_iota(jnp.int32, (1, 128), 1)

    def fill_meta(o, carry):
        first, found = find(o)
        row = jnp.zeros((1, 128), jnp.int32)
        for j in range(per_pair):
            u = first + j * dp_size
            valid = jnp.logical_and(found == 1, u < user_count)
            u = jnp.minimum(u, user_count - 1)
            row = jnp.where(lanes == 2 * j, jnp.where(valid, len_s[0, u], 0), row)
            row = jnp.where(lanes == 2 * j + 1, off_s[0, u], row)
        meta_my[o] = row
        return carry

    lax.fori_loop(0, dp_size, fill_meta, 0)
    meta_in[d] = meta_my[d]
    zero_block = 2 * pairs
    arr[zero_block] = jnp.zeros((BLOCK, quarter), arr.dtype)
    tok_copy.wait()

    def stage(s):
        k = s // per_pair
        u, _ = user_of(target(s), s - k * per_pair)
        start = start_s[0, u]
        for b in range(MAXB):
            buf[0, s, b] = tok[jnp.minimum(start + b, last_block)]

    def stage_moved(s, carry):
        @pl.when(moves(s))
        def _():
            stage(s)

        return carry

    def stage_home(s, carry):
        @pl.when(jnp.logical_not(moves(s)))
        def _():
            stage(s)

        return carry

    lax.fori_loop(0, slots, stage_moved, 0)
    own_w.wait()

    pl.semaphore_wait(barrier, dp_size * mp_size - 1)

    def meta_copy(step):
        o = lax.rem(d + step, dp_size)
        return pltpu.make_async_remote_copy(
            src_ref=meta_my.at[o], dst_ref=meta_in.at[d], send_sem=meta_send.at[step],
            recv_sem=meta_recv.at[d], device_id={"dp": o}, device_id_type=MESH,
        )

    def start_meta(step, carry):
        meta_copy(step).start()
        return carry

    lax.fori_loop(1, dp_size, start_meta, 0)

    def row_copy(s):
        return pltpu.make_async_remote_copy(
            src_ref=buf.at[0, s], dst_ref=buf.at[1, s], send_sem=row_send.at[s],
            recv_sem=row_recv.at[s], device_id={"dp": target(s)}, device_id_type=MESH,
        )

    def row_local(s):
        return pltpu.make_async_copy(buf.at[0, s], buf.at[1, s], row_recv.at[s])

    def start_rows(i, carry):
        late = i // slots
        s = i - late * slots

        @pl.when(jnp.logical_and(moves(s), crosses(s) == (late == 0)))
        def _():
            row_copy(s).start()

        return carry

    lax.fori_loop(0, 2 * slots, start_rows, 0)

    piece = D // CHUNKS

    def w_copy(src, dst, chunk, peer, index):
        rows = pl.ds(chunk * piece, piece)
        return pltpu.make_async_remote_copy(
            src_ref=wg.at[src, rows], dst_ref=wg.at[dst, rows], send_sem=w_send.at[index, chunk],
            recv_sem=w_recv.at[index, chunk], device_id={"mp": peer}, device_id_type=MESH,
        )

    far = [w_copy(0, 2, c, flip(2), 1) for c in range(CHUNKS)]
    near = [w_copy(0, 1, c, flip(1), 0) for c in range(CHUNKS)]
    relay = [w_copy(2, 3, c, flip(1), 2) for c in range(CHUNKS)]
    for copy in far:
        copy.start()
    for copy in near:
        copy.start()

    lax.fori_loop(0, slots, stage_home, 0)

    causal = lax.broadcasted_iota(jnp.int32, (BLOCK, BLOCK), 1) <= lax.broadcasted_iota(
        jnp.int32, (BLOCK, BLOCK), 0
    )
    half_scale = 0.5 * HEAD ** (-0.5)

    def scores(q, k):
        t = lax.dot_general(
            q, k, (((1,), (1,)), ((), ())), preferred_element_type=jnp.float32
        ) * half_scale
        return t + t * jnp.tanh(t)

    def one_head(rows_in, bits):
        h = jnp.dot(rows_in, wg[bits], preferred_element_type=jnp.float32) * 0.5
        p = (h + h * jnp.tanh(h)).astype(jnp.bfloat16)
        u, v, q, k = (p[:, i * HEAD : (i + 1) * HEAD] for i in range(4))
        low = jnp.where(causal, scores(q[:BLOCK], k[:BLOCK]), 0.0).astype(jnp.bfloat16)
        back = scores(q[BLOCK:], k[:BLOCK])
        diag = jnp.where(causal, scores(q[BLOCK:], k[BLOCK:]), 0.0)
        high = jnp.concatenate([back, diag], 1).astype(jnp.bfloat16)
        first = jnp.dot(low, v[:BLOCK], preferred_element_type=jnp.float32)
        second = jnp.dot(high, v, preferred_element_type=jnp.float32)
        return u, jnp.concatenate([first, second], 0) * (1.0 / WIN)

    for copy in wop_copies:
        copy.wait()
    for copy in near:
        copy.wait()
    for c in range(CHUNKS):
        far[c].wait()
        relay[c].start()
    for c in range(CHUNKS):
        relay[c].wait()

    def route(s):
        src, j = source(s)
        moved = moves(s)
        home = jnp.where(moved, src, d)
        there = jnp.where(moved, d, target(s))
        return moved, home, there, j

    def send_copy(s, q):
        _, home, there, j = route(s)
        pair = home * per_pair + j
        return pltpu.make_async_remote_copy(
            src_ref=send.at[s, q], dst_ref=arr.at[pl.ds(MAXB * pair, MAXB)],
            send_sem=send_sem.at[s, q], recv_sem=recv_sem.at[pair],
            device_id={"dp": there, "mp": q}, device_id_type=MESH,
        )

    def send_local(s, q, pair):
        return pltpu.make_async_copy(
            send.at[s, q], arr.at[pl.ds(MAXB * pair, MAXB)], recv_sem.at[pair]
        )

    def state_copy(s, q):
        _, home, there, j = route(s)
        pair = there * per_pair + j
        return pltpu.make_async_remote_copy(
            src_ref=state_out.at[s, q], dst_ref=state_in.at[pair], send_sem=state_send.at[s, q],
            recv_sem=state_recv.at[pair], device_id={"dp": home, "mp": q}, device_id_type=MESH,
        )

    def state_local(s, q, pair):
        return pltpu.make_async_copy(state_out.at[s, q], state_in.at[pair], state_recv.at[pair])

    picks = lax.broadcasted_iota(jnp.int32, (8, WIN), 1)
    positions = lax.broadcasted_iota(jnp.int32, (WIN, D), 0)

    def one_user(s, length):
        moved, home, there, j = route(s)
        rows_in = buf[jnp.where(moved, 1, 0), s].reshape(WIN, D).astype(jnp.float32)
        n = norm_rows(rows_in).astype(jnp.bfloat16)
        parts = [one_head(n, bits) for bits in range(mp_size)]
        a = jnp.concatenate([part[1] for part in parts], 1)
        g = jnp.concatenate([part[0] for part in parts], 1).astype(jnp.float32)
        gated = (norm_rows(a) * g).astype(jnp.bfloat16)
        y = jnp.dot(gated, wop[...], preferred_element_type=jnp.float32)
        y = jnp.where(positions < length, y + rows_in, 0.0).astype(jnp.bfloat16)
        for q in range(mp_size):
            send[s, q] = y[:, q * quarter : (q + 1) * quarter].reshape(MAXB, BLOCK, quarter)
        pick = jnp.where(picks == length - 1, 1.0, 0.0).astype(jnp.bfloat16)
        chosen = jnp.dot(pick, y, preferred_element_type=jnp.float32)
        for q in range(mp_size):
            state_out[s, q] = chosen[:, q * quarter : (q + 1) * quarter]
        pair = home * per_pair + j
        state_pair = there * per_pair + j
        for q in range(mp_size):
            own = jnp.logical_and(there == d, q == m)

            @pl.when(jnp.logical_not(own))
            def _():
                send_copy(s, q).start()

            @pl.when(own)
            def _():
                send_local(s, q, pair).start()

        for q in range(mp_size):
            own = jnp.logical_and(home == d, q == m)

            @pl.when(jnp.logical_not(own))
            def _():
                state_copy(s, q).start()

            @pl.when(own)
            def _():
                state_local(s, q, state_pair).start()

    def got_meta(step, carry):
        src = lax.rem(d + step, dp_size)
        pltpu.make_async_copy(meta_my.at[src], meta_in.at[src], meta_recv.at[src]).wait()
        return carry

    def read_meta():
        lax.fori_loop(1, dp_size, got_meta, 0)
        to_smem = pltpu.make_async_copy(meta_in, meta_s, local_sem)
        to_smem.start()
        to_smem.wait()

        def invert(i, row):
            src = i // per_pair
            j = i - src * per_pair
            length = meta_s[src, 0, 2 * j]
            offset = meta_s[src, 0, 2 * j + 1]
            for b in range(MAXB):
                at = jnp.where(length > b * BLOCK, offset + b, -1)
                row = jnp.where(lanes == at, MAXB * i + b, row)
            return row

        inv_v[...] = lax.fori_loop(
            0, pairs, invert, jnp.full((1, 128), zero_block, jnp.int32)
        )
        back = pltpu.make_async_copy(inv_v, inv_s, local_sem)
        back.start()
        back.wait()

    read_meta()

    def turn(i, carry):
        phase = i // slots
        s = i - phase * slots
        moved = moves(s)
        mine = jnp.where(moved, 2, jnp.where(crosses(s), 0, 1))

        @pl.when(mine == phase)
        def _():
            @pl.when(moved)
            def _():
                row_local(s).wait()

            k = s // per_pair
            j = s - k * per_pair
            src, _ = source(s)
            u, valid = user_of(target(s), j)
            home_len = jnp.where(valid, len_s[0, u], 0)
            one_user(s, jnp.where(moved, meta_s[src, 0, 2 * j], home_len))

        return carry

    lax.fori_loop(0, 3 * slots, turn, 0)

    def end_meta(step, carry):
        meta_copy(step).wait_send()
        return carry

    lax.fori_loop(1, dp_size, end_meta, 0)

    def end_rows(s, carry):
        @pl.when(moves(s))
        def _():
            row_copy(s).wait_send()

        return carry

    lax.fori_loop(0, slots, end_rows, 0)

    def sent(s, carry):
        _, home, there, _ = route(s)
        for q in range(mp_size):

            @pl.when(jnp.logical_not(jnp.logical_and(there == d, q == m)))
            def _():
                send_copy(s, q).wait_send()

            @pl.when(jnp.logical_not(jnp.logical_and(home == d, q == m)))
            def _():
                state_copy(s, q).wait_send()

        return carry

    lax.fori_loop(0, slots, sent, 0)

    def got(i, carry):
        send_local(0, 0, i).wait()
        state_local(0, 0, i).wait()
        return carry

    lax.fori_loop(0, pairs, got, 0)

    def place(b, carry):
        packed[b] = arr[inv_s[0, b]]
        return carry

    lax.fori_loop(0, blocks, place, 0)

    def pick_state(u, carry):
        at = owner_s[0, u] * per_pair + u // dp_size
        state32[pl.ds(u, 1), :] = state_in[at, 0:1, :]
        return carry

    lax.fori_loop(0, user_count, pick_state, 0)
    state[...] = state32[...].astype(state.dtype)


def per_device(tokens, w_uvqk, w_out, hist_len, owner, recv_offset, block_start):
    dp_size = lax.axis_size("dp")
    mp_size = lax.axis_size("mp")
    user_count = hist_len.shape[1]
    per_pair = -(-user_count // dp_size)
    pairs = dp_size * per_pair
    reach = dp_size // mp_size
    slots = reach * per_pair
    quarter = D // mp_size
    rows = tokens.shape[0]
    blocks = rows // BLOCK

    vmem = pl.BlockSpec(memory_space=pltpu.VMEM)
    smem = pl.BlockSpec(memory_space=pltpu.SMEM)
    anywhere = pl.BlockSpec(memory_space=pltpu.HBM)
    bf16, f32, i32 = jnp.bfloat16, jnp.float32, jnp.int32
    dma = pltpu.SemaphoreType.DMA
    packed, state = pl.pallas_call(
        functools.partial(layer_kernel, dp_size, mp_size, per_pair, user_count),
        out_shape=(
            pltpu.VMEM((blocks, BLOCK, quarter), bf16),
            pltpu.VMEM((user_count, quarter), bf16),
        ),
        in_specs=[anywhere] * 3 + [smem] * 4,
        out_specs=(vmem, vmem),
        scratch_shapes=[
            pltpu.VMEM((blocks, BLOCK, D), bf16),
            pltpu.VMEM((2, slots, MAXB, BLOCK, D), bf16),
            pltpu.VMEM((mp_size, D, 4 * HEAD), bf16),
            pltpu.VMEM((D, D), bf16),
            pltpu.VMEM((slots, mp_size, MAXB, BLOCK, quarter), bf16),
            pltpu.VMEM((slots, mp_size, 8, quarter), f32),
            pltpu.VMEM((MAXB * pairs + 1, BLOCK, quarter), bf16),
            pltpu.VMEM((pairs, 8, quarter), f32),
            pltpu.VMEM((user_count, quarter), f32),
            pltpu.VMEM((dp_size, 1, 128), i32),
            pltpu.VMEM((dp_size, 1, 128), i32),
            pltpu.VMEM((1, 128), i32),
            pltpu.SMEM((dp_size, 1, 128), i32),
            pltpu.SMEM((1, 128), i32),
            dma,
            dma,
            dma((mp_size,)),
            dma((3, CHUNKS)),
            dma((3, CHUNKS)),
            dma((dp_size,)),
            dma((dp_size,)),
            dma((slots,)),
            dma((slots,)),
            dma((slots, mp_size)),
            dma((pairs,)),
            dma((slots, mp_size)),
            dma((pairs,)),
            dma,
        ],
        compiler_params=pltpu.CompilerParams(
            collective_id=0, has_side_effects=True, vmem_limit_bytes=56 * 1024 * 1024
        ),
        name="layer",
    )(
        *(
            pltpu.with_memory_space_constraint(a, pltpu.HBM)
            for a in (tokens.reshape(blocks, BLOCK, D), w_uvqk, w_out)
        ),
        owner, hist_len, recv_offset, block_start,
    )
    return packed.reshape(rows, quarter), state


def solution(mesh):
    in_specs = (
        P("dp", None),
        P(None, "mp"),
        P(),
        P("dp", None),
        P("dp", None),
        P("dp", None),
        P("dp", None),
    )
    out_specs = (P("dp", "mp"), P("dp", "mp"))
    return jax.shard_map(
        per_device, mesh=mesh, in_specs=in_specs, out_specs=out_specs, check_vma=False
    )
```

```python
import functools

import jax
import jax.numpy as jnp
from jax import lax
from jax.experimental import pallas as pl
from jax.experimental.pallas import tpu as pltpu
from jax.sharding import PartitionSpec as P

D = 512
HEADS = 4
HEAD = D // HEADS
BLOCK = 128
MAXB = 2
WIN = MAXB * BLOCK
EPS = 1e-05
CHUNKS = 4
MESH = pl.DeviceIdType.MESH


def norm_rows(values):
    average = jnp.mean(values, axis=-1, keepdims=True)
    variance = jnp.mean(values * values, axis=-1, keepdims=True) - average * average
    return (values - average) * lax.rsqrt(variance + EPS)


def layer_kernel(
    dp_size, mp_size, per_pair, moving, user_count,
    tok_hbm, w_hbm, wout_hbm, owner_hbm, len_hbm, off_hbm, start_hbm,
    arr, inv_s, state,
    tok, rows_out, rows_in, rows_home, wg, wop, wop_side, send, state_out, send_home, state_home,
    state_in, state32, meta_my, meta_in, inv_v, normed, gate, att,
    owner_s, len_s, off_s, start_s, meta_s,
    tab_sem, tok_sem, w_sem, wop_sem, side_sem, w_send, w_recv, meta_send, meta_recv, row_send, row_recv,
    send_sem, recv_sem, state_send, state_recv, send_home_sem, state_home_sem, local_sem,
):
    d = lax.axis_index("dp")
    m = lax.axis_index("mp")
    quarter = D // mp_size
    reach = dp_size // mp_size
    staying = per_pair - moving
    slots = reach * moving
    homes = 2 * reach * staying
    pairs = dp_size * per_pair
    side = D // 2
    first_q = m // 2 * 2
    last_block = tok_hbm.shape[0] - 1
    barrier = pltpu.get_barrier_semaphore()

    def greet(step, carry):
        o = lax.rem(d + step // mp_size, dp_size)
        q = lax.rem(m + lax.rem(step, mp_size), mp_size)
        pl.semaphore_signal(barrier, inc=1, device_id={"dp": o, "mp": q}, device_id_type=MESH)
        return carry

    lax.fori_loop(1, dp_size * mp_size, greet, 0)
    tables = [
        pltpu.make_async_copy(src, dst, tab_sem.at[i])
        for i, (src, dst) in enumerate(
            ((owner_hbm, owner_s), (start_hbm, start_s), (len_hbm, len_s), (off_hbm, off_s))
        )
    ]
    for table in tables:
        table.start()
    tok_copy = pltpu.make_async_copy(tok_hbm, tok, tok_sem)
    tok_copy.start()
    own_w = pltpu.make_async_copy(w_hbm, wg.at[0], w_sem)
    own_w.start()

    def flip(bits):
        if bits == 1:
            return m + 1 - 2 * lax.rem(m, 2)
        return lax.rem(m + 2, 4)

    wop_copies = []
    for bits in range(mp_size):
        head = m
        if bits & 1:
            head = head + 1 - 2 * lax.rem(head, 2)
        if bits & 2:
            head = lax.rem(head + 2, 4)
        copy = pltpu.make_async_copy(
            wout_hbm.at[pl.ds(pl.multiple_of(head * HEAD, HEAD), HEAD)],
            wop.at[pl.ds(bits * HEAD, HEAD)], wop_sem.at[bits],
        )
        copy.start()
        wop_copies.append(copy)
        if homes:
            copy = pltpu.make_async_copy(
                wout_hbm.at[
                    pl.ds(pl.multiple_of(head * HEAD, HEAD), HEAD),
                    pl.ds(pl.multiple_of(first_q * quarter, side), side),
                ],
                wop_side.at[pl.ds(bits * HEAD, HEAD)], side_sem.at[bits],
            )
            copy.start()
            wop_copies.append(copy)

    def target(s):
        k = s // moving
        return lax.rem(d + m + mp_size * k, dp_size), s - k * moving

    def source(s):
        k = s // moving
        return lax.rem(d - m - mp_size * k + 2 * dp_size, dp_size), s - k * moving

    def home_target(h):
        g = h // (reach * staying)
        r = h - g * (reach * staying)
        k = r // staying
        group = lax.rem(m + 2 * g, mp_size)
        return lax.rem(d + group + mp_size * k, dp_size), moving + r - k * staying

    def crosses(o):
        return (o < dp_size // 2) != (d < dp_size // 2)

    def find(o):
        first = 0
        found = 0
        for u in range(min(dp_size, user_count)):
            hit = owner_s[0, u] == o
            first = jnp.where(hit, u, first)
            found = jnp.where(hit, 1, found)
        return first, found

    def user_of(o, j):
        first, found = find(o)
        u = first + j * dp_size
        valid = jnp.logical_and(found == 1, u < user_count)
        return jnp.minimum(u, user_count - 1), valid

    for table in tables:
        table.wait()

    lanes = lax.broadcasted_iota(jnp.int32, (1, 128), 1)

    def fill_meta(o, carry):
        first, found = find(o)
        row = jnp.zeros((1, 128), jnp.int32)
        for j in range(per_pair):
            u = first + j * dp_size
            valid = jnp.logical_and(found == 1, u < user_count)
            u = jnp.minimum(u, user_count - 1)
            row = jnp.where(lanes == 2 * j, jnp.where(valid, len_s[0, u], 0), row)
            row = jnp.where(lanes == 2 * j + 1, off_s[0, u], row)
        meta_my[o] = row
        return carry

    lax.fori_loop(0, dp_size, fill_meta, 0)
    meta_in[d] = meta_my[d]
    zero_block = 2 * pairs
    arr[zero_block] = jnp.zeros((BLOCK, quarter), arr.dtype)
    tok_copy.wait()

    def stage(o, j, into):
        u, _ = user_of(o, j)
        start = start_s[0, u]
        for b in range(MAXB):
            into[b] = tok[jnp.minimum(start + b, last_block)]

    def stage_moved(s, carry):
        o, j = target(s)
        stage(o, j, rows_out.at[s])
        return carry

    def stage_home(h, carry):
        o, j = home_target(h)
        stage(o, j, rows_home.at[h])
        return carry

    lax.fori_loop(0, slots, stage_moved, 0)
    own_w.wait()

    pl.semaphore_wait(barrier, dp_size * mp_size - 1)

    def meta_copy(step):
        o = lax.rem(d + step, dp_size)
        return pltpu.make_async_remote_copy(
            src_ref=meta_my.at[o], dst_ref=meta_in.at[d], send_sem=meta_send.at[step],
            recv_sem=meta_recv.at[d], device_id={"dp": o}, device_id_type=MESH,
        )

    def start_meta(step, carry):
        meta_copy(step).start()
        return carry

    lax.fori_loop(1, dp_size, start_meta, 0)

    def row_copy(s):
        return pltpu.make_async_remote_copy(
            src_ref=rows_out.at[s], dst_ref=rows_in.at[s], send_sem=row_send.at[s],
            recv_sem=row_recv.at[s], device_id={"dp": target(s)[0]}, device_id_type=MESH,
        )

    def row_local(s):
        return pltpu.make_async_copy(rows_out.at[s], rows_in.at[s], row_recv.at[s])

    def start_rows(i, carry):
        late = i // slots
        s = i - late * slots
        o, _ = target(s)
        now = crosses(o) == (late == 0)

        @pl.when(jnp.logical_and(now, o != d))
        def _():
            row_copy(s).start()

        @pl.when(jnp.logical_and(now, o == d))
        def _():
            row_local(s).start()

        return carry

    lax.fori_loop(0, 2 * slots, start_rows, 0)

    piece = D // CHUNKS

    def w_copy(src, dst, chunk, peer, index):
        rows = pl.ds(chunk * piece, piece)
        return pltpu.make_async_remote_copy(
            src_ref=wg.at[src, rows], dst_ref=wg.at[dst, rows], send_sem=w_send.at[index, chunk],
            recv_sem=w_recv.at[index, chunk], device_id={"mp": peer}, device_id_type=MESH,
        )

    far = [w_copy(0, 2, c, flip(2), 1) for c in range(CHUNKS)]
    near = [w_copy(0, 1, c, flip(1), 0) for c in range(CHUNKS)]
    relay = [w_copy(2, 3, c, flip(1), 2) for c in range(CHUNKS)]
    for copy in far:
        copy.start()
    for copy in near:
        copy.start()

    lax.fori_loop(0, homes, stage_home, 0)

    causal = lax.broadcasted_iota(jnp.int32, (BLOCK, BLOCK), 1) <= lax.broadcasted_iota(
        jnp.int32, (BLOCK, BLOCK), 0
    )
    half_scale = 0.5 * HEAD ** (-0.5)

    def scores(q, k):
        t = lax.dot_general(
            q, k, (((1,), (1,)), ((), ())), preferred_element_type=jnp.float32
        ) * half_scale
        return t + t * jnp.tanh(t)

    def one_head(rows_in, bits):
        h = jnp.dot(rows_in, wg[bits], preferred_element_type=jnp.float32) * 0.5
        p = (h + h * jnp.tanh(h)).astype(jnp.bfloat16)
        u, v, q, k = (p[:, i * HEAD : (i + 1) * HEAD] for i in range(4))
        low = jnp.where(causal, scores(q[:BLOCK], k[:BLOCK]), 0.0).astype(jnp.bfloat16)
        back = scores(q[BLOCK:], k[:BLOCK])
        diag = jnp.where(causal, scores(q[BLOCK:], k[BLOCK:]), 0.0)
        high = jnp.concatenate([back, diag], 1).astype(jnp.bfloat16)
        first = jnp.dot(low, v[:BLOCK], preferred_element_type=jnp.float32)
        second = jnp.dot(high, v, preferred_element_type=jnp.float32)
        return u, jnp.concatenate([first, second], 0) * (1.0 / WIN)

    def send_copy(s, q):
        src, j = source(s)
        pair = src * per_pair + j
        return pltpu.make_async_remote_copy(
            src_ref=send.at[s, q], dst_ref=arr.at[pl.ds(MAXB * pair, MAXB)],
            send_sem=send_sem.at[s, q], recv_sem=recv_sem.at[pair],
            device_id={"mp": q}, device_id_type=MESH,
        )

    def send_local(s, q, pair):
        return pltpu.make_async_copy(
            send.at[s, q], arr.at[pl.ds(MAXB * pair, MAXB)], recv_sem.at[pair]
        )

    def state_copy(s, q):
        src, j = source(s)
        pair = d * per_pair + j
        return pltpu.make_async_remote_copy(
            src_ref=state_out.at[s, q], dst_ref=state_in.at[pair], send_sem=state_send.at[s, q],
            recv_sem=state_recv.at[pair], device_id={"dp": src, "mp": q}, device_id_type=MESH,
        )

    def state_local(s, q, pair):
        return pltpu.make_async_copy(state_out.at[s, q], state_in.at[pair], state_recv.at[pair])

    def home_copy(h, i):
        o, j = home_target(h)
        pair = d * per_pair + j
        return pltpu.make_async_remote_copy(
            src_ref=send_home.at[h, i], dst_ref=arr.at[pl.ds(MAXB * pair, MAXB)],
            send_sem=send_home_sem.at[h, i], recv_sem=recv_sem.at[pair],
            device_id={"dp": o, "mp": first_q + i}, device_id_type=MESH,
        )

    def home_local(h, i):
        pair = d * per_pair + home_target(h)[1]
        return pltpu.make_async_copy(
            send_home.at[h, i], arr.at[pl.ds(MAXB * pair, MAXB)], recv_sem.at[pair]
        )

    def home_state_copy(h, i):
        o, j = home_target(h)
        pair = o * per_pair + j
        return pltpu.make_async_remote_copy(
            src_ref=state_home.at[h, i], dst_ref=state_in.at[pair],
            send_sem=state_home_sem.at[h, i], recv_sem=state_recv.at[pair],
            device_id={"mp": first_q + i}, device_id_type=MESH,
        )

    def home_state_local(h, i):
        o, j = home_target(h)
        pair = o * per_pair + j
        return pltpu.make_async_copy(
            state_home.at[h, i], state_in.at[pair], state_recv.at[pair]
        )

    picks = lax.broadcasted_iota(jnp.int32, (8, WIN), 1)

    def finish(parts, x, weight, length, out, chosen):
        a = jnp.concatenate([part[1] for part in parts], 1)
        g = jnp.concatenate([part[0] for part in parts], 1).astype(jnp.float32)
        gated = (norm_rows(a) * g).astype(jnp.bfloat16)
        y = jnp.dot(gated, weight, preferred_element_type=jnp.float32)
        positions = lax.broadcasted_iota(jnp.int32, y.shape, 0)
        y = jnp.where(positions < length, y + x, 0.0).astype(jnp.bfloat16)
        pick = jnp.where(picks == length - 1, 1.0, 0.0).astype(jnp.bfloat16)
        row = jnp.dot(pick, y, preferred_element_type=jnp.float32)
        for i in range(y.shape[1] // quarter):
            out[i] = y[:, i * quarter : (i + 1) * quarter].reshape(MAXB, BLOCK, quarter)
            chosen[i] = row[:, i * quarter : (i + 1) * quarter]

    half = mp_size // 2

    def near_heads(h, carry):
        x = rows_home[h].reshape(WIN, D).astype(jnp.float32)
        n = norm_rows(x).astype(jnp.bfloat16)
        normed[h] = n
        parts = [one_head(n, bits) for bits in range(half)]
        gate[h] = jnp.concatenate([part[0] for part in parts], 1)
        att[h] = jnp.concatenate([part[1] for part in parts], 1)
        return carry

    def far_heads(i, carry):
        late = i // homes
        h = i - late * homes
        o, j = home_target(h)

        @pl.when(crosses(o) == (late == 0))
        def _():
            u, valid = user_of(o, j)
            length = jnp.where(valid, len_s[0, u], 0)
            n = normed[h]
            parts = [(gate[h], att[h])]
            parts += [one_head(n, bits) for bits in range(half, mp_size)]
            x = rows_home[h, :, :, pl.ds(pl.multiple_of(first_q * quarter, side), side)]
            x = x.reshape(WIN, side).astype(jnp.float32)
            finish(parts, x, wop_side[...], length, send_home.at[h], state_home.at[h])
            for i in range(2):
                @pl.when(first_q + i != m)
                def _():
                    home_state_copy(h, i).start()

                @pl.when(first_q + i == m)
                def _():
                    home_state_local(h, i).start()

            for i in range(2):
                own = jnp.logical_and(o == d, first_q + i == m)

                @pl.when(jnp.logical_not(own))
                def _():
                    home_copy(h, i).start()

                @pl.when(own)
                def _():
                    home_local(h, i).start()

        return carry

    def moved_user(i, carry):
        late = i // slots
        s = i - late * slots
        src, j = source(s)

        @pl.when(crosses(src) == (late == 1))
        def _():
            row_local(s).wait()
            x = rows_in[s].reshape(WIN, D).astype(jnp.float32)
            n = norm_rows(x).astype(jnp.bfloat16)
            parts = [one_head(n, bits) for bits in range(mp_size)]
            finish(parts, x, wop[...], meta_s[src, 0, 2 * j], send.at[s], state_out.at[s])
            for q in range(mp_size):
                own = jnp.logical_and(src == d, q == m)

                @pl.when(jnp.logical_not(own))
                def _():
                    state_copy(s, q).start()

                @pl.when(own)
                def _():
                    state_local(s, q, d * per_pair + j).start()

            for q in range(mp_size):
                @pl.when(q != m)
                def _():
                    send_copy(s, q).start()

                @pl.when(q == m)
                def _():
                    send_local(s, q, src * per_pair + j).start()

        return carry

    def got_meta(step, carry):
        src = lax.rem(d + step, dp_size)
        pltpu.make_async_copy(meta_my.at[src], meta_in.at[src], meta_recv.at[src]).wait()
        return carry

    def read_meta():
        lax.fori_loop(1, dp_size, got_meta, 0)
        to_smem = pltpu.make_async_copy(meta_in, meta_s, local_sem)
        to_smem.start()
        to_smem.wait()

        def invert(i, row):
            src = i // per_pair
            j = i - src * per_pair
            length = meta_s[src, 0, 2 * j]
            offset = meta_s[src, 0, 2 * j + 1]
            for b in range(MAXB):
                at = jnp.where(length > b * BLOCK, offset + b, -1)
                row = jnp.where(lanes == at, MAXB * i + b, row)
            return row

        inv_v[...] = lax.fori_loop(
            0, pairs, invert, jnp.full((1, 128), zero_block, jnp.int32)
        )
        back = pltpu.make_async_copy(inv_v, inv_s, local_sem)
        back.start()
        back.wait()

    for copy in near:
        copy.wait()
    if homes:
        lax.fori_loop(0, homes, near_heads, 0)
    for c in range(CHUNKS):
        far[c].wait()
        relay[c].start()
    read_meta()
    for copy in wop_copies:
        copy.wait()
    for c in range(CHUNKS):
        relay[c].wait()
    if homes:
        lax.fori_loop(0, 2 * homes, far_heads, 0)
    lax.fori_loop(0, 2 * slots, moved_user, 0)

    def end_meta(step, carry):
        meta_copy(step).wait_send()
        return carry

    lax.fori_loop(1, dp_size, end_meta, 0)

    def end_rows(s, carry):
        @pl.when(target(s)[0] != d)
        def _():
            row_copy(s).wait_send()

        return carry

    lax.fori_loop(0, slots, end_rows, 0)

    def sent(s, carry):
        src, _ = source(s)
        for q in range(mp_size):
            @pl.when(q != m)
            def _():
                send_copy(s, q).wait_send()

            @pl.when(jnp.logical_not(jnp.logical_and(src == d, q == m)))
            def _():
                state_copy(s, q).wait_send()

        return carry

    lax.fori_loop(0, slots, sent, 0)

    def home_sent(h, carry):
        o, _ = home_target(h)
        for i in range(2):
            @pl.when(first_q + i != m)
            def _():
                home_state_copy(h, i).wait_send()

            @pl.when(jnp.logical_not(jnp.logical_and(o == d, first_q + i == m)))
            def _():
                home_copy(h, i).wait_send()

        return carry

    if homes:
        lax.fori_loop(0, homes, home_sent, 0)

    def got_state(i, carry):
        state_local(0, 0, i).wait()
        return carry

    lax.fori_loop(0, pairs, got_state, 0)

    def pick_state(u, carry):
        at = owner_s[0, u] * per_pair + u // dp_size
        state32[pl.ds(u, 1), :] = state_in[at, 0:1, :]
        return carry

    lax.fori_loop(0, user_count, pick_state, 0)
    state[...] = state32[...].astype(state.dtype)

    def got(i, carry):
        send_local(0, 0, i).wait()
        return carry

    lax.fori_loop(0, pairs, got, 0)


def place_kernel(arr, inv, state_in, packed, state, out_sem, state_sem):
    blocks = packed.shape[0]

    def put(b, carry):
        pltpu.make_async_copy(arr.at[inv[0, b]], packed.at[b], out_sem).start()
        return carry

    lax.fori_loop(0, blocks, put, 0, unroll=8)
    out = pltpu.make_async_copy(state_in, state, state_sem)
    out.start()
    pltpu.make_async_copy(arr.at[pl.ds(0, blocks)], packed, out_sem).wait()
    out.wait()


def per_device(tokens, w_uvqk, w_out, hist_len, owner, recv_offset, block_start):
    dp_size = lax.axis_size("dp")
    mp_size = lax.axis_size("mp")
    user_count = hist_len.shape[1]
    per_pair = -(-user_count // dp_size)
    pairs = dp_size * per_pair
    reach = dp_size // mp_size
    moving = (2 * per_pair + 2) // 3
    slots = reach * moving
    homes = max(2 * reach * (per_pair - moving), 1)
    quarter = D // mp_size
    rows = tokens.shape[0]
    blocks = rows // BLOCK

    vmem = pl.BlockSpec(memory_space=pltpu.VMEM)
    smem = pl.BlockSpec(memory_space=pltpu.SMEM)
    anywhere = pl.BlockSpec(memory_space=pltpu.HBM)
    bf16, f32, i32 = jnp.bfloat16, jnp.float32, jnp.int32
    dma = pltpu.SemaphoreType.DMA
    arr, inv, state_rows = pl.pallas_call(
        functools.partial(layer_kernel, dp_size, mp_size, per_pair, moving, user_count),
        out_shape=(
            pltpu.VMEM((MAXB * pairs + 1, BLOCK, quarter), bf16),
            pltpu.SMEM((1, 128), i32),
            pltpu.VMEM((user_count, quarter), bf16),
        ),
        in_specs=[anywhere] * 7,
        out_specs=(vmem, smem, vmem),
        scratch_shapes=[
            pltpu.VMEM((blocks, BLOCK, D), bf16),
            pltpu.VMEM((slots, MAXB, BLOCK, D), bf16),
            pltpu.VMEM((slots, MAXB, BLOCK, D), bf16),
            pltpu.VMEM((homes, MAXB, BLOCK, D), bf16),
            pltpu.VMEM((mp_size, D, 4 * HEAD), bf16),
            pltpu.VMEM((D, D), bf16),
            pltpu.VMEM((D, D // 2), bf16),
            pltpu.VMEM((slots, mp_size, MAXB, BLOCK, quarter), bf16),
            pltpu.VMEM((slots, mp_size, 8, quarter), f32),
            pltpu.VMEM((homes, 2, MAXB, BLOCK, quarter), bf16),
            pltpu.VMEM((homes, 2, 8, quarter), f32),
            pltpu.VMEM((pairs, 8, quarter), f32),
            pltpu.VMEM((user_count, quarter), f32),
            pltpu.VMEM((dp_size, 1, 128), i32),
            pltpu.VMEM((dp_size, 1, 128), i32),
            pltpu.VMEM((1, 128), i32),
            pltpu.VMEM((homes, WIN, D), bf16),
            pltpu.VMEM((homes, WIN, D // 2), bf16),
            pltpu.VMEM((homes, WIN, D // 2), f32),
            pltpu.SMEM((1, user_count), i32),
            pltpu.SMEM((1, user_count), i32),
            pltpu.SMEM((1, user_count), i32),
            pltpu.SMEM((1, user_count), i32),
            pltpu.SMEM((dp_size, 1, 128), i32),
            dma((4,)),
            dma,
            dma,
            dma((mp_size,)),
            dma((mp_size,)),
            dma((3, CHUNKS)),
            dma((3, CHUNKS)),
            dma((dp_size,)),
            dma((dp_size,)),
            dma((slots,)),
            dma((slots,)),
            dma((slots, mp_size)),
            dma((pairs,)),
            dma((slots, mp_size)),
            dma((pairs,)),
            dma((homes, 2)),
            dma((homes, 2)),
            dma,
        ],
        compiler_params=pltpu.CompilerParams(
            collective_id=0, has_side_effects=True, vmem_limit_bytes=48 * 1024 * 1024
        ),
        name="layer",
    )(
        *(
            pltpu.with_memory_space_constraint(a, pltpu.HBM)
            for a in (
                tokens.reshape(blocks, BLOCK, D), w_uvqk, w_out,
                owner, hist_len, recv_offset, block_start,
            )
        )
    )
    packed, state = pl.pallas_call(
        place_kernel,
        out_shape=(
            jax.ShapeDtypeStruct((blocks, BLOCK, quarter), bf16),
            jax.ShapeDtypeStruct((user_count, quarter), bf16),
        ),
        in_specs=[vmem, smem, vmem],
        out_specs=(anywhere, anywhere),
        scratch_shapes=[dma, dma],
        compiler_params=pltpu.CompilerParams(vmem_limit_bytes=4 * 1024 * 1024),
        name="place",
    )(
        pltpu.with_memory_space_constraint(arr, pltpu.VMEM),
        pltpu.with_memory_space_constraint(inv, pltpu.SMEM),
        pltpu.with_memory_space_constraint(state_rows, pltpu.VMEM),
    )
    return packed.reshape(rows, quarter), state


def solution(mesh):
    in_specs = (
        P("dp", None),
        P(None, "mp"),
        P(),
        P("dp", None),
        P("dp", None),
        P("dp", None),
        P("dp", None),
    )
    out_specs = (P("dp", "mp"), P("dp", "mp"))
    return jax.shard_map(
        per_device, mesh=mesh, in_specs=in_specs, out_specs=out_specs, check_vma=False
    )
```

```python
import functools

import jax
import jax.numpy as jnp
from jax import lax
from jax.experimental import pallas as pl
from jax.experimental.pallas import tpu as pltpu
from jax.sharding import PartitionSpec as P

D = 512
HEADS = 4
HEAD = D // HEADS
BLOCK = 128
MAXB = 2
WIN = MAXB * BLOCK
EPS = 1e-05
CHUNKS = 4
MESH = pl.DeviceIdType.MESH


def norm_rows(values):
    average = jnp.mean(values, axis=-1, keepdims=True)
    variance = jnp.mean(values * values, axis=-1, keepdims=True) - average * average
    return (values - average) * lax.rsqrt(variance + EPS)


def layer_kernel(
    dp_size, mp_size, per_pair, moving, user_count,
    tok_hbm, w_hbm, wout_hbm, owner_hbm, len_hbm, off_hbm, start_hbm,
    arr, inv_s, state,
    tok, rows_out, rows_in, rows_home, wg, wop, wop_side, send, state_out, send_home, state_home,
    state_in, state32, meta_my, meta_in, inv_v, normed, gate, att,
    owner_s, len_s, off_s, start_s, meta_s,
    tab_sem, tok_sem, w_sem, wop_sem, side_sem, w_send, w_recv, meta_send, meta_recv, row_send, row_recv,
    send_sem, recv_sem, state_send, state_recv, send_home_sem, state_home_sem, local_sem, group_sem,
):
    d = lax.axis_index("dp")
    m = lax.axis_index("mp")
    quarter = D // mp_size
    reach = dp_size // mp_size
    staying = per_pair - moving
    slots = reach * moving
    homes = 2 * reach * staying
    pairs = dp_size * per_pair
    side = D // 2
    first_q = m // 2 * 2
    last_block = tok_hbm.shape[0] - 1
    barrier = pltpu.get_barrier_semaphore()

    tok_copy = pltpu.make_async_copy(tok_hbm, tok, tok_sem)
    tok_copy.start()

    for step in range(dp_size - 1, 0, -1):
        pl.semaphore_signal(
            barrier, inc=1, device_id={"dp": lax.rem(d + step, dp_size)}, device_id_type=MESH
        )
    for step in range(1, mp_size):
        pl.semaphore_signal(
            barrier, inc=1, device_id={"mp": lax.rem(m + step, mp_size)}, device_id_type=MESH
        )
    tables = [
        pltpu.make_async_copy(src, dst, tab_sem.at[i])
        for i, (src, dst) in enumerate(
            ((owner_hbm, owner_s), (start_hbm, start_s), (len_hbm, len_s), (off_hbm, off_s))
        )
    ]
    for table in tables:
        table.start()
    own_w = pltpu.make_async_copy(w_hbm, wg.at[0], w_sem)
    own_w.start()

    def flip(bits):
        if bits == 1:
            return m + 1 - 2 * lax.rem(m, 2)
        return lax.rem(m + 2, 4)

    wop_copies = []
    for bits in range(mp_size):
        head = m
        if bits & 1:
            head = head + 1 - 2 * lax.rem(head, 2)
        if bits & 2:
            head = lax.rem(head + 2, 4)
        copy = pltpu.make_async_copy(
            wout_hbm.at[pl.ds(pl.multiple_of(head * HEAD, HEAD), HEAD)],
            wop.at[pl.ds(bits * HEAD, HEAD)], wop_sem.at[bits],
        )
        copy.start()
        wop_copies.append(copy)
        if homes:
            copy = pltpu.make_async_copy(
                wout_hbm.at[
                    pl.ds(pl.multiple_of(head * HEAD, HEAD), HEAD),
                    pl.ds(pl.multiple_of(first_q * quarter, side), side),
                ],
                wop_side.at[pl.ds(bits * HEAD, HEAD)], side_sem.at[bits],
            )
            copy.start()
            wop_copies.append(copy)

    def target(s):
        k = s // moving
        return lax.rem(d + m + mp_size * k, dp_size), s - k * moving

    def source(s):
        k = s // moving
        return lax.rem(d - m - mp_size * k + 2 * dp_size, dp_size), s - k * moving

    def home_target(h):
        g = h // (reach * staying)
        r = h - g * (reach * staying)
        k = r // staying
        group = lax.rem(m + 2 * g, mp_size)
        return lax.rem(d + group + mp_size * k, dp_size), moving + r - k * staying

    def crosses(o):
        return (o < dp_size // 2) != (d < dp_size // 2)

    def find(o):
        first = 0
        found = 0
        for u in range(min(dp_size, user_count)):
            hit = owner_s[0, u] == o
            first = jnp.where(hit, u, first)
            found = jnp.where(hit, 1, found)
        return first, found

    def user_of(o, j):
        first, found = find(o)
        u = first + j * dp_size
        valid = jnp.logical_and(found == 1, u < user_count)
        return jnp.minimum(u, user_count - 1), valid

    for table in tables:
        table.wait()

    lanes = lax.broadcasted_iota(jnp.int32, (1, 128), 1)

    def fill_meta(o, carry):
        first, found = find(o)
        row = jnp.zeros((1, 128), jnp.int32)
        for j in range(per_pair):
            u = first + j * dp_size
            valid = jnp.logical_and(found == 1, u < user_count)
            u = jnp.minimum(u, user_count - 1)
            row = jnp.where(lanes == 2 * j, jnp.where(valid, len_s[0, u], 0), row)
            row = jnp.where(lanes == 2 * j + 1, off_s[0, u], row)
        meta_my[o] = row
        return carry

    lax.fori_loop(0, dp_size, fill_meta, 0)
    meta_in[d] = meta_my[d]
    zero_block = 2 * pairs
    arr[zero_block] = jnp.zeros((BLOCK, quarter), arr.dtype)
    def stage(o, j, into):
        u, _ = user_of(o, j)
        start = start_s[0, u]
        for b in range(MAXB):
            into[b] = tok[jnp.minimum(start + b, last_block)]

    def stage_home(h, carry):
        o, j = home_target(h)
        stage(o, j, rows_home.at[h])
        return carry

    own_w.wait()
    pl.semaphore_wait(barrier, dp_size + mp_size - 2)
    for step in range(1, mp_size):
        pl.semaphore_signal(
            group_sem, inc=1, device_id={"mp": lax.rem(m + step, mp_size)}, device_id_type=MESH
        )

    def meta_copy(step):
        o = lax.rem(d + step, dp_size)
        return pltpu.make_async_remote_copy(
            src_ref=meta_my.at[o], dst_ref=meta_in.at[d], send_sem=meta_send.at[step],
            recv_sem=meta_recv.at[d], device_id={"dp": o}, device_id_type=MESH,
        )

    def start_meta(step, carry):
        meta_copy(step).start()
        return carry

    lax.fori_loop(1, dp_size, start_meta, 0)

    def row_copy(s):
        return pltpu.make_async_remote_copy(
            src_ref=rows_out.at[s], dst_ref=rows_in.at[s], send_sem=row_send.at[s],
            recv_sem=row_recv.at[s], device_id={"dp": target(s)[0]}, device_id_type=MESH,
        )

    def row_local(s):
        return pltpu.make_async_copy(rows_out.at[s], rows_in.at[s], row_recv.at[s])

    piece = D // CHUNKS

    def w_copy(src, dst, chunk, peer, index):
        rows = pl.ds(chunk * piece, piece)
        return pltpu.make_async_remote_copy(
            src_ref=wg.at[src, rows], dst_ref=wg.at[dst, rows], send_sem=w_send.at[index, chunk],
            recv_sem=w_recv.at[index, chunk], device_id={"mp": peer}, device_id_type=MESH,
        )

    far = [w_copy(0, 2, c, flip(2), 1) for c in range(CHUNKS)]
    near = [w_copy(0, 1, c, flip(1), 0) for c in range(CHUNKS)]
    relay = [w_copy(2, 3, c, flip(1), 2) for c in range(CHUNKS)]
    for copy in far:
        copy.start()
    for copy in near:
        copy.start()

    tok_copy.wait()

    def stage_rows(i, carry):
        late = i // slots
        s = i - late * slots
        o, j = target(s)

        @pl.when(crosses(o) == (late == 0))
        def _():
            stage(o, j, rows_out.at[s])

        return carry

    def start_rows(i, carry):
        late = i // slots
        s = i - late * slots
        o, _ = target(s)
        now = crosses(o) == (late == 0)

        @pl.when(jnp.logical_and(now, o != d))
        def _():
            row_copy(s).start()

        @pl.when(jnp.logical_and(now, o == d))
        def _():
            row_local(s).start()

        return carry

    lax.fori_loop(0, slots, stage_rows, 0)
    lax.fori_loop(0, slots, start_rows, 0)
    lax.fori_loop(slots, 2 * slots, stage_rows, 0)
    lax.fori_loop(slots, 2 * slots, start_rows, 0)
    lax.fori_loop(0, homes, stage_home, 0)

    causal = lax.broadcasted_iota(jnp.int32, (BLOCK, BLOCK), 1) <= lax.broadcasted_iota(
        jnp.int32, (BLOCK, BLOCK), 0
    )
    half_scale = 0.5 * HEAD ** (-0.5)

    def scores(q, k):
        t = lax.dot_general(
            q, k, (((1,), (1,)), ((), ())), preferred_element_type=jnp.float32
        ) * half_scale
        return t + t * jnp.tanh(t)

    def one_head(rows_in, bits):
        h = jnp.dot(rows_in, wg[bits], preferred_element_type=jnp.float32) * 0.5
        p = (h + h * jnp.tanh(h)).astype(jnp.bfloat16)
        u, v, q, k = (p[:, i * HEAD : (i + 1) * HEAD] for i in range(4))
        low = jnp.where(causal, scores(q[:BLOCK], k[:BLOCK]), 0.0).astype(jnp.bfloat16)
        back = scores(q[BLOCK:], k[:BLOCK])
        diag = jnp.where(causal, scores(q[BLOCK:], k[BLOCK:]), 0.0)
        high = jnp.concatenate([back, diag], 1).astype(jnp.bfloat16)
        first = jnp.dot(low, v[:BLOCK], preferred_element_type=jnp.float32)
        second = jnp.dot(high, v, preferred_element_type=jnp.float32)
        return u, jnp.concatenate([first, second], 0) * (1.0 / WIN)

    def send_copy(s, q):
        src, j = source(s)
        pair = src * per_pair + j
        return pltpu.make_async_remote_copy(
            src_ref=send.at[s, q], dst_ref=arr.at[pl.ds(MAXB * pair, MAXB)],
            send_sem=send_sem.at[s, q], recv_sem=recv_sem,
            device_id={"mp": q}, device_id_type=MESH,
        )

    def send_local(s, q, pair):
        return pltpu.make_async_copy(
            send.at[s, q], arr.at[pl.ds(MAXB * pair, MAXB)], recv_sem
        )

    def state_copy(s, q):
        src, j = source(s)
        pair = d * per_pair + j
        return pltpu.make_async_remote_copy(
            src_ref=state_out.at[s, q], dst_ref=state_in.at[pair], send_sem=state_send.at[s, q],
            recv_sem=state_recv, device_id={"dp": src, "mp": q}, device_id_type=MESH,
        )

    def state_local(s, q, pair):
        return pltpu.make_async_copy(state_out.at[s, q], state_in.at[pair], state_recv)

    def home_copy(h, i):
        o, j = home_target(h)
        pair = d * per_pair + j
        return pltpu.make_async_remote_copy(
            src_ref=send_home.at[h, i], dst_ref=arr.at[pl.ds(MAXB * pair, MAXB)],
            send_sem=send_home_sem.at[h, i], recv_sem=recv_sem,
            device_id={"dp": o, "mp": first_q + i}, device_id_type=MESH,
        )

    def home_local(h, i):
        pair = d * per_pair + home_target(h)[1]
        return pltpu.make_async_copy(
            send_home.at[h, i], arr.at[pl.ds(MAXB * pair, MAXB)], recv_sem
        )

    def home_state_copy(h, i):
        o, j = home_target(h)
        pair = o * per_pair + j
        return pltpu.make_async_remote_copy(
            src_ref=state_home.at[h, i], dst_ref=state_in.at[pair],
            send_sem=state_home_sem.at[h, i], recv_sem=state_recv,
            device_id={"mp": first_q + i}, device_id_type=MESH,
        )

    def home_state_local(h, i):
        o, j = home_target(h)
        pair = o * per_pair + j
        return pltpu.make_async_copy(
            state_home.at[h, i], state_in.at[pair], state_recv
        )

    picks = lax.broadcasted_iota(jnp.int32, (8, WIN), 1)

    def finish(parts, x, weight, length, out, chosen):
        a = jnp.concatenate([part[1] for part in parts], 1)
        g = jnp.concatenate([part[0] for part in parts], 1).astype(jnp.float32)
        gated = (norm_rows(a) * g).astype(jnp.bfloat16)
        y = jnp.dot(gated, weight, preferred_element_type=jnp.float32)
        positions = lax.broadcasted_iota(jnp.int32, y.shape, 0)
        y = jnp.where(positions < length, y + x, 0.0).astype(jnp.bfloat16)
        pick = jnp.where(picks == length - 1, 1.0, 0.0).astype(jnp.bfloat16)
        row = jnp.dot(pick, y, preferred_element_type=jnp.float32)
        for i in range(y.shape[1] // quarter):
            out[i] = y[:, i * quarter : (i + 1) * quarter].reshape(MAXB, BLOCK, quarter)
            chosen[i] = row[:, i * quarter : (i + 1) * quarter]

    half = mp_size // 2

    def near_heads(h, carry):
        x = rows_home[h].reshape(WIN, D).astype(jnp.float32)
        n = norm_rows(x).astype(jnp.bfloat16)
        normed[h] = n
        parts = [one_head(n, bits) for bits in range(half)]
        gate[h] = jnp.concatenate([part[0] for part in parts], 1)
        att[h] = jnp.concatenate([part[1] for part in parts], 1)
        return carry

    def far_heads(i, carry):
        late = i // homes
        h = i - late * homes
        o, j = home_target(h)

        @pl.when(crosses(o) == (late == 0))
        def _():
            u, valid = user_of(o, j)
            length = jnp.where(valid, len_s[0, u], 0)
            n = normed[h]
            parts = [(gate[h], att[h])]
            parts += [one_head(n, bits) for bits in range(half, mp_size)]
            x = rows_home[h, :, :, pl.ds(pl.multiple_of(first_q * quarter, side), side)]
            x = x.reshape(WIN, side).astype(jnp.float32)
            finish(parts, x, wop_side[...], length, send_home.at[h], state_home.at[h])
            for i in range(2):
                @pl.when(first_q + i != m)
                def _():
                    home_state_copy(h, i).start()

                @pl.when(first_q + i == m)
                def _():
                    home_state_local(h, i).start()

            for i in range(2):
                own = jnp.logical_and(o == d, first_q + i == m)

                @pl.when(jnp.logical_not(own))
                def _():
                    home_copy(h, i).start()

                @pl.when(own)
                def _():
                    home_local(h, i).start()

        return carry

    def moved_user(i, carry):
        late = i // slots
        s = i - late * slots
        src, j = source(s)

        @pl.when(crosses(src) == (late == 1))
        def _():
            row_local(s).wait()
            x = rows_in[s].reshape(WIN, D).astype(jnp.float32)
            n = norm_rows(x).astype(jnp.bfloat16)
            parts = [one_head(n, bits) for bits in range(mp_size)]
            finish(parts, x, wop[...], meta_s[src, 0, 2 * j], send.at[s], state_out.at[s])
            for q in range(mp_size):
                own = jnp.logical_and(src == d, q == m)

                @pl.when(jnp.logical_not(own))
                def _():
                    state_copy(s, q).start()

                @pl.when(own)
                def _():
                    state_local(s, q, d * per_pair + j).start()

            for q in range(mp_size):
                @pl.when(q != m)
                def _():
                    send_copy(s, q).start()

                @pl.when(q == m)
                def _():
                    send_local(s, q, src * per_pair + j).start()

        return carry

    def got_meta(step, carry):
        src = lax.rem(d + step, dp_size)
        pltpu.make_async_copy(meta_my.at[src], meta_in.at[src], meta_recv.at[src]).wait()
        return carry

    def read_meta():
        lax.fori_loop(1, dp_size, got_meta, 0)
        to_smem = pltpu.make_async_copy(meta_in, meta_s, local_sem)
        to_smem.start()
        to_smem.wait()

        def invert(i, row):
            src = i // per_pair
            j = i - src * per_pair
            length = meta_s[src, 0, 2 * j]
            offset = meta_s[src, 0, 2 * j + 1]
            for b in range(MAXB):
                at = jnp.where(length > b * BLOCK, offset + b, -1)
                row = jnp.where(lanes == at, MAXB * i + b, row)
            return row

        inv_v[...] = lax.fori_loop(
            0, pairs, invert, jnp.full((1, 128), zero_block, jnp.int32)
        )
        back = pltpu.make_async_copy(inv_v, inv_s, local_sem)
        back.start()
        back.wait()

    for copy in near:
        copy.wait()
    if homes:
        lax.fori_loop(0, homes, near_heads, 0)
    for c in range(CHUNKS):
        far[c].wait()
        relay[c].start()
    read_meta()
    for copy in wop_copies:
        copy.wait()
    for c in range(CHUNKS):
        relay[c].wait()
    pl.semaphore_wait(group_sem, mp_size - 1)
    if homes:
        lax.fori_loop(0, 2 * homes, far_heads, 0)
    lax.fori_loop(0, 2 * slots, moved_user, 0)

    def end_meta(step, carry):
        meta_copy(step).wait_send()
        return carry

    lax.fori_loop(1, dp_size, end_meta, 0)

    def end_rows(s, carry):
        @pl.when(target(s)[0] != d)
        def _():
            row_copy(s).wait_send()

        return carry

    lax.fori_loop(0, slots, end_rows, 0)

    def sent(s, carry):
        src, _ = source(s)
        for q in range(mp_size):
            @pl.when(q != m)
            def _():
                send_copy(s, q).wait_send()

            @pl.when(jnp.logical_not(jnp.logical_and(src == d, q == m)))
            def _():
                state_copy(s, q).wait_send()

        return carry

    lax.fori_loop(0, slots, sent, 0)

    def home_sent(h, carry):
        o, _ = home_target(h)
        for i in range(2):
            @pl.when(first_q + i != m)
            def _():
                home_state_copy(h, i).wait_send()

            @pl.when(jnp.logical_not(jnp.logical_and(o == d, first_q + i == m)))
            def _():
                home_copy(h, i).wait_send()

        return carry

    if homes:
        lax.fori_loop(0, homes, home_sent, 0)

    pltpu.make_async_copy(state_in, state_in, state_recv).wait()

    def pick_state(u, carry):
        at = owner_s[0, u] * per_pair + u // dp_size
        state32[pl.ds(u, 1), :] = state_in[at, 0:1, :]
        return carry

    lax.fori_loop(0, user_count, pick_state, 0)
    state[...] = state32[...].astype(state.dtype)

    every = arr.at[pl.ds(0, MAXB * pairs)]
    pltpu.make_async_copy(every, every, recv_sem).wait()


def place_kernel(arr, inv, state_in, packed, state, out_sem, state_sem):
    blocks = packed.shape[0]

    def put(b, carry):
        pltpu.make_async_copy(arr.at[inv[0, b]], packed.at[b], out_sem).start()
        return carry

    lax.fori_loop(0, blocks, put, 0, unroll=8)
    out = pltpu.make_async_copy(state_in, state, state_sem)
    out.start()
    pltpu.make_async_copy(arr.at[pl.ds(0, blocks)], packed, out_sem).wait()
    out.wait()


def per_device(tokens, w_uvqk, w_out, hist_len, owner, recv_offset, block_start):
    dp_size = lax.axis_size("dp")
    mp_size = lax.axis_size("mp")
    user_count = hist_len.shape[1]
    per_pair = -(-user_count // dp_size)
    pairs = dp_size * per_pair
    reach = dp_size // mp_size
    moving = (2 * per_pair + 2) // 3
    slots = reach * moving
    homes = max(2 * reach * (per_pair - moving), 1)
    quarter = D // mp_size
    rows = tokens.shape[0]
    blocks = rows // BLOCK

    vmem = pl.BlockSpec(memory_space=pltpu.VMEM)
    smem = pl.BlockSpec(memory_space=pltpu.SMEM)
    anywhere = pl.BlockSpec(memory_space=pltpu.HBM)
    bf16, f32, i32 = jnp.bfloat16, jnp.float32, jnp.int32
    dma = pltpu.SemaphoreType.DMA
    arr, inv, state_rows = pl.pallas_call(
        functools.partial(layer_kernel, dp_size, mp_size, per_pair, moving, user_count),
        out_shape=(
            pltpu.VMEM((MAXB * pairs + 1, BLOCK, quarter), bf16),
            pltpu.SMEM((1, 128), i32),
            pltpu.VMEM((user_count, quarter), bf16),
        ),
        in_specs=[anywhere] * 7,
        out_specs=(vmem, smem, vmem),
        scratch_shapes=[
            pltpu.VMEM((blocks, BLOCK, D), bf16),
            pltpu.VMEM((slots, MAXB, BLOCK, D), bf16),
            pltpu.VMEM((slots, MAXB, BLOCK, D), bf16),
            pltpu.VMEM((homes, MAXB, BLOCK, D), bf16),
            pltpu.VMEM((mp_size, D, 4 * HEAD), bf16),
            pltpu.VMEM((D, D), bf16),
            pltpu.VMEM((D, D // 2), bf16),
            pltpu.VMEM((slots, mp_size, MAXB, BLOCK, quarter), bf16),
            pltpu.VMEM((slots, mp_size, 8, quarter), f32),
            pltpu.VMEM((homes, 2, MAXB, BLOCK, quarter), bf16),
            pltpu.VMEM((homes, 2, 8, quarter), f32),
            pltpu.VMEM((pairs, 8, quarter), f32),
            pltpu.VMEM((user_count, quarter), f32),
            pltpu.VMEM((dp_size, 1, 128), i32),
            pltpu.VMEM((dp_size, 1, 128), i32),
            pltpu.VMEM((1, 128), i32),
            pltpu.VMEM((homes, WIN, D), bf16),
            pltpu.VMEM((homes, WIN, D // 2), bf16),
            pltpu.VMEM((homes, WIN, D // 2), f32),
            pltpu.SMEM((1, user_count), i32),
            pltpu.SMEM((1, user_count), i32),
            pltpu.SMEM((1, user_count), i32),
            pltpu.SMEM((1, user_count), i32),
            pltpu.SMEM((dp_size, 1, 128), i32),
            dma((4,)),
            dma,
            dma,
            dma((mp_size,)),
            dma((mp_size,)),
            dma((3, CHUNKS)),
            dma((3, CHUNKS)),
            dma((dp_size,)),
            dma((dp_size,)),
            dma((slots,)),
            dma((slots,)),
            dma((slots, mp_size)),
            dma,
            dma((slots, mp_size)),
            dma,
            dma((homes, 2)),
            dma((homes, 2)),
            dma,
            pltpu.SemaphoreType.REGULAR,
        ],
        compiler_params=pltpu.CompilerParams(
            collective_id=0, has_side_effects=True, vmem_limit_bytes=48 * 1024 * 1024
        ),
        name="layer",
    )(
        *(
            pltpu.with_memory_space_constraint(a, pltpu.HBM)
            for a in (
                tokens.reshape(blocks, BLOCK, D), w_uvqk, w_out,
                owner, hist_len, recv_offset, block_start,
            )
        )
    )
    packed, state = pl.pallas_call(
        place_kernel,
        out_shape=(
            jax.ShapeDtypeStruct((blocks, BLOCK, quarter), bf16),
            jax.ShapeDtypeStruct((user_count, quarter), bf16),
        ),
        in_specs=[vmem, smem, vmem],
        out_specs=(anywhere, anywhere),
        scratch_shapes=[dma, dma],
        compiler_params=pltpu.CompilerParams(vmem_limit_bytes=4 * 1024 * 1024),
        name="place",
    )(
        pltpu.with_memory_space_constraint(arr, pltpu.VMEM),
        pltpu.with_memory_space_constraint(inv, pltpu.SMEM),
        pltpu.with_memory_space_constraint(state_rows, pltpu.VMEM),
    )
    return packed.reshape(rows, quarter), state


def solution(mesh):
    in_specs = (
        P("dp", None),
        P(None, "mp"),
        P(),
        P("dp", None),
        P("dp", None),
        P("dp", None),
        P("dp", None),
    )
    out_specs = (P("dp", "mp"), P("dp", "mp"))
    return jax.shard_map(
        per_device, mesh=mesh, in_specs=in_specs, out_specs=out_specs, check_vma=False
    )
```

```python
import functools

import jax
import jax.numpy as jnp
from jax import lax
from jax.experimental import pallas as pl
from jax.experimental.pallas import tpu as pltpu
from jax.sharding import PartitionSpec as P

D = 512
HEADS = 4
HEAD = D // HEADS
BLOCK = 128
MAXB = 2
WIN = MAXB * BLOCK
EPS = 1e-05
CHUNKS = 4
MESH = pl.DeviceIdType.MESH


def norm_rows(values):
    average = jnp.mean(values, axis=-1, keepdims=True)
    variance = jnp.mean(values * values, axis=-1, keepdims=True) - average * average
    return (values - average) * lax.rsqrt(variance + EPS)


def layer_kernel(
    dp_size, mp_size, per_pair, moving, user_count, bounds,
    tok_hbm, w_hbm, wout_hbm, owner_hbm, len_hbm, off_hbm, start_hbm,
    arr, inv_s, state,
    parts_of_tok, rows_out, rows_in, rows_home, wg, wop, wop_side, send, state_out, send_home, state_home,
    state_in, state32, meta_my, meta_in, inv_v, normed, gate, att,
    owner_s, len_s, off_s, start_s, meta_s,
    tab_sem, tok_sem, w_sem, wop_sem, side_sem, w_send, w_recv, meta_send, meta_recv, fwd_send, fwd_recv,
    row_send, row_recv,
    send_sem, recv_sem, state_send, state_recv, send_home_sem, state_home_sem, local_sem, line_sem, group_sem,
):
    d = lax.axis_index("dp")
    m = lax.axis_index("mp")
    quarter = D // mp_size
    reach = dp_size // mp_size
    staying = per_pair - moving
    slots = reach * moving
    homes = 2 * reach * staying
    pairs = dp_size * per_pair
    side = D // 2
    first_q = m // 2 * 2
    barrier = pltpu.get_barrier_semaphore()

    starts = (0,) + bounds[:-1]
    tok_copies = [
        pltpu.make_async_copy(
            tok_hbm.at[pl.ds(starts[p], bounds[p] - starts[p])], part, tok_sem.at[p]
        )
        for p, part in enumerate(parts_of_tok)
    ]
    tok_copies[0].start()

    def line_signal(semaphore):
        def tell(k, carry):
            ahead = m + mp_size * k
            ahead = jnp.where(ahead == 0, mp_size, ahead)
            for o in (d + ahead, d - ahead + dp_size):
                pl.semaphore_signal(
                    semaphore, inc=1, device_id={"dp": lax.rem(o, dp_size)}, device_id_type=MESH
                )
            return carry

        lax.fori_loop(0, reach, tell, 0)

    line_count = 2 * reach
    line_signal(barrier)
    for step in range(1, mp_size):
        pl.semaphore_signal(
            barrier, inc=1, device_id={"mp": lax.rem(m + step, mp_size)}, device_id_type=MESH
        )
    tables = [
        pltpu.make_async_copy(src, dst, tab_sem.at[i])
        for i, (src, dst) in enumerate(
            ((owner_hbm, owner_s), (start_hbm, start_s), (len_hbm, len_s), (off_hbm, off_s))
        )
    ]
    for table in tables:
        table.start()
    own_w = pltpu.make_async_copy(w_hbm, wg.at[0], w_sem)

    def flip(bits):
        if bits == 1:
            return m + 1 - 2 * lax.rem(m, 2)
        return lax.rem(m + 2, 4)

    wop_copies = []
    for bits in range(mp_size):
        head = m
        if bits & 1:
            head = head + 1 - 2 * lax.rem(head, 2)
        if bits & 2:
            head = lax.rem(head + 2, 4)
        copy = pltpu.make_async_copy(
            wout_hbm.at[pl.ds(pl.multiple_of(head * HEAD, HEAD), HEAD)],
            wop.at[pl.ds(bits * HEAD, HEAD)], wop_sem.at[bits],
        )
        wop_copies.append(copy)
        if homes:
            copy = pltpu.make_async_copy(
                wout_hbm.at[
                    pl.ds(pl.multiple_of(head * HEAD, HEAD), HEAD),
                    pl.ds(pl.multiple_of(first_q * quarter, side), side),
                ],
                wop_side.at[pl.ds(bits * HEAD, HEAD)], side_sem.at[bits],
            )
            wop_copies.append(copy)

    def target(s):
        k = s // moving
        return lax.rem(d + m + mp_size * k, dp_size), s - k * moving

    def source(s):
        k = s // moving
        return lax.rem(d - m - mp_size * k + 2 * dp_size, dp_size), s - k * moving

    def home_target(h):
        g = h // (reach * staying)
        r = h - g * (reach * staying)
        k = r // staying
        group = lax.rem(m + 2 * g, mp_size)
        return lax.rem(d + group + mp_size * k, dp_size), moving + r - k * staying

    def crosses(o):
        return (o < dp_size // 2) != (d < dp_size // 2)

    def find(o):
        first = 0
        found = 0
        for u in range(min(dp_size, user_count)):
            hit = owner_s[0, u] == o
            first = jnp.where(hit, u, first)
            found = jnp.where(hit, 1, found)
        return first, found

    def user_of(o, j):
        first, found = find(o)
        u = first + j * dp_size
        valid = jnp.logical_and(found == 1, u < user_count)
        return jnp.minimum(u, user_count - 1), valid

    for table in tables:
        table.wait()

    lanes = lax.broadcasted_iota(jnp.int32, (1, 128), 1)

    def fill_meta(k, carry):
        o = lax.rem(d + m + mp_size * k, dp_size)
        first, found = find(o)
        row = jnp.zeros((1, 128), jnp.int32)
        for j in range(per_pair):
            u = first + j * dp_size
            valid = jnp.logical_and(found == 1, u < user_count)
            u = jnp.minimum(u, user_count - 1)
            row = jnp.where(lanes == 2 * j, jnp.where(valid, len_s[0, u], 0), row)
            row = jnp.where(lanes == 2 * j + 1, off_s[0, u], row)
        meta_my[k] = row

        @pl.when(o == d)
        def _():
            meta_in[d] = row

        return carry

    lax.fori_loop(0, reach, fill_meta, 0)
    zero_block = 2 * pairs
    arr[zero_block] = jnp.zeros((BLOCK, quarter), arr.dtype)
    def stage(o, j, into):
        u, _ = user_of(o, j)
        start = start_s[0, u]
        for b in range(MAXB):
            at = jnp.minimum(start + b, bounds[j] - 1)
            value = parts_of_tok[0][jnp.minimum(at, bounds[0] - 1)]
            for p in range(1, j + 1):
                other = parts_of_tok[p][jnp.clip(at - starts[p], 0, bounds[p] - starts[p] - 1)]
                value = jnp.where(at >= starts[p], other, value)
            into[b] = value

    def stage_home(i, carry):
        for j in range(moving, per_pair):
            h = i * staying + j - moving
            stage(home_target(h)[0], j, rows_home.at[h])
        return carry

    def meta_copy(k):
        return pltpu.make_async_remote_copy(
            src_ref=meta_my.at[k], dst_ref=meta_in.at[d], send_sem=meta_send.at[k],
            recv_sem=meta_recv.at[k], device_id={"dp": lax.rem(d + m + mp_size * k, dp_size)},
            device_id_type=MESH,
        )

    def start_meta(k, carry):
        @pl.when(m + k != 0)
        def _():
            meta_copy(k).start()

        return carry

    def meta_from(lane, k):
        return lax.rem(d - lane - mp_size * k + 2 * dp_size, dp_size)

    def forward(k, step):
        row = meta_in.at[meta_from(m, k)]
        return pltpu.make_async_remote_copy(
            src_ref=row, dst_ref=row, send_sem=fwd_send.at[k, step],
            recv_sem=fwd_recv.at[k, m], device_id={"mp": lax.rem(m + step, mp_size)},
            device_id_type=MESH,
        )

    def forward_meta(k, carry):
        @pl.when(m + k != 0)
        def _():
            pltpu.make_async_copy(meta_my.at[k], meta_my.at[k], meta_recv.at[k]).wait()

        for step in range(1, mp_size):
            forward(k, step).start()
        return carry

    def row_copy(s):
        return pltpu.make_async_remote_copy(
            src_ref=rows_out.at[s], dst_ref=rows_in.at[s], send_sem=row_send.at[s],
            recv_sem=row_recv.at[s], device_id={"dp": target(s)[0]}, device_id_type=MESH,
        )

    def row_local(s):
        return pltpu.make_async_copy(rows_out.at[s], rows_in.at[s], row_recv.at[s])

    piece = D // CHUNKS

    def w_copy(src, dst, chunk, peer, index):
        rows = pl.ds(chunk * piece, piece)
        return pltpu.make_async_remote_copy(
            src_ref=wg.at[src, rows], dst_ref=wg.at[dst, rows], send_sem=w_send.at[index, chunk],
            recv_sem=w_recv.at[index, chunk], device_id={"mp": peer}, device_id_type=MESH,
        )

    far = [w_copy(0, 2, c, flip(2), 1) for c in range(CHUNKS)]
    near = [w_copy(0, 1, c, flip(1), 0) for c in range(CHUNKS)]
    relay = [w_copy(2, 3, c, flip(1), 2) for c in range(CHUNKS)]

    def stage_rows(i, carry, j):
        late = i // reach
        s = (i - late * reach) * moving + j
        o, _ = target(s)

        @pl.when(crosses(o) == (late == 0))
        def _():
            stage(o, j, rows_out.at[s])

        return carry

    def start_rows(i, carry, j):
        late = i // reach
        s = (i - late * reach) * moving + j
        o, _ = target(s)
        now = crosses(o) == (late == 0)

        @pl.when(jnp.logical_and(now, o != d))
        def _():
            row_copy(s).start()

        @pl.when(jnp.logical_and(now, o == d))
        def _():
            row_local(s).start()

        return carry

    tok_copies[0].wait()
    for copy in tok_copies[1:]:
        copy.start()
    own_w.start()
    lax.fori_loop(0, 2 * reach, functools.partial(stage_rows, j=0), 0)
    pl.semaphore_wait(barrier, line_count + mp_size - 1)
    lax.fori_loop(0, reach, start_meta, 0)
    lax.fori_loop(0, 2 * reach, functools.partial(start_rows, j=0), 0)
    line_signal(line_sem)
    own_w.wait()
    for copy in far:
        copy.start()
    for copy in near:
        copy.start()
    for j in range(1, moving):
        tok_copies[j].wait()
        lax.fori_loop(0, 2 * reach, functools.partial(stage_rows, j=j), 0)
        lax.fori_loop(0, 2 * reach, functools.partial(start_rows, j=j), 0)
    for copy in tok_copies[max(moving, 1):]:
        copy.wait()
    for copy in wop_copies:
        copy.start()
    lax.fori_loop(0, 2 * reach, stage_home, 0)
    pl.semaphore_wait(line_sem, line_count)
    for step in range(1, mp_size):
        pl.semaphore_signal(
            group_sem, inc=1, device_id={"mp": lax.rem(m + step, mp_size)}, device_id_type=MESH
        )
    lax.fori_loop(0, reach, forward_meta, 0)

    causal = lax.broadcasted_iota(jnp.int32, (BLOCK, BLOCK), 1) <= lax.broadcasted_iota(
        jnp.int32, (BLOCK, BLOCK), 0
    )
    half_scale = 0.5 * HEAD ** (-0.5)

    def scores(q, k):
        t = lax.dot_general(
            q, k, (((1,), (1,)), ((), ())), preferred_element_type=jnp.float32
        ) * half_scale
        return t + t * jnp.tanh(t)

    def one_head(rows_in, bits):
        h = jnp.dot(rows_in, wg[bits], preferred_element_type=jnp.float32) * 0.5
        p = (h + h * jnp.tanh(h)).astype(jnp.bfloat16)
        u, v, q, k = (p[:, i * HEAD : (i + 1) * HEAD] for i in range(4))
        low = jnp.where(causal, scores(q[:BLOCK], k[:BLOCK]), 0.0).astype(jnp.bfloat16)
        back = scores(q[BLOCK:], k[:BLOCK])
        diag = jnp.where(causal, scores(q[BLOCK:], k[BLOCK:]), 0.0)
        high = jnp.concatenate([back, diag], 1).astype(jnp.bfloat16)
        first = jnp.dot(low, v[:BLOCK], preferred_element_type=jnp.float32)
        second = jnp.dot(high, v, preferred_element_type=jnp.float32)
        return u, jnp.concatenate([first, second], 0) * (1.0 / WIN)

    def send_copy(s, q):
        src, j = source(s)
        pair = src * per_pair + j
        return pltpu.make_async_remote_copy(
            src_ref=send.at[s, q], dst_ref=arr.at[pl.ds(MAXB * pair, MAXB)],
            send_sem=send_sem.at[s, q], recv_sem=recv_sem,
            device_id={"mp": q}, device_id_type=MESH,
        )

    def send_local(s, q, pair):
        return pltpu.make_async_copy(
            send.at[s, q], arr.at[pl.ds(MAXB * pair, MAXB)], recv_sem
        )

    def state_copy(s, q):
        src, j = source(s)
        pair = d * per_pair + j
        return pltpu.make_async_remote_copy(
            src_ref=state_out.at[s, q], dst_ref=state_in.at[pair], send_sem=state_send.at[s, q],
            recv_sem=state_recv, device_id={"dp": src, "mp": q}, device_id_type=MESH,
        )

    def state_local(s, q, pair):
        return pltpu.make_async_copy(state_out.at[s, q], state_in.at[pair], state_recv)

    def home_copy(h, i):
        o, j = home_target(h)
        pair = d * per_pair + j
        return pltpu.make_async_remote_copy(
            src_ref=send_home.at[h, i], dst_ref=arr.at[pl.ds(MAXB * pair, MAXB)],
            send_sem=send_home_sem.at[h, i], recv_sem=recv_sem,
            device_id={"dp": o, "mp": first_q + i}, device_id_type=MESH,
        )

    def home_local(h, i):
        pair = d * per_pair + home_target(h)[1]
        return pltpu.make_async_copy(
            send_home.at[h, i], arr.at[pl.ds(MAXB * pair, MAXB)], recv_sem
        )

    def home_state_copy(h, i):
        o, j = home_target(h)
        pair = o * per_pair + j
        return pltpu.make_async_remote_copy(
            src_ref=state_home.at[h, i], dst_ref=state_in.at[pair],
            send_sem=state_home_sem.at[h, i], recv_sem=state_recv,
            device_id={"mp": first_q + i}, device_id_type=MESH,
        )

    def home_state_local(h, i):
        o, j = home_target(h)
        pair = o * per_pair + j
        return pltpu.make_async_copy(
            state_home.at[h, i], state_in.at[pair], state_recv
        )

    picks = lax.broadcasted_iota(jnp.int32, (8, WIN), 1)

    def finish(parts, x, weight, length, out, chosen):
        a = jnp.concatenate([part[1] for part in parts], 1)
        g = jnp.concatenate([part[0] for part in parts], 1).astype(jnp.float32)
        gated = (norm_rows(a) * g).astype(jnp.bfloat16)
        y = jnp.dot(gated, weight, preferred_element_type=jnp.float32)
        positions = lax.broadcasted_iota(jnp.int32, y.shape, 0)
        y = jnp.where(positions < length, y + x, 0.0).astype(jnp.bfloat16)
        pick = jnp.where(picks == length - 1, 1.0, 0.0).astype(jnp.bfloat16)
        row = jnp.dot(pick, y, preferred_element_type=jnp.float32)
        for i in range(y.shape[1] // quarter):
            out[i] = y[:, i * quarter : (i + 1) * quarter].reshape(MAXB, BLOCK, quarter)
            chosen[i] = row[:, i * quarter : (i + 1) * quarter]

    half = mp_size // 2

    def near_heads(h, carry):
        x = rows_home[h].reshape(WIN, D).astype(jnp.float32)
        n = norm_rows(x).astype(jnp.bfloat16)
        normed[h] = n
        parts = [one_head(n, bits) for bits in range(half)]
        gate[h] = jnp.concatenate([part[0] for part in parts], 1)
        att[h] = jnp.concatenate([part[1] for part in parts], 1)
        return carry

    def far_heads(i, carry):
        late = i // homes
        h = i - late * homes
        o, j = home_target(h)

        @pl.when(crosses(o) == (late == 0))
        def _():
            u, valid = user_of(o, j)
            length = jnp.where(valid, len_s[0, u], 0)
            n = normed[h]
            parts = [(gate[h], att[h])]
            parts += [one_head(n, bits) for bits in range(half, mp_size)]
            x = rows_home[h, :, :, pl.ds(pl.multiple_of(first_q * quarter, side), side)]
            x = x.reshape(WIN, side).astype(jnp.float32)
            finish(parts, x, wop_side[...], length, send_home.at[h], state_home.at[h])
            for i in range(2):
                @pl.when(first_q + i != m)
                def _():
                    home_state_copy(h, i).start()

                @pl.when(first_q + i == m)
                def _():
                    home_state_local(h, i).start()

            for i in range(2):
                own = jnp.logical_and(o == d, first_q + i == m)

                @pl.when(jnp.logical_not(own))
                def _():
                    home_copy(h, i).start()

                @pl.when(own)
                def _():
                    home_local(h, i).start()

        return carry

    def outer(o):
        return jnp.logical_or(4 * o < dp_size, 4 * o >= 3 * dp_size)

    def moved_user(i, carry, turn):
        j = i // reach
        s = (i - j * reach) * moving + j
        src, _ = source(s)
        mine = jnp.where(crosses(src), jnp.where(outer(src), 0, 2), 1)

        @pl.when(mine == turn)
        def _():
            row_local(s).wait()
            x = rows_in[s].reshape(WIN, D).astype(jnp.float32)
            n = norm_rows(x).astype(jnp.bfloat16)
            parts = [one_head(n, bits) for bits in range(mp_size)]
            finish(parts, x, wop[...], meta_s[src, 0, 2 * j], send.at[s], state_out.at[s])
            for q in range(mp_size):
                own = jnp.logical_and(src == d, q == m)

                @pl.when(jnp.logical_not(own))
                def _():
                    state_copy(s, q).start()

                @pl.when(own)
                def _():
                    state_local(s, q, d * per_pair + j).start()

            for q in range(mp_size):
                @pl.when(q != m)
                def _():
                    send_copy(s, q).start()

                @pl.when(q == m)
                def _():
                    send_local(s, q, src * per_pair + j).start()

        return carry

    def read_meta():
        def got_meta(i, carry):
            k = i // mp_size
            lane = i - k * mp_size

            @pl.when(lane != m)
            def _():
                pltpu.make_async_copy(meta_my.at[k], meta_my.at[k], fwd_recv.at[k, lane]).wait()

            return carry

        lax.fori_loop(0, reach * mp_size, got_meta, 0)
        to_smem = pltpu.make_async_copy(meta_in, meta_s, local_sem)
        to_smem.start()
        to_smem.wait()

        def invert(i, row):
            src = i // per_pair
            j = i - src * per_pair
            length = meta_s[src, 0, 2 * j]
            offset = meta_s[src, 0, 2 * j + 1]
            for b in range(MAXB):
                at = jnp.where(length > b * BLOCK, offset + b, -1)
                row = jnp.where(lanes == at, MAXB * i + b, row)
            return row

        inv_v[...] = lax.fori_loop(
            0, pairs, invert, jnp.full((1, 128), zero_block, jnp.int32)
        )
        back = pltpu.make_async_copy(inv_v, inv_s, local_sem)
        back.start()
        back.wait()

    for copy in near:
        copy.wait()
    if homes:
        lax.fori_loop(0, homes, near_heads, 0)
    for c in range(CHUNKS):
        far[c].wait()
        relay[c].start()
    read_meta()
    for copy in wop_copies:
        copy.wait()
    for c in range(CHUNKS):
        relay[c].wait()
    pl.semaphore_wait(group_sem, mp_size - 1)
    lax.fori_loop(0, slots, functools.partial(moved_user, turn=0), 0)
    if homes:
        lax.fori_loop(0, 2 * homes, far_heads, 0)
    lax.fori_loop(0, slots, functools.partial(moved_user, turn=1), 0)
    lax.fori_loop(0, slots, functools.partial(moved_user, turn=2), 0)

    def end_meta(k, carry):
        @pl.when(m + k != 0)
        def _():
            meta_copy(k).wait_send()

        for step in range(1, mp_size):
            forward(k, step).wait_send()
        return carry

    lax.fori_loop(0, reach, end_meta, 0)

    def end_rows(s, carry):
        @pl.when(target(s)[0] != d)
        def _():
            row_copy(s).wait_send()

        return carry

    lax.fori_loop(0, slots, end_rows, 0)

    def sent(s, carry):
        src, _ = source(s)
        for q in range(mp_size):
            @pl.when(q != m)
            def _():
                send_copy(s, q).wait_send()

            @pl.when(jnp.logical_not(jnp.logical_and(src == d, q == m)))
            def _():
                state_copy(s, q).wait_send()

        return carry

    lax.fori_loop(0, slots, sent, 0)

    def home_sent(h, carry):
        o, _ = home_target(h)
        for i in range(2):
            @pl.when(first_q + i != m)
            def _():
                home_state_copy(h, i).wait_send()

            @pl.when(jnp.logical_not(jnp.logical_and(o == d, first_q + i == m)))
            def _():
                home_copy(h, i).wait_send()

        return carry

    if homes:
        lax.fori_loop(0, homes, home_sent, 0)

    pltpu.make_async_copy(state_in, state_in, state_recv).wait()

    def pick_state(u, carry):
        at = owner_s[0, u] * per_pair + u // dp_size
        state32[pl.ds(u, 1), :] = state_in[at, 0:1, :]
        return carry

    lax.fori_loop(0, user_count, pick_state, 0)
    state[...] = state32[...].astype(state.dtype)

    every = arr.at[pl.ds(0, MAXB * pairs)]
    pltpu.make_async_copy(every, every, recv_sem).wait()


def place_kernel(arr, inv, state_in, packed, state, out_sem, state_sem):
    blocks = packed.shape[0]

    def put(b, carry):
        pltpu.make_async_copy(arr.at[inv[0, b]], packed.at[b], out_sem).start()
        return carry

    lax.fori_loop(0, blocks, put, 0, unroll=8)
    out = pltpu.make_async_copy(state_in, state, state_sem)
    out.start()
    pltpu.make_async_copy(arr.at[pl.ds(0, blocks)], packed, out_sem).wait()
    out.wait()


def per_device(tokens, w_uvqk, w_out, hist_len, owner, recv_offset, block_start):
    dp_size = lax.axis_size("dp")
    mp_size = lax.axis_size("mp")
    user_count = hist_len.shape[1]
    per_pair = -(-user_count // dp_size)
    pairs = dp_size * per_pair
    reach = dp_size // mp_size
    moving = (2 * per_pair + 2) // 3
    slots = reach * moving
    homes = max(2 * reach * (per_pair - moving), 1)
    quarter = D // mp_size
    rows = tokens.shape[0]
    blocks = rows // BLOCK
    bounds = tuple(
        blocks - max(0, user_count - (j + 1) * dp_size) for j in range(per_pair)
    )
    sizes = [b - a for a, b in zip((0,) + bounds[:-1], bounds)]

    vmem = pl.BlockSpec(memory_space=pltpu.VMEM)
    smem = pl.BlockSpec(memory_space=pltpu.SMEM)
    anywhere = pl.BlockSpec(memory_space=pltpu.HBM)
    bf16, f32, i32 = jnp.bfloat16, jnp.float32, jnp.int32
    dma = pltpu.SemaphoreType.DMA
    arr, inv, state_rows = pl.pallas_call(
        functools.partial(layer_kernel, dp_size, mp_size, per_pair, moving, user_count, bounds),
        out_shape=(
            pltpu.VMEM((MAXB * pairs + 1, BLOCK, quarter), bf16),
            pltpu.SMEM((1, 128), i32),
            pltpu.VMEM((user_count, quarter), bf16),
        ),
        in_specs=[anywhere] * 7,
        out_specs=(vmem, smem, vmem),
        scratch_shapes=[
            tuple(pltpu.VMEM((size, BLOCK, D), bf16) for size in sizes),
            pltpu.VMEM((slots, MAXB, BLOCK, D), bf16),
            pltpu.VMEM((slots, MAXB, BLOCK, D), bf16),
            pltpu.VMEM((homes, MAXB, BLOCK, D), bf16),
            pltpu.VMEM((mp_size, D, 4 * HEAD), bf16),
            pltpu.VMEM((D, D), bf16),
            pltpu.VMEM((D, D // 2), bf16),
            pltpu.VMEM((slots, mp_size, MAXB, BLOCK, quarter), bf16),
            pltpu.VMEM((slots, mp_size, 8, quarter), f32),
            pltpu.VMEM((homes, 2, MAXB, BLOCK, quarter), bf16),
            pltpu.VMEM((homes, 2, 8, quarter), f32),
            pltpu.VMEM((pairs, 8, quarter), f32),
            pltpu.VMEM((user_count, quarter), f32),
            pltpu.VMEM((reach, 1, 128), i32),
            pltpu.VMEM((dp_size, 1, 128), i32),
            pltpu.VMEM((1, 128), i32),
            pltpu.VMEM((homes, WIN, D), bf16),
            pltpu.VMEM((homes, WIN, D // 2), bf16),
            pltpu.VMEM((homes, WIN, D // 2), f32),
            pltpu.SMEM((1, user_count), i32),
            pltpu.SMEM((1, user_count), i32),
            pltpu.SMEM((1, user_count), i32),
            pltpu.SMEM((1, user_count), i32),
            pltpu.SMEM((dp_size, 1, 128), i32),
            dma((4,)),
            dma((per_pair,)),
            dma,
            dma((mp_size,)),
            dma((mp_size,)),
            dma((3, CHUNKS)),
            dma((3, CHUNKS)),
            dma((reach,)),
            dma((reach,)),
            dma((reach, mp_size)),
            dma((reach, mp_size)),
            dma((slots,)),
            dma((slots,)),
            dma((slots, mp_size)),
            dma,
            dma((slots, mp_size)),
            dma,
            dma((homes, 2)),
            dma((homes, 2)),
            dma,
            pltpu.SemaphoreType.REGULAR,
            pltpu.SemaphoreType.REGULAR,
        ],
        compiler_params=pltpu.CompilerParams(
            collective_id=0, has_side_effects=True, vmem_limit_bytes=48 * 1024 * 1024
        ),
        name="layer",
    )(
        *(
            pltpu.with_memory_space_constraint(a, pltpu.HBM)
            for a in (
                tokens.reshape(blocks, BLOCK, D), w_uvqk, w_out,
                owner, hist_len, recv_offset, block_start,
            )
        )
    )
    packed, state = pl.pallas_call(
        place_kernel,
        out_shape=(
            jax.ShapeDtypeStruct((blocks, BLOCK, quarter), bf16),
            jax.ShapeDtypeStruct((user_count, quarter), bf16),
        ),
        in_specs=[vmem, smem, vmem],
        out_specs=(anywhere, anywhere),
        scratch_shapes=[dma, dma],
        compiler_params=pltpu.CompilerParams(vmem_limit_bytes=4 * 1024 * 1024),
        name="place",
    )(
        pltpu.with_memory_space_constraint(arr, pltpu.VMEM),
        pltpu.with_memory_space_constraint(inv, pltpu.SMEM),
        pltpu.with_memory_space_constraint(state_rows, pltpu.VMEM),
    )
    return packed.reshape(rows, quarter), state


def solution(mesh):
    in_specs = (
        P("dp", None),
        P(None, "mp"),
        P(),
        P("dp", None),
        P("dp", None),
        P("dp", None),
        P("dp", None),
    )
    out_specs = (P("dp", "mp"), P("dp", "mp"))
    return jax.shard_map(
        per_device, mesh=mesh, in_specs=in_specs, out_specs=out_specs, check_vma=False
    )
```

```python
import functools

import jax
import jax.numpy as jnp
from jax import lax
from jax.experimental import pallas as pl
from jax.experimental.pallas import tpu as pltpu
from jax.sharding import PartitionSpec as P

D = 512
HEADS = 4
HEAD = D // HEADS
BLOCK = 128
MAXB = 2
WIN = MAXB * BLOCK
EPS = 1e-05
CHUNKS = 4
MESH = pl.DeviceIdType.MESH


def norm_rows(values):
    average = jnp.mean(values, axis=-1, keepdims=True)
    variance = jnp.mean(values * values, axis=-1, keepdims=True) - average * average
    return (values - average) * lax.rsqrt(variance + EPS)


def layer_kernel(
    dp_size, mp_size, per_pair, moving, user_count, bounds,
    tok_hbm, w_hbm, wout_hbm, owner_hbm, len_hbm, off_hbm, start_hbm,
    arr, inv_s, state,
    parts_of_tok, rows_out, rows_in, rows_home, wg, wop, wop_side, send, state_out, send_home, state_home,
    state_in, state32, meta_my, meta_in, inv_v, normed, gate, att,
    owner_s, len_s, off_s, start_s, meta_s,
    tab_sem, tok_sem, w_sem, wop_sem, side_sem, w_send, w_recv, meta_send, meta_recv, fwd_send, fwd_recv,
    row_send, row_recv,
    send_sem, recv_sem, state_send, state_recv, send_home_sem, state_home_sem, local_sem, line_sem, group_sem,
):
    d = lax.axis_index("dp")
    m = lax.axis_index("mp")
    quarter = D // mp_size
    reach = dp_size // mp_size
    staying = per_pair - moving
    slots = reach * moving
    homes = 2 * reach * staying
    pairs = dp_size * per_pair
    side = D // 2
    first_q = m // 2 * 2
    barrier = pltpu.get_barrier_semaphore()

    starts = (0,) + bounds[:-1]
    tok_copies = [
        pltpu.make_async_copy(
            tok_hbm.at[pl.ds(starts[p], bounds[p] - starts[p])], part, tok_sem.at[p]
        )
        for p, part in enumerate(parts_of_tok)
    ]
    tok_copies[0].start()

    def line_signal(semaphore):
        def tell(k, carry):
            ahead = m + mp_size * k
            ahead = jnp.where(ahead == 0, mp_size, ahead)
            for o in (d + ahead, d - ahead + dp_size):
                pl.semaphore_signal(
                    semaphore, inc=1, device_id={"dp": lax.rem(o, dp_size)}, device_id_type=MESH
                )
            return carry

        lax.fori_loop(0, reach, tell, 0)

    line_count = 2 * reach
    line_signal(barrier)
    for step in range(1, mp_size):
        pl.semaphore_signal(
            barrier, inc=1, device_id={"mp": lax.rem(m + step, mp_size)}, device_id_type=MESH
        )
    tables = [
        pltpu.make_async_copy(src, dst, tab_sem.at[i])
        for i, (src, dst) in enumerate(
            ((owner_hbm, owner_s), (start_hbm, start_s), (len_hbm, len_s), (off_hbm, off_s))
        )
    ]
    for table in tables:
        table.start()
    own_w = pltpu.make_async_copy(w_hbm, wg.at[0], w_sem)

    def flip(bits):
        if bits == 1:
            return m + 1 - 2 * lax.rem(m, 2)
        return lax.rem(m + 2, 4)

    wop_copies = []
    for bits in range(mp_size):
        head = m
        if bits & 1:
            head = head + 1 - 2 * lax.rem(head, 2)
        if bits & 2:
            head = lax.rem(head + 2, 4)
        copy = pltpu.make_async_copy(
            wout_hbm.at[pl.ds(pl.multiple_of(head * HEAD, HEAD), HEAD)],
            wop.at[pl.ds(bits * HEAD, HEAD)], wop_sem.at[bits],
        )
        wop_copies.append(copy)
        if homes:
            copy = pltpu.make_async_copy(
                wout_hbm.at[
                    pl.ds(pl.multiple_of(head * HEAD, HEAD), HEAD),
                    pl.ds(pl.multiple_of(first_q * quarter, side), side),
                ],
                wop_side.at[pl.ds(bits * HEAD, HEAD)], side_sem.at[bits],
            )
            wop_copies.append(copy)

    def target(s):
        k = s // moving
        return lax.rem(d + m + mp_size * k, dp_size), s - k * moving

    def source(s):
        k = s // moving
        return lax.rem(d - m - mp_size * k + 2 * dp_size, dp_size), s - k * moving

    def home_target(h):
        g = h // (reach * staying)
        r = h - g * (reach * staying)
        k = r // staying
        group = lax.rem(m + 2 * g, mp_size)
        return lax.rem(d + group + mp_size * k, dp_size), moving + r - k * staying

    def crosses(o):
        return (o < dp_size // 2) != (d < dp_size // 2)

    def find(o):
        first = 0
        found = 0
        for u in range(min(dp_size, user_count)):
            hit = owner_s[0, u] == o
            first = jnp.where(hit, u, first)
            found = jnp.where(hit, 1, found)
        return first, found

    def user_of(o, j):
        first, found = find(o)
        u = first + j * dp_size
        valid = jnp.logical_and(found == 1, u < user_count)
        return jnp.minimum(u, user_count - 1), valid

    for table in tables:
        table.wait()

    lanes = lax.broadcasted_iota(jnp.int32, (1, 128), 1)

    def fill_meta(k, carry):
        o = lax.rem(d + m + mp_size * k, dp_size)
        first, found = find(o)
        row = jnp.zeros((1, 128), jnp.int32)
        for j in range(per_pair):
            u = first + j * dp_size
            valid = jnp.logical_and(found == 1, u < user_count)
            u = jnp.minimum(u, user_count - 1)
            row = jnp.where(lanes == 2 * j, jnp.where(valid, len_s[0, u], 0), row)
            row = jnp.where(lanes == 2 * j + 1, off_s[0, u], row)
        meta_my[k] = row

        @pl.when(o == d)
        def _():
            meta_in[d] = row

        return carry

    lax.fori_loop(0, reach, fill_meta, 0)
    zero_block = 2 * pairs
    arr[zero_block] = jnp.zeros((BLOCK, quarter), arr.dtype)
    def stage(o, j, into):
        u, _ = user_of(o, j)
        start = start_s[0, u]
        for b in range(MAXB):
            at = jnp.minimum(start + b, bounds[j] - 1)
            value = parts_of_tok[0][jnp.minimum(at, bounds[0] - 1)]
            for p in range(1, j + 1):
                other = parts_of_tok[p][jnp.clip(at - starts[p], 0, bounds[p] - starts[p] - 1)]
                value = jnp.where(at >= starts[p], other, value)
            into[b] = value

    def stage_home(i, carry):
        for j in range(moving, per_pair):
            h = i * staying + j - moving
            stage(home_target(h)[0], j, rows_home.at[h])
        return carry

    def meta_copy(k):
        return pltpu.make_async_remote_copy(
            src_ref=meta_my.at[k], dst_ref=meta_in.at[d], send_sem=meta_send.at[k],
            recv_sem=meta_recv.at[k], device_id={"dp": lax.rem(d + m + mp_size * k, dp_size)},
            device_id_type=MESH,
        )

    def start_meta(k, carry):
        @pl.when(m + k != 0)
        def _():
            meta_copy(k).start()

        return carry

    def meta_from(lane, k):
        return lax.rem(d - lane - mp_size * k + 2 * dp_size, dp_size)

    def forward(k, step):
        row = meta_in.at[meta_from(m, k)]
        return pltpu.make_async_remote_copy(
            src_ref=row, dst_ref=row, send_sem=fwd_send.at[k, step],
            recv_sem=fwd_recv.at[k, m], device_id={"mp": lax.rem(m + step, mp_size)},
            device_id_type=MESH,
        )

    def forward_meta(k, carry):
        @pl.when(m + k != 0)
        def _():
            pltpu.make_async_copy(meta_my.at[k], meta_my.at[k], meta_recv.at[k]).wait()

        for step in range(1, mp_size):
            forward(k, step).start()
        return carry

    def row_copy(s):
        return pltpu.make_async_remote_copy(
            src_ref=rows_out.at[s], dst_ref=rows_in.at[s], send_sem=row_send.at[s],
            recv_sem=row_recv.at[s], device_id={"dp": target(s)[0]}, device_id_type=MESH,
        )

    def row_local(s):
        return pltpu.make_async_copy(rows_out.at[s], rows_in.at[s], row_recv.at[s])

    piece = D // CHUNKS

    def w_copy(src, dst, chunk, peer, index):
        rows = pl.ds(chunk * piece, piece)
        return pltpu.make_async_remote_copy(
            src_ref=wg.at[src, rows], dst_ref=wg.at[dst, rows], send_sem=w_send.at[index, chunk],
            recv_sem=w_recv.at[index, chunk], device_id={"mp": peer}, device_id_type=MESH,
        )

    far = [w_copy(0, 2, c, flip(2), 1) for c in range(CHUNKS)]
    near = [w_copy(0, 1, c, flip(1), 0) for c in range(CHUNKS)]
    relay = [w_copy(2, 3, c, flip(1), 2) for c in range(CHUNKS)]

    def stage_rows(i, carry, j):
        late = i // reach
        s = (i - late * reach) * moving + j
        o, _ = target(s)

        @pl.when(crosses(o) == (late == 0))
        def _():
            stage(o, j, rows_out.at[s])

        return carry

    def start_rows(i, carry, j):
        late = i // reach
        s = (i - late * reach) * moving + j
        o, _ = target(s)
        now = crosses(o) == (late == 0)

        @pl.when(jnp.logical_and(now, o != d))
        def _():
            row_copy(s).start()

        @pl.when(jnp.logical_and(now, o == d))
        def _():
            row_local(s).start()

        return carry

    tok_copies[0].wait()
    for copy in tok_copies[1:]:
        copy.start()
    own_w.start()
    lax.fori_loop(0, 2 * reach, functools.partial(stage_rows, j=0), 0)
    pl.semaphore_wait(barrier, line_count + mp_size - 1)
    lax.fori_loop(0, reach, start_meta, 0)
    lax.fori_loop(0, 2 * reach, functools.partial(start_rows, j=0), 0)
    line_signal(line_sem)
    own_w.wait()
    for copy in far:
        copy.start()
    for copy in near:
        copy.start()
    for j in range(1, moving):
        tok_copies[j].wait()
        lax.fori_loop(0, 2 * reach, functools.partial(stage_rows, j=j), 0)
        lax.fori_loop(0, 2 * reach, functools.partial(start_rows, j=j), 0)
    for copy in tok_copies[max(moving, 1):]:
        copy.wait()
    for copy in wop_copies:
        copy.start()
    lax.fori_loop(0, 2 * reach, stage_home, 0)
    pl.semaphore_wait(line_sem, line_count)
    for step in range(1, mp_size):
        pl.semaphore_signal(
            group_sem, inc=1, device_id={"mp": lax.rem(m + step, mp_size)}, device_id_type=MESH
        )
    lax.fori_loop(0, reach, forward_meta, 0)

    causal = lax.broadcasted_iota(jnp.int32, (BLOCK, BLOCK), 1) <= lax.broadcasted_iota(
        jnp.int32, (BLOCK, BLOCK), 0
    )
    half_scale = 0.5 * HEAD ** (-0.5)

    def scores(q, k):
        t = lax.dot_general(
            q, k, (((1,), (1,)), ((), ())), preferred_element_type=jnp.float32
        ) * half_scale
        return t + t * jnp.tanh(t)

    def heads(n, which):
        hidden = [jnp.dot(n, wg[bits], preferred_element_type=jnp.float32) for bits in which]
        projected = [(h + h * jnp.tanh(h)).astype(jnp.bfloat16) for h in hidden]
        weights = []
        for p in projected:
            q, k = p[:, 2 * HEAD : 3 * HEAD], p[:, 3 * HEAD :]
            low = jnp.where(causal, scores(q[:BLOCK], k[:BLOCK]), 0.0)
            high = scores(q[BLOCK:], k)
            diag = jnp.where(causal, high[:, BLOCK:], 0.0)
            high = jnp.concatenate([high[:, :BLOCK], diag], 1)
            weights.append((low.astype(jnp.bfloat16), high.astype(jnp.bfloat16)))
        parts = []
        for p, (low, high) in zip(projected, weights):
            v = p[:, HEAD : 2 * HEAD]
            first = jnp.dot(low, v[:BLOCK], preferred_element_type=jnp.float32)
            second = jnp.dot(high, v, preferred_element_type=jnp.float32)
            parts.append((p[:, :HEAD], jnp.concatenate([first, second], 0) * (1.0 / WIN)))
        return parts

    def send_copy(s, q):
        src, j = source(s)
        pair = src * per_pair + j
        return pltpu.make_async_remote_copy(
            src_ref=send.at[s, q], dst_ref=arr.at[pl.ds(MAXB * pair, MAXB)],
            send_sem=send_sem.at[s, q], recv_sem=recv_sem,
            device_id={"mp": q}, device_id_type=MESH,
        )

    def send_local(s, q, pair):
        return pltpu.make_async_copy(
            send.at[s, q], arr.at[pl.ds(MAXB * pair, MAXB)], recv_sem
        )

    def state_copy(s, q):
        src, j = source(s)
        pair = d * per_pair + j
        return pltpu.make_async_remote_copy(
            src_ref=state_out.at[s, q], dst_ref=state_in.at[pair], send_sem=state_send.at[s, q],
            recv_sem=state_recv, device_id={"dp": src, "mp": q}, device_id_type=MESH,
        )

    def state_local(s, q, pair):
        return pltpu.make_async_copy(state_out.at[s, q], state_in.at[pair], state_recv)

    def home_copy(h, i):
        o, j = home_target(h)
        pair = d * per_pair + j
        return pltpu.make_async_remote_copy(
            src_ref=send_home.at[h, i], dst_ref=arr.at[pl.ds(MAXB * pair, MAXB)],
            send_sem=send_home_sem.at[h, i], recv_sem=recv_sem,
            device_id={"dp": o, "mp": first_q + i}, device_id_type=MESH,
        )

    def home_local(h, i):
        pair = d * per_pair + home_target(h)[1]
        return pltpu.make_async_copy(
            send_home.at[h, i], arr.at[pl.ds(MAXB * pair, MAXB)], recv_sem
        )

    def home_state_copy(h, i):
        o, j = home_target(h)
        pair = o * per_pair + j
        return pltpu.make_async_remote_copy(
            src_ref=state_home.at[h, i], dst_ref=state_in.at[pair],
            send_sem=state_home_sem.at[h, i], recv_sem=state_recv,
            device_id={"mp": first_q + i}, device_id_type=MESH,
        )

    def home_state_local(h, i):
        o, j = home_target(h)
        pair = o * per_pair + j
        return pltpu.make_async_copy(
            state_home.at[h, i], state_in.at[pair], state_recv
        )

    picks = lax.broadcasted_iota(jnp.int32, (8, WIN), 1)

    def finish(parts, x, weight, length, out, chosen):
        a = jnp.concatenate([part[1] for part in parts], 1)
        g = jnp.concatenate([part[0] for part in parts], 1).astype(jnp.float32)
        gated = (norm_rows(a) * g).astype(jnp.bfloat16)
        y = jnp.dot(gated, weight, preferred_element_type=jnp.float32)
        positions = lax.broadcasted_iota(jnp.int32, y.shape, 0)
        y = jnp.where(positions < length, y + x, 0.0).astype(jnp.bfloat16)
        pick = jnp.where(picks == length - 1, 1.0, 0.0).astype(jnp.bfloat16)
        row = jnp.dot(pick, y, preferred_element_type=jnp.float32)
        for i in range(y.shape[1] // quarter):
            out[i] = y[:, i * quarter : (i + 1) * quarter].reshape(MAXB, BLOCK, quarter)
            chosen[i] = row[:, i * quarter : (i + 1) * quarter]

    half = mp_size // 2

    def near_heads(h, carry):
        x = rows_home[h].reshape(WIN, D).astype(jnp.float32)
        n = (norm_rows(x) * 0.5).astype(jnp.bfloat16)
        normed[h] = n
        parts = heads(n, range(half))
        gate[h] = jnp.concatenate([part[0] for part in parts], 1)
        att[h] = jnp.concatenate([part[1] for part in parts], 1)
        return carry

    def far_heads(i, carry):
        late = i // homes
        h = i - late * homes
        o, j = home_target(h)

        @pl.when(crosses(o) == (late == 0))
        def _():
            u, valid = user_of(o, j)
            length = jnp.where(valid, len_s[0, u], 0)
            n = normed[h]
            parts = [(gate[h], att[h])]
            parts += heads(n, range(half, mp_size))
            x = rows_home[h, :, :, pl.ds(pl.multiple_of(first_q * quarter, side), side)]
            x = x.reshape(WIN, side).astype(jnp.float32)
            finish(parts, x, wop_side[...], length, send_home.at[h], state_home.at[h])
            for i in range(2):
                @pl.when(first_q + i != m)
                def _():
                    home_state_copy(h, i).start()

                @pl.when(first_q + i == m)
                def _():
                    home_state_local(h, i).start()

            for i in range(2):
                own = jnp.logical_and(o == d, first_q + i == m)

                @pl.when(jnp.logical_not(own))
                def _():
                    home_copy(h, i).start()

                @pl.when(own)
                def _():
                    home_local(h, i).start()

        return carry

    def outer(o):
        return jnp.logical_or(4 * o < dp_size, 4 * o >= 3 * dp_size)

    def moved_user(i, carry, turn):
        j = i // reach
        s = (i - j * reach) * moving + j
        src, _ = source(s)
        mine = jnp.where(crosses(src), jnp.where(outer(src), 0, 2), 1)

        @pl.when(mine == turn)
        def _():
            row_local(s).wait()
            x = rows_in[s].reshape(WIN, D).astype(jnp.float32)
            n = (norm_rows(x) * 0.5).astype(jnp.bfloat16)
            parts = heads(n, range(mp_size))
            finish(parts, x, wop[...], meta_s[src, 0, 2 * j], send.at[s], state_out.at[s])
            for q in range(mp_size):
                own = jnp.logical_and(src == d, q == m)

                @pl.when(jnp.logical_not(own))
                def _():
                    state_copy(s, q).start()

                @pl.when(own)
                def _():
                    state_local(s, q, d * per_pair + j).start()

            for q in range(mp_size):
                @pl.when(q != m)
                def _():
                    send_copy(s, q).start()

                @pl.when(q == m)
                def _():
                    send_local(s, q, src * per_pair + j).start()

        return carry

    def read_meta():
        def got_meta(i, carry):
            k = i // mp_size
            lane = i - k * mp_size

            @pl.when(lane != m)
            def _():
                pltpu.make_async_copy(meta_my.at[k], meta_my.at[k], fwd_recv.at[k, lane]).wait()

            return carry

        lax.fori_loop(0, reach * mp_size, got_meta, 0)
        to_smem = pltpu.make_async_copy(meta_in, meta_s, local_sem)
        to_smem.start()
        to_smem.wait()

        def invert(i, row):
            src = i // per_pair
            j = i - src * per_pair
            length = meta_s[src, 0, 2 * j]
            offset = meta_s[src, 0, 2 * j + 1]
            for b in range(MAXB):
                at = jnp.where(length > b * BLOCK, offset + b, -1)
                row = jnp.where(lanes == at, MAXB * i + b, row)
            return row

        inv_v[...] = lax.fori_loop(
            0, pairs, invert, jnp.full((1, 128), zero_block, jnp.int32)
        )
        back = pltpu.make_async_copy(inv_v, inv_s, local_sem)
        back.start()
        back.wait()

    for copy in near:
        copy.wait()
    if homes:
        lax.fori_loop(0, homes, near_heads, 0)
    for c in range(CHUNKS):
        far[c].wait()
        relay[c].start()
    read_meta()
    for copy in wop_copies:
        copy.wait()
    for c in range(CHUNKS):
        relay[c].wait()
    pl.semaphore_wait(group_sem, mp_size - 1)
    lax.fori_loop(0, slots, functools.partial(moved_user, turn=0), 0)
    if homes:
        lax.fori_loop(0, 2 * homes, far_heads, 0)
    lax.fori_loop(0, slots, functools.partial(moved_user, turn=1), 0)
    lax.fori_loop(0, slots, functools.partial(moved_user, turn=2), 0)

    def end_meta(k, carry):
        @pl.when(m + k != 0)
        def _():
            meta_copy(k).wait_send()

        for step in range(1, mp_size):
            forward(k, step).wait_send()
        return carry

    lax.fori_loop(0, reach, end_meta, 0)

    def end_rows(s, carry):
        @pl.when(target(s)[0] != d)
        def _():
            row_copy(s).wait_send()

        return carry

    lax.fori_loop(0, slots, end_rows, 0)

    def sent(s, carry):
        src, _ = source(s)
        for q in range(mp_size):
            @pl.when(q != m)
            def _():
                send_copy(s, q).wait_send()

            @pl.when(jnp.logical_not(jnp.logical_and(src == d, q == m)))
            def _():
                state_copy(s, q).wait_send()

        return carry

    lax.fori_loop(0, slots, sent, 0)

    def home_sent(h, carry):
        o, _ = home_target(h)
        for i in range(2):
            @pl.when(first_q + i != m)
            def _():
                home_state_copy(h, i).wait_send()

            @pl.when(jnp.logical_not(jnp.logical_and(o == d, first_q + i == m)))
            def _():
                home_copy(h, i).wait_send()

        return carry

    if homes:
        lax.fori_loop(0, homes, home_sent, 0)

    pltpu.make_async_copy(state_in, state_in, state_recv).wait()

    def pick_state(u, carry):
        at = owner_s[0, u] * per_pair + u // dp_size
        state32[pl.ds(u, 1), :] = state_in[at, 0:1, :]
        return carry

    lax.fori_loop(0, user_count, pick_state, 0)
    state[...] = state32[...].astype(state.dtype)

    every = arr.at[pl.ds(0, MAXB * pairs)]
    pltpu.make_async_copy(every, every, recv_sem).wait()


def place_kernel(arr, inv, state_in, packed, state, out_sem, state_sem):
    blocks = packed.shape[0]

    def put(b, carry):
        pltpu.make_async_copy(arr.at[inv[0, b]], packed.at[b], out_sem).start()
        return carry

    lax.fori_loop(0, blocks, put, 0, unroll=8)
    out = pltpu.make_async_copy(state_in, state, state_sem)
    out.start()
    pltpu.make_async_copy(arr.at[pl.ds(0, blocks)], packed, out_sem).wait()
    out.wait()


def per_device(tokens, w_uvqk, w_out, hist_len, owner, recv_offset, block_start):
    dp_size = lax.axis_size("dp")
    mp_size = lax.axis_size("mp")
    user_count = hist_len.shape[1]
    per_pair = -(-user_count // dp_size)
    pairs = dp_size * per_pair
    reach = dp_size // mp_size
    moving = (2 * per_pair + 2) // 3
    slots = reach * moving
    homes = max(2 * reach * (per_pair - moving), 1)
    quarter = D // mp_size
    rows = tokens.shape[0]
    blocks = rows // BLOCK
    bounds = tuple(
        blocks - max(0, user_count - (j + 1) * dp_size) for j in range(per_pair)
    )
    sizes = [b - a for a, b in zip((0,) + bounds[:-1], bounds)]

    vmem = pl.BlockSpec(memory_space=pltpu.VMEM)
    smem = pl.BlockSpec(memory_space=pltpu.SMEM)
    anywhere = pl.BlockSpec(memory_space=pltpu.HBM)
    bf16, f32, i32 = jnp.bfloat16, jnp.float32, jnp.int32
    dma = pltpu.SemaphoreType.DMA
    arr, inv, state_rows = pl.pallas_call(
        functools.partial(layer_kernel, dp_size, mp_size, per_pair, moving, user_count, bounds),
        out_shape=(
            pltpu.VMEM((MAXB * pairs + 1, BLOCK, quarter), bf16),
            pltpu.SMEM((1, 128), i32),
            pltpu.VMEM((user_count, quarter), bf16),
        ),
        in_specs=[anywhere] * 7,
        out_specs=(vmem, smem, vmem),
        scratch_shapes=[
            tuple(pltpu.VMEM((size, BLOCK, D), bf16) for size in sizes),
            pltpu.VMEM((slots, MAXB, BLOCK, D), bf16),
            pltpu.VMEM((slots, MAXB, BLOCK, D), bf16),
            pltpu.VMEM((homes, MAXB, BLOCK, D), bf16),
            pltpu.VMEM((mp_size, D, 4 * HEAD), bf16),
            pltpu.VMEM((D, D), bf16),
            pltpu.VMEM((D, D // 2), bf16),
            pltpu.VMEM((slots, mp_size, MAXB, BLOCK, quarter), bf16),
            pltpu.VMEM((slots, mp_size, 8, quarter), f32),
            pltpu.VMEM((homes, 2, MAXB, BLOCK, quarter), bf16),
            pltpu.VMEM((homes, 2, 8, quarter), f32),
            pltpu.VMEM((pairs, 8, quarter), f32),
            pltpu.VMEM((user_count, quarter), f32),
            pltpu.VMEM((reach, 1, 128), i32),
            pltpu.VMEM((dp_size, 1, 128), i32),
            pltpu.VMEM((1, 128), i32),
            pltpu.VMEM((homes, WIN, D), bf16),
            pltpu.VMEM((homes, WIN, D // 2), bf16),
            pltpu.VMEM((homes, WIN, D // 2), f32),
            pltpu.SMEM((1, user_count), i32),
            pltpu.SMEM((1, user_count), i32),
            pltpu.SMEM((1, user_count), i32),
            pltpu.SMEM((1, user_count), i32),
            pltpu.SMEM((dp_size, 1, 128), i32),
            dma((4,)),
            dma((per_pair,)),
            dma,
            dma((mp_size,)),
            dma((mp_size,)),
            dma((3, CHUNKS)),
            dma((3, CHUNKS)),
            dma((reach,)),
            dma((reach,)),
            dma((reach, mp_size)),
            dma((reach, mp_size)),
            dma((slots,)),
            dma((slots,)),
            dma((slots, mp_size)),
            dma,
            dma((slots, mp_size)),
            dma,
            dma((homes, 2)),
            dma((homes, 2)),
            dma,
            pltpu.SemaphoreType.REGULAR,
            pltpu.SemaphoreType.REGULAR,
        ],
        compiler_params=pltpu.CompilerParams(
            collective_id=0, has_side_effects=True, vmem_limit_bytes=48 * 1024 * 1024
        ),
        name="layer",
    )(
        *(
            pltpu.with_memory_space_constraint(a, pltpu.HBM)
            for a in (
                tokens.reshape(blocks, BLOCK, D), w_uvqk, w_out,
                owner, hist_len, recv_offset, block_start,
            )
        )
    )
    packed, state = pl.pallas_call(
        place_kernel,
        out_shape=(
            jax.ShapeDtypeStruct((blocks, BLOCK, quarter), bf16),
            jax.ShapeDtypeStruct((user_count, quarter), bf16),
        ),
        in_specs=[vmem, smem, vmem],
        out_specs=(anywhere, anywhere),
        scratch_shapes=[dma, dma],
        compiler_params=pltpu.CompilerParams(vmem_limit_bytes=4 * 1024 * 1024),
        name="place",
    )(
        pltpu.with_memory_space_constraint(arr, pltpu.VMEM),
        pltpu.with_memory_space_constraint(inv, pltpu.SMEM),
        pltpu.with_memory_space_constraint(state_rows, pltpu.VMEM),
    )
    return packed.reshape(rows, quarter), state


def solution(mesh):
    in_specs = (
        P("dp", None),
        P(None, "mp"),
        P(),
        P("dp", None),
        P("dp", None),
        P("dp", None),
        P("dp", None),
    )
    out_specs = (P("dp", "mp"), P("dp", "mp"))
    return jax.shard_map(
        per_device, mesh=mesh, in_specs=in_specs, out_specs=out_specs, check_vma=False
    )
```

```python
import functools

import jax
import jax.numpy as jnp
from jax import lax
from jax.experimental import pallas as pl
from jax.experimental.pallas import tpu as pltpu
from jax.sharding import PartitionSpec as P

D = 512
HEADS = 4
HEAD = D // HEADS
BLOCK = 128
MAXB = 2
WIN = MAXB * BLOCK
EPS = 1e-05
CHUNKS = 4
MESH = pl.DeviceIdType.MESH


def norm_rows(values):
    average = jnp.mean(values, axis=-1, keepdims=True)
    variance = jnp.mean(values * values, axis=-1, keepdims=True) - average * average
    return (values - average) * lax.rsqrt(variance + EPS)


def layer_kernel(
    dp_size, mp_size, per_pair, moving, inner_moving, user_count, bounds,
    tok_hbm, w_hbm, wout_hbm, owner_hbm, len_hbm, off_hbm, start_hbm,
    arr, inv_s, state,
    parts_of_tok, rows_out, rows_in, rows_home, wg, wop, wop_side, send, state_out, send_home, state_home,
    state_in, state32, meta_my, meta_in, inv_v, normed, gate, att,
    owner_s, len_s, off_s, start_s, meta_s,
    tab_sem, tok_sem, w_sem, wop_sem, side_sem, w_send, w_recv, meta_send, meta_recv, fwd_send, fwd_recv,
    row_send, row_recv,
    send_sem, recv_sem, state_send, state_recv, send_home_sem, state_home_sem, local_sem, line_sem, group_sem,
):
    d = lax.axis_index("dp")
    m = lax.axis_index("mp")
    quarter = D // mp_size
    reach = dp_size // mp_size
    staying = per_pair - inner_moving
    slots = reach * moving
    homes = 2 * reach * staying
    pairs = dp_size * per_pair
    side = D // 2
    first_q = m // 2 * 2
    barrier = pltpu.get_barrier_semaphore()

    starts = (0,) + bounds[:-1]
    tok_copies = [
        pltpu.make_async_copy(
            tok_hbm.at[pl.ds(starts[p], bounds[p] - starts[p])], part, tok_sem.at[p]
        )
        for p, part in enumerate(parts_of_tok)
    ]
    tok_copies[0].start()

    def line_signal(semaphore):
        def tell(k, carry):
            ahead = m + mp_size * k
            ahead = jnp.where(ahead == 0, mp_size, ahead)
            for o in (d + ahead, d - ahead + dp_size):
                pl.semaphore_signal(
                    semaphore, inc=1, device_id={"dp": lax.rem(o, dp_size)}, device_id_type=MESH
                )
            return carry

        lax.fori_loop(0, reach, tell, 0)

    line_count = 2 * reach
    line_signal(barrier)
    for step in range(1, mp_size):
        pl.semaphore_signal(
            barrier, inc=1, device_id={"mp": lax.rem(m + step, mp_size)}, device_id_type=MESH
        )
    tables = [
        pltpu.make_async_copy(src, dst, tab_sem.at[i])
        for i, (src, dst) in enumerate(
            ((owner_hbm, owner_s), (start_hbm, start_s), (len_hbm, len_s), (off_hbm, off_s))
        )
    ]
    for table in tables:
        table.start()
    own_w = pltpu.make_async_copy(w_hbm, wg.at[0], w_sem)

    def flip(bits):
        if bits == 1:
            return m + 1 - 2 * lax.rem(m, 2)
        return lax.rem(m + 2, 4)

    wop_copies = []
    for bits in range(mp_size):
        head = m
        if bits & 1:
            head = head + 1 - 2 * lax.rem(head, 2)
        if bits & 2:
            head = lax.rem(head + 2, 4)
        copy = pltpu.make_async_copy(
            wout_hbm.at[pl.ds(pl.multiple_of(head * HEAD, HEAD), HEAD)],
            wop.at[pl.ds(bits * HEAD, HEAD)], wop_sem.at[bits],
        )
        wop_copies.append(copy)
        if homes:
            copy = pltpu.make_async_copy(
                wout_hbm.at[
                    pl.ds(pl.multiple_of(head * HEAD, HEAD), HEAD),
                    pl.ds(pl.multiple_of(first_q * quarter, side), side),
                ],
                wop_side.at[pl.ds(bits * HEAD, HEAD)], side_sem.at[bits],
            )
            wop_copies.append(copy)

    def target(s):
        k = s // moving
        return lax.rem(d + m + mp_size * k, dp_size), s - k * moving

    def source(s):
        k = s // moving
        return lax.rem(d - m - mp_size * k + 2 * dp_size, dp_size), s - k * moving

    def home_target(h):
        g = h // (reach * staying)
        r = h - g * (reach * staying)
        k = r // staying
        group = lax.rem(m + 2 * g, mp_size)
        return lax.rem(d + group + mp_size * k, dp_size), inner_moving + r - k * staying

    def crosses(o):
        return (o < dp_size // 2) != (d < dp_size // 2)

    def outer(o):
        return jnp.logical_or(4 * o < dp_size, 4 * o >= 3 * dp_size)

    def moves(src, o, j):
        few = jnp.logical_and(crosses(src + o - d), jnp.logical_not(outer(src)))
        few = jnp.logical_and(few, lax.rem(m, 2) == 0)
        return j < jnp.where(few, inner_moving, moving)

    def stays(h):
        o, j = home_target(h)
        return jnp.logical_not(moves(d, o, j))

    def find(o):
        first = 0
        found = 0
        for u in range(min(dp_size, user_count)):
            hit = owner_s[0, u] == o
            first = jnp.where(hit, u, first)
            found = jnp.where(hit, 1, found)
        return first, found

    def user_of(o, j):
        first, found = find(o)
        u = first + j * dp_size
        valid = jnp.logical_and(found == 1, u < user_count)
        return jnp.minimum(u, user_count - 1), valid

    for table in tables:
        table.wait()

    lanes = lax.broadcasted_iota(jnp.int32, (1, 128), 1)

    def fill_meta(k, carry):
        o = lax.rem(d + m + mp_size * k, dp_size)
        first, found = find(o)
        row = jnp.zeros((1, 128), jnp.int32)
        for j in range(per_pair):
            u = first + j * dp_size
            valid = jnp.logical_and(found == 1, u < user_count)
            u = jnp.minimum(u, user_count - 1)
            row = jnp.where(lanes == 2 * j, jnp.where(valid, len_s[0, u], 0), row)
            row = jnp.where(lanes == 2 * j + 1, off_s[0, u], row)
        meta_my[k] = row

        @pl.when(o == d)
        def _():
            meta_in[d] = row

        return carry

    lax.fori_loop(0, reach, fill_meta, 0)
    zero_block = 2 * pairs
    arr[zero_block] = jnp.zeros((BLOCK, quarter), arr.dtype)
    def stage(o, j, into):
        u, _ = user_of(o, j)
        start = start_s[0, u]
        for b in range(MAXB):
            at = jnp.minimum(start + b, bounds[j] - 1)
            value = parts_of_tok[0][jnp.minimum(at, bounds[0] - 1)]
            for p in range(1, j + 1):
                other = parts_of_tok[p][jnp.clip(at - starts[p], 0, bounds[p] - starts[p] - 1)]
                value = jnp.where(at >= starts[p], other, value)
            into[b] = value

    def stage_home(i, carry):
        for j in range(inner_moving, per_pair):
            h = i * staying + j - inner_moving

            @pl.when(stays(h))
            def _():
                stage(home_target(h)[0], j, rows_home.at[h])

        return carry

    def meta_copy(k):
        return pltpu.make_async_remote_copy(
            src_ref=meta_my.at[k], dst_ref=meta_in.at[d], send_sem=meta_send.at[k],
            recv_sem=meta_recv.at[k], device_id={"dp": lax.rem(d + m + mp_size * k, dp_size)},
            device_id_type=MESH,
        )

    def start_meta(k, carry):
        @pl.when(m + k != 0)
        def _():
            meta_copy(k).start()

        return carry

    def meta_from(lane, k):
        return lax.rem(d - lane - mp_size * k + 2 * dp_size, dp_size)

    def forward(k, step):
        row = meta_in.at[meta_from(m, k)]
        return pltpu.make_async_remote_copy(
            src_ref=row, dst_ref=row, send_sem=fwd_send.at[k, step],
            recv_sem=fwd_recv.at[k, m], device_id={"mp": lax.rem(m + step, mp_size)},
            device_id_type=MESH,
        )

    def forward_meta(k, carry):
        @pl.when(m + k != 0)
        def _():
            pltpu.make_async_copy(meta_my.at[k], meta_my.at[k], meta_recv.at[k]).wait()

        for step in range(1, mp_size):
            forward(k, step).start()
        return carry

    def row_copy(s):
        return pltpu.make_async_remote_copy(
            src_ref=rows_out.at[s], dst_ref=rows_in.at[s], send_sem=row_send.at[s],
            recv_sem=row_recv.at[s], device_id={"dp": target(s)[0]}, device_id_type=MESH,
        )

    def row_local(s):
        return pltpu.make_async_copy(rows_out.at[s], rows_in.at[s], row_recv.at[s])

    piece = D // CHUNKS

    def w_copy(src, dst, chunk, peer, index):
        rows = pl.ds(chunk * piece, piece)
        return pltpu.make_async_remote_copy(
            src_ref=wg.at[src, rows], dst_ref=wg.at[dst, rows], send_sem=w_send.at[index, chunk],
            recv_sem=w_recv.at[index, chunk], device_id={"mp": peer}, device_id_type=MESH,
        )

    far = [w_copy(0, 2, c, flip(2), 1) for c in range(CHUNKS)]
    near = [w_copy(0, 1, c, flip(1), 0) for c in range(CHUNKS)]
    relay = [w_copy(2, 3, c, flip(1), 2) for c in range(CHUNKS)]

    def stage_rows(i, carry, j):
        late = i // reach
        s = (i - late * reach) * moving + j
        o, _ = target(s)

        @pl.when(jnp.logical_and(crosses(o) == (late == 0), moves(d, o, j)))
        def _():
            stage(o, j, rows_out.at[s])

        return carry

    def start_rows(i, carry, j):
        late = i // reach
        s = (i - late * reach) * moving + j
        o, _ = target(s)
        now = jnp.logical_and(crosses(o) == (late == 0), moves(d, o, j))

        @pl.when(jnp.logical_and(now, o != d))
        def _():
            row_copy(s).start()

        @pl.when(jnp.logical_and(now, o == d))
        def _():
            row_local(s).start()

        return carry

    tok_copies[0].wait()
    for copy in tok_copies[1:]:
        copy.start()
    own_w.start()
    pl.semaphore_wait(barrier, line_count + mp_size - 1)
    lax.fori_loop(0, reach, start_meta, 0)
    lax.fori_loop(0, reach, functools.partial(stage_rows, j=0), 0)
    lax.fori_loop(0, reach, functools.partial(start_rows, j=0), 0)
    lax.fori_loop(reach, 2 * reach, functools.partial(stage_rows, j=0), 0)
    lax.fori_loop(reach, 2 * reach, functools.partial(start_rows, j=0), 0)
    line_signal(line_sem)
    own_w.wait()
    for copy in far:
        copy.start()
    for copy in near:
        copy.start()
    for j in range(1, moving):
        tok_copies[j].wait()
        lax.fori_loop(0, 2 * reach, functools.partial(stage_rows, j=j), 0)
        lax.fori_loop(0, 2 * reach, functools.partial(start_rows, j=j), 0)
    for copy in tok_copies[max(moving, 1):]:
        copy.wait()
    for copy in wop_copies:
        copy.start()
    lax.fori_loop(0, 2 * reach, stage_home, 0)
    pl.semaphore_wait(line_sem, line_count)
    for step in range(1, mp_size):
        pl.semaphore_signal(
            group_sem, inc=1, device_id={"mp": lax.rem(m + step, mp_size)}, device_id_type=MESH
        )
    lax.fori_loop(0, reach, forward_meta, 0)

    causal = lax.broadcasted_iota(jnp.int32, (BLOCK, BLOCK), 1) <= lax.broadcasted_iota(
        jnp.int32, (BLOCK, BLOCK), 0
    )
    half_scale = 0.5 * HEAD ** (-0.5)

    def scores(q, k):
        t = lax.dot_general(
            q, k, (((1,), (1,)), ((), ())), preferred_element_type=jnp.float32
        ) * half_scale
        return t + t * jnp.tanh(t)

    def heads(n, which):
        hidden = [jnp.dot(n, wg[bits], preferred_element_type=jnp.float32) for bits in which]
        projected = [(h + h * jnp.tanh(h)).astype(jnp.bfloat16) for h in hidden]
        weights = []
        for p in projected:
            q, k = p[:, 2 * HEAD : 3 * HEAD], p[:, 3 * HEAD :]
            low = jnp.where(causal, scores(q[:BLOCK], k[:BLOCK]), 0.0)
            high = scores(q[BLOCK:], k)
            diag = jnp.where(causal, high[:, BLOCK:], 0.0)
            high = jnp.concatenate([high[:, :BLOCK], diag], 1)
            weights.append((low.astype(jnp.bfloat16), high.astype(jnp.bfloat16)))
        parts = []
        for p, (low, high) in zip(projected, weights):
            v = p[:, HEAD : 2 * HEAD]
            first = jnp.dot(low, v[:BLOCK], preferred_element_type=jnp.float32)
            second = jnp.dot(high, v, preferred_element_type=jnp.float32)
            parts.append((p[:, :HEAD], jnp.concatenate([first, second], 0) * (1.0 / WIN)))
        return parts

    def send_copy(s, q):
        src, j = source(s)
        pair = src * per_pair + j
        return pltpu.make_async_remote_copy(
            src_ref=send.at[s, q], dst_ref=arr.at[pl.ds(MAXB * pair, MAXB)],
            send_sem=send_sem.at[s, q], recv_sem=recv_sem,
            device_id={"mp": q}, device_id_type=MESH,
        )

    def send_local(s, q, pair):
        return pltpu.make_async_copy(
            send.at[s, q], arr.at[pl.ds(MAXB * pair, MAXB)], recv_sem
        )

    def state_copy(s, q):
        src, j = source(s)
        pair = d * per_pair + j
        return pltpu.make_async_remote_copy(
            src_ref=state_out.at[s, q], dst_ref=state_in.at[pair], send_sem=state_send.at[s, q],
            recv_sem=state_recv, device_id={"dp": src, "mp": q}, device_id_type=MESH,
        )

    def state_local(s, q, pair):
        return pltpu.make_async_copy(state_out.at[s, q], state_in.at[pair], state_recv)

    def home_copy(h, i):
        o, j = home_target(h)
        pair = d * per_pair + j
        return pltpu.make_async_remote_copy(
            src_ref=send_home.at[h, i], dst_ref=arr.at[pl.ds(MAXB * pair, MAXB)],
            send_sem=send_home_sem.at[h, i], recv_sem=recv_sem,
            device_id={"dp": o, "mp": first_q + i}, device_id_type=MESH,
        )

    def home_local(h, i):
        pair = d * per_pair + home_target(h)[1]
        return pltpu.make_async_copy(
            send_home.at[h, i], arr.at[pl.ds(MAXB * pair, MAXB)], recv_sem
        )

    def home_state_copy(h, i):
        o, j = home_target(h)
        pair = o * per_pair + j
        return pltpu.make_async_remote_copy(
            src_ref=state_home.at[h, i], dst_ref=state_in.at[pair],
            send_sem=state_home_sem.at[h, i], recv_sem=state_recv,
            device_id={"mp": first_q + i}, device_id_type=MESH,
        )

    def home_state_local(h, i):
        o, j = home_target(h)
        pair = o * per_pair + j
        return pltpu.make_async_copy(
            state_home.at[h, i], state_in.at[pair], state_recv
        )

    picks = lax.broadcasted_iota(jnp.int32, (8, WIN), 1)

    def finish(parts, x, weight, length, out, chosen):
        a = jnp.concatenate([part[1] for part in parts], 1)
        g = jnp.concatenate([part[0] for part in parts], 1).astype(jnp.float32)
        gated = (norm_rows(a) * g).astype(jnp.bfloat16)
        y = jnp.dot(gated, weight, preferred_element_type=jnp.float32)
        positions = lax.broadcasted_iota(jnp.int32, y.shape, 0)
        y = jnp.where(positions < length, y + x, 0.0).astype(jnp.bfloat16)
        pick = jnp.where(picks == length - 1, 1.0, 0.0).astype(jnp.bfloat16)
        row = jnp.dot(pick, y, preferred_element_type=jnp.float32)
        for i in range(y.shape[1] // quarter):
            out[i] = y[:, i * quarter : (i + 1) * quarter].reshape(MAXB, BLOCK, quarter)
            chosen[i] = row[:, i * quarter : (i + 1) * quarter]

    half = mp_size // 2

    def near_heads(h, carry):
        @pl.when(stays(h))
        def _():
            near_user(h)

        return carry

    def near_user(h):
        x = rows_home[h].reshape(WIN, D).astype(jnp.float32)
        n = (norm_rows(x) * 0.5).astype(jnp.bfloat16)
        normed[h] = n
        parts = heads(n, range(half))
        gate[h] = jnp.concatenate([part[0] for part in parts], 1)
        att[h] = jnp.concatenate([part[1] for part in parts], 1)

    def far_heads(i, carry):
        late = i // homes
        h = i - late * homes
        o, j = home_target(h)

        @pl.when(jnp.logical_and(crosses(o) == (late == 0), stays(h)))
        def _():
            u, valid = user_of(o, j)
            length = jnp.where(valid, len_s[0, u], 0)
            n = normed[h]
            parts = [(gate[h], att[h])]
            parts += heads(n, range(half, mp_size))
            x = rows_home[h, :, :, pl.ds(pl.multiple_of(first_q * quarter, side), side)]
            x = x.reshape(WIN, side).astype(jnp.float32)
            finish(parts, x, wop_side[...], length, send_home.at[h], state_home.at[h])
            for i in range(2):
                @pl.when(first_q + i != m)
                def _():
                    home_state_copy(h, i).start()

                @pl.when(first_q + i == m)
                def _():
                    home_state_local(h, i).start()

            for i in range(2):
                own = jnp.logical_and(o == d, first_q + i == m)

                @pl.when(jnp.logical_not(own))
                def _():
                    home_copy(h, i).start()

                @pl.when(own)
                def _():
                    home_local(h, i).start()

        return carry

    def moved_user(i, carry, turn):
        j = i // reach
        s = (i - j * reach) * moving + j
        src, _ = source(s)
        mine = jnp.where(crosses(src), jnp.where(outer(src), 0, 2), 1)

        @pl.when(jnp.logical_and(mine == turn, moves(src, d, j)))
        def _():
            row_local(s).wait()
            x = rows_in[s].reshape(WIN, D).astype(jnp.float32)
            n = (norm_rows(x) * 0.5).astype(jnp.bfloat16)
            parts = heads(n, range(mp_size))
            finish(parts, x, wop[...], meta_s[src, 0, 2 * j], send.at[s], state_out.at[s])
            for q in range(mp_size):
                own = jnp.logical_and(src == d, q == m)

                @pl.when(jnp.logical_not(own))
                def _():
                    state_copy(s, q).start()

                @pl.when(own)
                def _():
                    state_local(s, q, d * per_pair + j).start()

            for q in range(mp_size):
                @pl.when(q != m)
                def _():
                    send_copy(s, q).start()

                @pl.when(q == m)
                def _():
                    send_local(s, q, src * per_pair + j).start()

        return carry

    def read_meta():
        def got_meta(i, carry):
            k = i // mp_size
            lane = i - k * mp_size

            @pl.when(lane != m)
            def _():
                pltpu.make_async_copy(meta_my.at[k], meta_my.at[k], fwd_recv.at[k, lane]).wait()

            return carry

        lax.fori_loop(0, reach * mp_size, got_meta, 0)
        to_smem = pltpu.make_async_copy(meta_in, meta_s, local_sem)
        to_smem.start()
        to_smem.wait()

        def invert(i, row):
            src = i // per_pair
            j = i - src * per_pair
            length = meta_s[src, 0, 2 * j]
            offset = meta_s[src, 0, 2 * j + 1]
            for b in range(MAXB):
                at = jnp.where(length > b * BLOCK, offset + b, -1)
                row = jnp.where(lanes == at, MAXB * i + b, row)
            return row

        inv_v[...] = lax.fori_loop(
            0, pairs, invert, jnp.full((1, 128), zero_block, jnp.int32)
        )
        back = pltpu.make_async_copy(inv_v, inv_s, local_sem)
        back.start()
        back.wait()

    for copy in near:
        copy.wait()
    if homes:
        lax.fori_loop(0, homes, near_heads, 0)
    for c in range(CHUNKS):
        far[c].wait()
        relay[c].start()
    read_meta()
    for copy in wop_copies:
        copy.wait()
    for c in range(CHUNKS):
        relay[c].wait()
    pl.semaphore_wait(group_sem, mp_size - 1)
    lax.fori_loop(0, slots, functools.partial(moved_user, turn=0), 0)
    if homes:
        lax.fori_loop(0, 2 * homes, far_heads, 0)
    lax.fori_loop(0, slots, functools.partial(moved_user, turn=1), 0)
    lax.fori_loop(0, slots, functools.partial(moved_user, turn=2), 0)

    def end_meta(k, carry):
        @pl.when(m + k != 0)
        def _():
            meta_copy(k).wait_send()

        for step in range(1, mp_size):
            forward(k, step).wait_send()
        return carry

    lax.fori_loop(0, reach, end_meta, 0)

    def end_rows(s, carry):
        o, j = target(s)

        @pl.when(jnp.logical_and(o != d, moves(d, o, j)))
        def _():
            row_copy(s).wait_send()

        return carry

    lax.fori_loop(0, slots, end_rows, 0)

    def sent(s, carry):
        src, j = source(s)
        mine = moves(src, d, j)
        for q in range(mp_size):
            @pl.when(jnp.logical_and(q != m, mine))
            def _():
                send_copy(s, q).wait_send()

            @pl.when(jnp.logical_and(jnp.logical_not(jnp.logical_and(src == d, q == m)), mine))
            def _():
                state_copy(s, q).wait_send()

        return carry

    lax.fori_loop(0, slots, sent, 0)

    def home_sent(h, carry):
        o, _ = home_target(h)
        mine = stays(h)
        for i in range(2):
            @pl.when(jnp.logical_and(first_q + i != m, mine))
            def _():
                home_state_copy(h, i).wait_send()

            @pl.when(
                jnp.logical_and(jnp.logical_not(jnp.logical_and(o == d, first_q + i == m)), mine)
            )
            def _():
                home_copy(h, i).wait_send()

        return carry

    if homes:
        lax.fori_loop(0, homes, home_sent, 0)

    pltpu.make_async_copy(state_in, state_in, state_recv).wait()

    def pick_state(u, carry):
        at = owner_s[0, u] * per_pair + u // dp_size
        state32[pl.ds(u, 1), :] = state_in[at, 0:1, :]
        return carry

    lax.fori_loop(0, user_count, pick_state, 0)
    state[...] = state32[...].astype(state.dtype)

    every = arr.at[pl.ds(0, MAXB * pairs)]
    pltpu.make_async_copy(every, every, recv_sem).wait()


def place_kernel(arr, inv, state_in, packed, state, out_sem, state_sem):
    blocks = packed.shape[0]

    def put(b, carry):
        pltpu.make_async_copy(arr.at[inv[0, b]], packed.at[b], out_sem).start()
        return carry

    lax.fori_loop(0, blocks, put, 0, unroll=8)
    out = pltpu.make_async_copy(state_in, state, state_sem)
    out.start()
    pltpu.make_async_copy(arr.at[pl.ds(0, blocks)], packed, out_sem).wait()
    out.wait()


def per_device(tokens, w_uvqk, w_out, hist_len, owner, recv_offset, block_start):
    dp_size = lax.axis_size("dp")
    mp_size = lax.axis_size("mp")
    user_count = hist_len.shape[1]
    per_pair = -(-user_count // dp_size)
    pairs = dp_size * per_pair
    reach = dp_size // mp_size
    moving = (2 * per_pair + 2) // 3
    slots = reach * moving
    inner_moving = max(moving - 1, 1)
    homes = max(2 * reach * (per_pair - inner_moving), 1)
    quarter = D // mp_size
    rows = tokens.shape[0]
    blocks = rows // BLOCK
    bounds = tuple(
        blocks - max(0, user_count - (j + 1) * dp_size) for j in range(per_pair)
    )
    sizes = [b - a for a, b in zip((0,) + bounds[:-1], bounds)]

    vmem = pl.BlockSpec(memory_space=pltpu.VMEM)
    smem = pl.BlockSpec(memory_space=pltpu.SMEM)
    anywhere = pl.BlockSpec(memory_space=pltpu.HBM)
    bf16, f32, i32 = jnp.bfloat16, jnp.float32, jnp.int32
    dma = pltpu.SemaphoreType.DMA
    arr, inv, state_rows = pl.pallas_call(
        functools.partial(layer_kernel, dp_size, mp_size, per_pair, moving, inner_moving, user_count, bounds),
        out_shape=(
            pltpu.VMEM((MAXB * pairs + 1, BLOCK, quarter), bf16),
            pltpu.SMEM((1, 128), i32),
            pltpu.VMEM((user_count, quarter), bf16),
        ),
        in_specs=[anywhere] * 7,
        out_specs=(vmem, smem, vmem),
        scratch_shapes=[
            tuple(pltpu.VMEM((size, BLOCK, D), bf16) for size in sizes),
            pltpu.VMEM((slots, MAXB, BLOCK, D), bf16),
            pltpu.VMEM((slots, MAXB, BLOCK, D), bf16),
            pltpu.VMEM((homes, MAXB, BLOCK, D), bf16),
            pltpu.VMEM((mp_size, D, 4 * HEAD), bf16),
            pltpu.VMEM((D, D), bf16),
            pltpu.VMEM((D, D // 2), bf16),
            pltpu.VMEM((slots, mp_size, MAXB, BLOCK, quarter), bf16),
            pltpu.VMEM((slots, mp_size, 8, quarter), f32),
            pltpu.VMEM((homes, 2, MAXB, BLOCK, quarter), bf16),
            pltpu.VMEM((homes, 2, 8, quarter), f32),
            pltpu.VMEM((pairs, 8, quarter), f32),
            pltpu.VMEM((user_count, quarter), f32),
            pltpu.VMEM((reach, 1, 128), i32),
            pltpu.VMEM((dp_size, 1, 128), i32),
            pltpu.VMEM((1, 128), i32),
            pltpu.VMEM((homes, WIN, D), bf16),
            pltpu.VMEM((homes, WIN, D // 2), bf16),
            pltpu.VMEM((homes, WIN, D // 2), f32),
            pltpu.SMEM((1, user_count), i32),
            pltpu.SMEM((1, user_count), i32),
            pltpu.SMEM((1, user_count), i32),
            pltpu.SMEM((1, user_count), i32),
            pltpu.SMEM((dp_size, 1, 128), i32),
            dma((4,)),
            dma((per_pair,)),
            dma,
            dma((mp_size,)),
            dma((mp_size,)),
            dma((3, CHUNKS)),
            dma((3, CHUNKS)),
            dma((reach,)),
            dma((reach,)),
            dma((reach, mp_size)),
            dma((reach, mp_size)),
            dma((slots,)),
            dma((slots,)),
            dma((slots, mp_size)),
            dma,
            dma((slots, mp_size)),
            dma,
            dma((homes, 2)),
            dma((homes, 2)),
            dma,
            pltpu.SemaphoreType.REGULAR,
            pltpu.SemaphoreType.REGULAR,
        ],
        compiler_params=pltpu.CompilerParams(
            collective_id=0, has_side_effects=True, vmem_limit_bytes=48 * 1024 * 1024
        ),
        name="layer",
    )(
        *(
            pltpu.with_memory_space_constraint(a, pltpu.HBM)
            for a in (
                tokens.reshape(blocks, BLOCK, D), w_uvqk, w_out,
                owner, hist_len, recv_offset, block_start,
            )
        )
    )
    packed, state = pl.pallas_call(
        place_kernel,
        out_shape=(
            jax.ShapeDtypeStruct((blocks, BLOCK, quarter), bf16),
            jax.ShapeDtypeStruct((user_count, quarter), bf16),
        ),
        in_specs=[vmem, smem, vmem],
        out_specs=(anywhere, anywhere),
        scratch_shapes=[dma, dma],
        compiler_params=pltpu.CompilerParams(vmem_limit_bytes=4 * 1024 * 1024),
        name="place",
    )(
        pltpu.with_memory_space_constraint(arr, pltpu.VMEM),
        pltpu.with_memory_space_constraint(inv, pltpu.SMEM),
        pltpu.with_memory_space_constraint(state_rows, pltpu.VMEM),
    )
    return packed.reshape(rows, quarter), state


def solution(mesh):
    in_specs = (
        P("dp", None),
        P(None, "mp"),
        P(),
        P("dp", None),
        P("dp", None),
        P("dp", None),
        P("dp", None),
    )
    out_specs = (P("dp", "mp"), P("dp", "mp"))
    return jax.shard_map(
        per_device, mesh=mesh, in_specs=in_specs, out_specs=out_specs, check_vma=False
    )
```

```python
import functools

import jax
import jax.numpy as jnp
from jax import lax
from jax.experimental import pallas as pl
from jax.experimental.pallas import tpu as pltpu
from jax.sharding import PartitionSpec as P

D = 512
HEADS = 4
HEAD = D // HEADS
BLOCK = 128
MAXB = 2
WIN = MAXB * BLOCK
EPS = 1e-05
CHUNKS = 4
MESH = pl.DeviceIdType.MESH


def norm_rows(values):
    average = jnp.mean(values, axis=-1, keepdims=True)
    variance = jnp.mean(values * values, axis=-1, keepdims=True) - average * average
    return (values - average) * lax.rsqrt(variance + EPS)


def layer_kernel(
    dp_size, mp_size, per_pair, moving, inner_moving, user_count, bounds,
    tok_hbm, w_hbm, wout_hbm, owner_hbm, len_hbm, off_hbm, start_hbm,
    arr, inv_s, state,
    parts_of_tok, rows_out, rows_in, rows_home, wg, wop, wop_side, send, state_out, send_home, state_home,
    state_in, state32, meta_my, meta_in, inv_v, normed, gate, att,
    owner_s, len_s, off_s, start_s, meta_s,
    tab_sem, tok_sem, w_sem, wop_sem, side_sem, w_send, w_recv, meta_send, meta_recv, fwd_send, fwd_recv,
    row_send, row_recv,
    send_sem, recv_sem, state_send, state_recv, send_home_sem, state_home_sem, local_sem, line_sem, group_sem,
):
    d = lax.axis_index("dp")
    m = lax.axis_index("mp")
    quarter = D // mp_size
    reach = dp_size // mp_size
    staying = per_pair - inner_moving
    slots = reach * moving
    homes = 2 * reach * staying
    pairs = dp_size * per_pair
    side = D // 2
    first_q = m // 2 * 2
    barrier = pltpu.get_barrier_semaphore()

    starts = (0,) + bounds[:-1]
    tok_copies = [
        pltpu.make_async_copy(
            tok_hbm.at[pl.ds(starts[p], bounds[p] - starts[p])], part, tok_sem.at[p]
        )
        for p, part in enumerate(parts_of_tok)
    ]
    tok_copies[0].start()

    def line_signal(semaphore):
        def tell(k, carry):
            ahead = m + mp_size * k
            ahead = jnp.where(ahead == 0, mp_size, ahead)
            for o in (d + ahead, d - ahead + dp_size):
                pl.semaphore_signal(
                    semaphore, inc=1, device_id={"dp": lax.rem(o, dp_size)}, device_id_type=MESH
                )
            return carry

        lax.fori_loop(0, reach, tell, 0)

    line_count = 2 * reach
    line_signal(barrier)
    for step in range(1, mp_size):
        pl.semaphore_signal(
            barrier, inc=1, device_id={"mp": lax.rem(m + step, mp_size)}, device_id_type=MESH
        )
    tables = [
        pltpu.make_async_copy(src, dst, tab_sem.at[i])
        for i, (src, dst) in enumerate(
            ((owner_hbm, owner_s), (start_hbm, start_s), (len_hbm, len_s), (off_hbm, off_s))
        )
    ]
    for table in tables:
        table.start()
    own_w = pltpu.make_async_copy(w_hbm, wg.at[0], w_sem)

    def flip(bits):
        if bits == 1:
            return m + 1 - 2 * lax.rem(m, 2)
        return lax.rem(m + 2, 4)

    wop_copies = []
    for bits in range(mp_size):
        head = m
        if bits & 1:
            head = head + 1 - 2 * lax.rem(head, 2)
        if bits & 2:
            head = lax.rem(head + 2, 4)
        copy = pltpu.make_async_copy(
            wout_hbm.at[pl.ds(pl.multiple_of(head * HEAD, HEAD), HEAD)],
            wop.at[pl.ds(bits * HEAD, HEAD)], wop_sem.at[bits],
        )
        wop_copies.append(copy)
        if homes:
            copy = pltpu.make_async_copy(
                wout_hbm.at[
                    pl.ds(pl.multiple_of(head * HEAD, HEAD), HEAD),
                    pl.ds(pl.multiple_of(first_q * quarter, side), side),
                ],
                wop_side.at[pl.ds(bits * HEAD, HEAD)], side_sem.at[bits],
            )
            wop_copies.append(copy)

    def target(s):
        k = s // moving
        return lax.rem(d + m + mp_size * k, dp_size), s - k * moving

    def source(s):
        k = s // moving
        return lax.rem(d - m - mp_size * k + 2 * dp_size, dp_size), s - k * moving

    def home_target(h):
        g = h // (reach * staying)
        r = h - g * (reach * staying)
        k = r // staying
        group = lax.rem(m + 2 * g, mp_size)
        return lax.rem(d + group + mp_size * k, dp_size), inner_moving + r - k * staying

    def crosses(o):
        return (o < dp_size // 2) != (d < dp_size // 2)

    def outer(o):
        return jnp.logical_or(4 * o < dp_size, 4 * o >= 3 * dp_size)

    def moves(src, o, j):
        few = jnp.logical_and(crosses(src + o - d), jnp.logical_not(outer(src)))
        few = jnp.logical_and(few, lax.rem(m, 2) == 0)
        return j < jnp.where(few, inner_moving, moving)

    def stays(h):
        o, j = home_target(h)
        return jnp.logical_not(moves(d, o, j))

    def find(o):
        first = 0
        found = 0
        for u in range(min(dp_size, user_count)):
            hit = owner_s[0, u] == o
            first = jnp.where(hit, u, first)
            found = jnp.where(hit, 1, found)
        return first, found

    def user_of(o, j):
        first, found = find(o)
        u = first + j * dp_size
        valid = jnp.logical_and(found == 1, u < user_count)
        return jnp.minimum(u, user_count - 1), valid

    for table in tables:
        table.wait()

    lanes = lax.broadcasted_iota(jnp.int32, (1, 128), 1)

    def fill_meta(k, carry):
        o = lax.rem(d + m + mp_size * k, dp_size)
        first, found = find(o)
        row = jnp.zeros((1, 128), jnp.int32)
        for j in range(per_pair):
            u = first + j * dp_size
            valid = jnp.logical_and(found == 1, u < user_count)
            u = jnp.minimum(u, user_count - 1)
            row = jnp.where(lanes == 2 * j, jnp.where(valid, len_s[0, u], 0), row)
            row = jnp.where(lanes == 2 * j + 1, off_s[0, u], row)
        meta_my[k] = row

        @pl.when(o == d)
        def _():
            meta_in[d] = row

        return carry

    lax.fori_loop(0, reach, fill_meta, 0)
    zero_block = 2 * pairs
    arr[zero_block] = jnp.zeros((BLOCK, quarter), arr.dtype)
    def stage(o, j, into):
        u, _ = user_of(o, j)
        start = start_s[0, u]
        for b in range(MAXB):
            at = jnp.minimum(start + b, bounds[j] - 1)
            value = parts_of_tok[0][jnp.minimum(at, bounds[0] - 1)]
            for p in range(1, j + 1):
                other = parts_of_tok[p][jnp.clip(at - starts[p], 0, bounds[p] - starts[p] - 1)]
                value = jnp.where(at >= starts[p], other, value)
            into[b] = value

    def stage_home(i, carry):
        for j in range(inner_moving, per_pair):
            h = i * staying + j - inner_moving

            @pl.when(stays(h))
            def _():
                stage(home_target(h)[0], j, rows_home.at[h])

        return carry

    def meta_copy(k):
        return pltpu.make_async_remote_copy(
            src_ref=meta_my.at[k], dst_ref=meta_in.at[d], send_sem=meta_send.at[k],
            recv_sem=meta_recv.at[k], device_id={"dp": lax.rem(d + m + mp_size * k, dp_size)},
            device_id_type=MESH,
        )

    def start_meta(k, carry):
        @pl.when(m + k != 0)
        def _():
            meta_copy(k).start()

        return carry

    def meta_from(lane, k):
        return lax.rem(d - lane - mp_size * k + 2 * dp_size, dp_size)

    def forward(k, step):
        row = meta_in.at[meta_from(m, k)]
        return pltpu.make_async_remote_copy(
            src_ref=row, dst_ref=row, send_sem=fwd_send.at[k, step],
            recv_sem=fwd_recv.at[k, m], device_id={"mp": lax.rem(m + step, mp_size)},
            device_id_type=MESH,
        )

    def forward_meta(k, carry):
        @pl.when(m + k != 0)
        def _():
            pltpu.make_async_copy(meta_my.at[k], meta_my.at[k], meta_recv.at[k]).wait()

        for step in range(1, mp_size):
            forward(k, step).start()
        return carry

    def row_copy(s):
        return pltpu.make_async_remote_copy(
            src_ref=rows_out.at[s], dst_ref=rows_in.at[s], send_sem=row_send.at[s],
            recv_sem=row_recv.at[s], device_id={"dp": target(s)[0]}, device_id_type=MESH,
        )

    def row_local(s):
        return pltpu.make_async_copy(rows_out.at[s], rows_in.at[s], row_recv.at[s])

    piece = D // CHUNKS

    def w_copy(src, dst, chunk, peer, index):
        rows = pl.ds(chunk * piece, piece)
        return pltpu.make_async_remote_copy(
            src_ref=wg.at[src, rows], dst_ref=wg.at[dst, rows], send_sem=w_send.at[index, chunk],
            recv_sem=w_recv.at[index, chunk], device_id={"mp": peer}, device_id_type=MESH,
        )

    far = [w_copy(0, 2, c, flip(2), 1) for c in range(CHUNKS)]
    near = [w_copy(0, 1, c, flip(1), 0) for c in range(CHUNKS)]
    relay = [w_copy(2, 3, c, flip(1), 2) for c in range(CHUNKS)]

    def stage_rows(i, carry, j):
        late = i // reach
        s = (i - late * reach) * moving + j
        o, _ = target(s)

        @pl.when(jnp.logical_and(crosses(o) == (late == 0), moves(d, o, j)))
        def _():
            stage(o, j, rows_out.at[s])

        return carry

    def start_rows(i, carry, j):
        late = i // reach
        s = (i - late * reach) * moving + j
        o, _ = target(s)
        now = jnp.logical_and(crosses(o) == (late == 0), moves(d, o, j))

        @pl.when(jnp.logical_and(now, o != d))
        def _():
            row_copy(s).start()

        @pl.when(jnp.logical_and(now, o == d))
        def _():
            row_local(s).start()

        return carry

    tok_copies[0].wait()
    for copy in tok_copies[1:]:
        copy.start()
    own_w.start()
    pl.semaphore_wait(barrier, line_count + mp_size - 1)
    lax.fori_loop(0, reach, start_meta, 0)
    lax.fori_loop(0, reach, functools.partial(stage_rows, j=0), 0)
    lax.fori_loop(0, reach, functools.partial(start_rows, j=0), 0)
    lax.fori_loop(reach, 2 * reach, functools.partial(stage_rows, j=0), 0)
    lax.fori_loop(reach, 2 * reach, functools.partial(start_rows, j=0), 0)
    line_signal(line_sem)
    own_w.wait()
    for copy in far:
        copy.start()
    for copy in near:
        copy.start()
    for j in range(1, moving):
        tok_copies[j].wait()
        lax.fori_loop(0, 2 * reach, functools.partial(stage_rows, j=j), 0)
        lax.fori_loop(0, 2 * reach, functools.partial(start_rows, j=j), 0)
    for copy in tok_copies[max(moving, 1):]:
        copy.wait()
    for copy in wop_copies:
        copy.start()
    lax.fori_loop(0, 2 * reach, stage_home, 0)
    pl.semaphore_wait(line_sem, line_count)
    for step in range(1, mp_size):
        pl.semaphore_signal(
            group_sem, inc=1, device_id={"mp": lax.rem(m + step, mp_size)}, device_id_type=MESH
        )
    lax.fori_loop(0, reach, forward_meta, 0)

    causal = lax.broadcasted_iota(jnp.int32, (BLOCK, BLOCK), 1) <= lax.broadcasted_iota(
        jnp.int32, (BLOCK, BLOCK), 0
    )
    half_scale = 0.5 * HEAD ** (-0.5)

    def scores(q, k):
        t = lax.dot_general(
            q, k, (((1,), (1,)), ((), ())), preferred_element_type=jnp.float32
        ) * half_scale
        return t + t * jnp.tanh(t)

    def heads(n, which):
        hidden = [jnp.dot(n, wg[bits], preferred_element_type=jnp.float32) for bits in which]
        projected = [(h + h * jnp.tanh(h)).astype(jnp.bfloat16) for h in hidden]
        weights = []
        for p in projected:
            q, k = p[:, 2 * HEAD : 3 * HEAD], p[:, 3 * HEAD :]
            low = jnp.where(causal, scores(q[:BLOCK], k[:BLOCK]), 0.0)
            high = scores(q[BLOCK:], k)
            diag = jnp.where(causal, high[:, BLOCK:], 0.0)
            high = jnp.concatenate([high[:, :BLOCK], diag], 1)
            weights.append((low.astype(jnp.bfloat16), high.astype(jnp.bfloat16)))
        parts = []
        for p, (low, high) in zip(projected, weights):
            v = p[:, HEAD : 2 * HEAD]
            first = jnp.dot(low, v[:BLOCK], preferred_element_type=jnp.float32)
            second = jnp.dot(high, v, preferred_element_type=jnp.float32)
            parts.append((p[:, :HEAD], jnp.concatenate([first, second], 0) * (1.0 / WIN)))
        return parts

    def send_copy(s, q):
        src, j = source(s)
        pair = src * per_pair + j
        return pltpu.make_async_remote_copy(
            src_ref=send.at[s, q], dst_ref=arr.at[pl.ds(MAXB * pair, MAXB)],
            send_sem=send_sem.at[s, q], recv_sem=recv_sem,
            device_id={"mp": q}, device_id_type=MESH,
        )

    def send_local(s, q, pair):
        return pltpu.make_async_copy(
            send.at[s, q], arr.at[pl.ds(MAXB * pair, MAXB)], recv_sem
        )

    def state_copy(s, q):
        src, j = source(s)
        pair = d * per_pair + j
        return pltpu.make_async_remote_copy(
            src_ref=state_out.at[s, q], dst_ref=state_in.at[pair], send_sem=state_send.at[s, q],
            recv_sem=state_recv, device_id={"dp": src, "mp": q}, device_id_type=MESH,
        )

    def state_local(s, q, pair):
        return pltpu.make_async_copy(state_out.at[s, q], state_in.at[pair], state_recv)

    def home_copy(h, i):
        o, j = home_target(h)
        pair = d * per_pair + j
        return pltpu.make_async_remote_copy(
            src_ref=send_home.at[h, i], dst_ref=arr.at[pl.ds(MAXB * pair, MAXB)],
            send_sem=send_home_sem.at[h, i], recv_sem=recv_sem,
            device_id={"dp": o, "mp": first_q + i}, device_id_type=MESH,
        )

    def home_local(h, i):
        pair = d * per_pair + home_target(h)[1]
        return pltpu.make_async_copy(
            send_home.at[h, i], arr.at[pl.ds(MAXB * pair, MAXB)], recv_sem
        )

    def home_state_copy(h, i):
        o, j = home_target(h)
        pair = o * per_pair + j
        return pltpu.make_async_remote_copy(
            src_ref=state_home.at[h, i], dst_ref=state_in.at[pair],
            send_sem=state_home_sem.at[h, i], recv_sem=state_recv,
            device_id={"mp": first_q + i}, device_id_type=MESH,
        )

    def home_state_local(h, i):
        o, j = home_target(h)
        pair = o * per_pair + j
        return pltpu.make_async_copy(
            state_home.at[h, i], state_in.at[pair], state_recv
        )

    picks = lax.broadcasted_iota(jnp.int32, (8, WIN), 1)

    def finish(parts, x, weight, length, out, chosen):
        a = jnp.concatenate([part[1] for part in parts], 1)
        g = jnp.concatenate([part[0] for part in parts], 1).astype(jnp.float32)
        gated = (norm_rows(a) * g).astype(jnp.bfloat16)
        y = jnp.dot(gated, weight, preferred_element_type=jnp.float32)
        positions = lax.broadcasted_iota(jnp.int32, y.shape, 0)
        y = jnp.where(positions < length, y + x, 0.0).astype(jnp.bfloat16)
        pick = jnp.where(picks == length - 1, 1.0, 0.0).astype(jnp.bfloat16)
        row = jnp.dot(pick, y, preferred_element_type=jnp.float32)
        for i in range(y.shape[1] // quarter):
            out[i] = y[:, i * quarter : (i + 1) * quarter].reshape(MAXB, BLOCK, quarter)
            chosen[i] = row[:, i * quarter : (i + 1) * quarter]

    half = mp_size // 2

    def near_heads(h, carry):
        @pl.when(stays(h))
        def _():
            near_user(h)

        return carry

    def near_user(h):
        x = rows_home[h].reshape(WIN, D).astype(jnp.float32)
        n = (norm_rows(x) * 0.5).astype(jnp.bfloat16)
        normed[h] = n
        parts = heads(n, range(half))
        gate[h] = jnp.concatenate([part[0] for part in parts], 1)
        att[h] = jnp.concatenate([part[1] for part in parts], 1)

    def far_heads(i, carry):
        late = i // homes
        h = i - late * homes
        o, j = home_target(h)

        @pl.when(jnp.logical_and(crosses(o) == (late == 0), stays(h)))
        def _():
            u, valid = user_of(o, j)
            length = jnp.where(valid, len_s[0, u], 0)
            n = normed[h]
            parts = [(gate[h], att[h])]
            parts += heads(n, range(half, mp_size))
            x = rows_home[h, :, :, pl.ds(pl.multiple_of(first_q * quarter, side), side)]
            x = x.reshape(WIN, side).astype(jnp.float32)
            finish(parts, x, wop_side[...], length, send_home.at[h], state_home.at[h])
            for i in range(2):
                @pl.when(first_q + i != m)
                def _():
                    home_state_copy(h, i).start()

                @pl.when(first_q + i == m)
                def _():
                    home_state_local(h, i).start()

            for i in range(2):
                own = jnp.logical_and(o == d, first_q + i == m)

                @pl.when(jnp.logical_not(own))
                def _():
                    home_copy(h, i).start()

                @pl.when(own)
                def _():
                    home_local(h, i).start()

        return carry

    def moved_user(i, carry, turn):
        j = i // reach
        s = (i - j * reach) * moving + j
        src, _ = source(s)
        mine = jnp.where(crosses(src), jnp.where(outer(src), 0, 2), 1)

        @pl.when(jnp.logical_and(mine == turn, moves(src, d, j)))
        def _():
            row_local(s).wait()
            x = rows_in[s].reshape(WIN, D).astype(jnp.float32)
            n = (norm_rows(x) * 0.5).astype(jnp.bfloat16)
            parts = heads(n, range(mp_size))
            finish(parts, x, wop[...], meta_s[src, 0, 2 * j], send.at[s], state_out.at[s])
            for q in range(mp_size):
                own = jnp.logical_and(src == d, q == m)

                @pl.when(jnp.logical_not(own))
                def _():
                    state_copy(s, q).start()

                @pl.when(own)
                def _():
                    state_local(s, q, d * per_pair + j).start()

            for q in range(mp_size):
                @pl.when(q != m)
                def _():
                    send_copy(s, q).start()

                @pl.when(q == m)
                def _():
                    send_local(s, q, src * per_pair + j).start()

        return carry

    def read_meta():
        def got_meta(i, carry):
            k = i // mp_size
            lane = i - k * mp_size

            @pl.when(lane != m)
            def _():
                pltpu.make_async_copy(meta_my.at[k], meta_my.at[k], fwd_recv.at[k, lane]).wait()

            return carry

        lax.fori_loop(0, reach * mp_size, got_meta, 0)
        to_smem = pltpu.make_async_copy(meta_in, meta_s, local_sem)
        to_smem.start()
        to_smem.wait()

        def invert(i, row):
            src = i // per_pair
            j = i - src * per_pair
            length = meta_s[src, 0, 2 * j]
            offset = meta_s[src, 0, 2 * j + 1]
            for b in range(MAXB):
                at = jnp.where(length > b * BLOCK, offset + b, -1)
                row = jnp.where(lanes == at, MAXB * i + b, row)
            return row

        inv_v[...] = lax.fori_loop(
            0, pairs, invert, jnp.full((1, 128), zero_block, jnp.int32)
        )
        back = pltpu.make_async_copy(inv_v, inv_s, local_sem)
        back.start()
        back.wait()

    for copy in near:
        copy.wait()
    if homes:
        lax.fori_loop(0, homes, near_heads, 0)
    for c in range(CHUNKS):
        far[c].wait()
        relay[c].start()
    read_meta()
    for copy in wop_copies:
        copy.wait()
    for c in range(CHUNKS):
        relay[c].wait()
    pl.semaphore_wait(group_sem, mp_size - 1)
    lax.fori_loop(0, slots, functools.partial(moved_user, turn=0), 0)
    if homes:
        lax.fori_loop(0, homes, far_heads, 0)
    lax.fori_loop(0, slots, functools.partial(moved_user, turn=1), 0)
    if homes:
        lax.fori_loop(homes, 2 * homes, far_heads, 0)
    lax.fori_loop(0, slots, functools.partial(moved_user, turn=2), 0)

    def end_meta(k, carry):
        @pl.when(m + k != 0)
        def _():
            meta_copy(k).wait_send()

        for step in range(1, mp_size):
            forward(k, step).wait_send()
        return carry

    lax.fori_loop(0, reach, end_meta, 0)

    def end_rows(s, carry):
        o, j = target(s)

        @pl.when(jnp.logical_and(o != d, moves(d, o, j)))
        def _():
            row_copy(s).wait_send()

        return carry

    lax.fori_loop(0, slots, end_rows, 0)

    def sent(s, carry):
        src, j = source(s)
        mine = moves(src, d, j)
        for q in range(mp_size):
            @pl.when(jnp.logical_and(q != m, mine))
            def _():
                send_copy(s, q).wait_send()

            @pl.when(jnp.logical_and(jnp.logical_not(jnp.logical_and(src == d, q == m)), mine))
            def _():
                state_copy(s, q).wait_send()

        return carry

    lax.fori_loop(0, slots, sent, 0)

    def home_sent(h, carry):
        o, _ = home_target(h)
        mine = stays(h)
        for i in range(2):
            @pl.when(jnp.logical_and(first_q + i != m, mine))
            def _():
                home_state_copy(h, i).wait_send()

            @pl.when(
                jnp.logical_and(jnp.logical_not(jnp.logical_and(o == d, first_q + i == m)), mine)
            )
            def _():
                home_copy(h, i).wait_send()

        return carry

    if homes:
        lax.fori_loop(0, homes, home_sent, 0)

    pltpu.make_async_copy(state_in, state_in, state_recv).wait()

    def pick_state(u, carry):
        at = owner_s[0, u] * per_pair + u // dp_size
        state32[pl.ds(u, 1), :] = state_in[at, 0:1, :]
        return carry

    lax.fori_loop(0, user_count, pick_state, 0)
    state[...] = state32[...].astype(state.dtype)

    every = arr.at[pl.ds(0, MAXB * pairs)]
    pltpu.make_async_copy(every, every, recv_sem).wait()


def place_kernel(arr, inv, state_in, packed, state, out_sem, state_sem):
    blocks = packed.shape[0]

    def put(b, carry):
        pltpu.make_async_copy(arr.at[inv[0, b]], packed.at[b], out_sem).start()
        return carry

    out = pltpu.make_async_copy(state_in, state, state_sem)
    out.start()
    lax.fori_loop(0, blocks, put, 0, unroll=True)
    pltpu.make_async_copy(arr.at[pl.ds(0, blocks)], packed, out_sem).wait()
    out.wait()


def per_device(tokens, w_uvqk, w_out, hist_len, owner, recv_offset, block_start):
    dp_size = lax.axis_size("dp")
    mp_size = lax.axis_size("mp")
    user_count = hist_len.shape[1]
    per_pair = -(-user_count // dp_size)
    pairs = dp_size * per_pair
    reach = dp_size // mp_size
    moving = (2 * per_pair + 2) // 3
    slots = reach * moving
    inner_moving = max(moving - 1, 1)
    homes = max(2 * reach * (per_pair - inner_moving), 1)
    quarter = D // mp_size
    rows = tokens.shape[0]
    blocks = rows // BLOCK
    bounds = tuple(
        blocks - max(0, user_count - (j + 1) * dp_size) for j in range(per_pair)
    )
    sizes = [b - a for a, b in zip((0,) + bounds[:-1], bounds)]

    vmem = pl.BlockSpec(memory_space=pltpu.VMEM)
    smem = pl.BlockSpec(memory_space=pltpu.SMEM)
    anywhere = pl.BlockSpec(memory_space=pltpu.HBM)
    bf16, f32, i32 = jnp.bfloat16, jnp.float32, jnp.int32
    dma = pltpu.SemaphoreType.DMA
    arr, inv, state_rows = pl.pallas_call(
        functools.partial(layer_kernel, dp_size, mp_size, per_pair, moving, inner_moving, user_count, bounds),
        out_shape=(
            pltpu.VMEM((MAXB * pairs + 1, BLOCK, quarter), bf16),
            pltpu.SMEM((1, 128), i32),
            pltpu.VMEM((user_count, quarter), bf16),
        ),
        in_specs=[anywhere] * 7,
        out_specs=(vmem, smem, vmem),
        scratch_shapes=[
            tuple(pltpu.VMEM((size, BLOCK, D), bf16) for size in sizes),
            pltpu.VMEM((slots, MAXB, BLOCK, D), bf16),
            pltpu.VMEM((slots, MAXB, BLOCK, D), bf16),
            pltpu.VMEM((homes, MAXB, BLOCK, D), bf16),
            pltpu.VMEM((mp_size, D, 4 * HEAD), bf16),
            pltpu.VMEM((D, D), bf16),
            pltpu.VMEM((D, D // 2), bf16),
            pltpu.VMEM((slots, mp_size, MAXB, BLOCK, quarter), bf16),
            pltpu.VMEM((slots, mp_size, 8, quarter), f32),
            pltpu.VMEM((homes, 2, MAXB, BLOCK, quarter), bf16),
            pltpu.VMEM((homes, 2, 8, quarter), f32),
            pltpu.VMEM((pairs, 8, quarter), f32),
            pltpu.VMEM((user_count, quarter), f32),
            pltpu.VMEM((reach, 1, 128), i32),
            pltpu.VMEM((dp_size, 1, 128), i32),
            pltpu.VMEM((1, 128), i32),
            pltpu.VMEM((homes, WIN, D), bf16),
            pltpu.VMEM((homes, WIN, D // 2), bf16),
            pltpu.VMEM((homes, WIN, D // 2), f32),
            pltpu.SMEM((1, user_count), i32),
            pltpu.SMEM((1, user_count), i32),
            pltpu.SMEM((1, user_count), i32),
            pltpu.SMEM((1, user_count), i32),
            pltpu.SMEM((dp_size, 1, 128), i32),
            dma((4,)),
            dma((per_pair,)),
            dma,
            dma((mp_size,)),
            dma((mp_size,)),
            dma((3, CHUNKS)),
            dma((3, CHUNKS)),
            dma((reach,)),
            dma((reach,)),
            dma((reach, mp_size)),
            dma((reach, mp_size)),
            dma((slots,)),
            dma((slots,)),
            dma((slots, mp_size)),
            dma,
            dma((slots, mp_size)),
            dma,
            dma((homes, 2)),
            dma((homes, 2)),
            dma,
            pltpu.SemaphoreType.REGULAR,
            pltpu.SemaphoreType.REGULAR,
        ],
        compiler_params=pltpu.CompilerParams(
            collective_id=0, has_side_effects=True, vmem_limit_bytes=48 * 1024 * 1024
        ),
        name="layer",
    )(
        *(
            pltpu.with_memory_space_constraint(a, pltpu.HBM)
            for a in (
                tokens.reshape(blocks, BLOCK, D), w_uvqk, w_out,
                owner, hist_len, recv_offset, block_start,
            )
        )
    )
    packed, state = pl.pallas_call(
        place_kernel,
        out_shape=(
            jax.ShapeDtypeStruct((blocks, BLOCK, quarter), bf16),
            jax.ShapeDtypeStruct((user_count, quarter), bf16),
        ),
        in_specs=[vmem, smem, vmem],
        out_specs=(anywhere, anywhere),
        scratch_shapes=[dma, dma],
        compiler_params=pltpu.CompilerParams(vmem_limit_bytes=4 * 1024 * 1024),
        name="place",
    )(
        pltpu.with_memory_space_constraint(arr, pltpu.VMEM),
        pltpu.with_memory_space_constraint(inv, pltpu.SMEM),
        pltpu.with_memory_space_constraint(state_rows, pltpu.VMEM),
    )
    return packed.reshape(rows, quarter), state


def solution(mesh):
    in_specs = (
        P("dp", None),
        P(None, "mp"),
        P(),
        P("dp", None),
        P("dp", None),
        P("dp", None),
        P("dp", None),
    )
    out_specs = (P("dp", "mp"), P("dp", "mp"))
    return jax.shard_map(
        per_device, mesh=mesh, in_specs=in_specs, out_specs=out_specs, check_vma=False
    )
```
